32 devices in a mesh: replica: 2 (over y), kv: 4 (over z), head: 2 (over x), sub: 2 (over core).
Axes of the slice: x: 2, y: 2, z: 4, core: 2. Of those that a mesh axis runs over, the one named last changes fastest.
Arguments:
- queries: bfloat16 [256, 64, 128], P(('replica', 'kv'), 'head'), parts along dimension 0, may hold values from -12 to 12
- sys_keys: bfloat16 [16, 1024, 128], P(('replica', 'head'), ('kv', 'sub')), parts along dimension 0, may hold values from -5 to 5
- sys_values: bfloat16 [16, 1024, 128], P(('replica', 'head'), ('kv', 'sub')), parts along dimension 0, may hold values from -6 to 6
- task_keys: bfloat16 [8, 8, 4096, 128], P(('replica', 'kv'), 'head', 'sub'), parts along dimension 0, may hold values from -5 to 5
- task_values: bfloat16 [8, 8, 4096, 128], P(('replica', 'kv'), 'head', 'sub'), parts along dimension 0, may hold values from -6 to 6
- suffix_keys: bfloat16 [256, 8, 512, 128], P(('replica', 'kv', 'sub'), 'head'), parts along dimension 0, may hold values from -5 to 5
- suffix_values: bfloat16 [256, 8, 512, 128], P(('replica', 'kv', 'sub'), 'head'), parts along dimension 0, may hold values from -6 to 6
- task_ids: int32 [256], P(('replica', 'kv')), parts along dimension 0, may hold values from 0 to 3, as said below
- suffix_len: int32 [256], P(('replica', 'kv', 'sub')), parts along dimension 0, may hold values from 256 to 512, as said below
Outputs:
- attended: bfloat16 [256, 64, 128], P(('replica', 'kv', 'sub'), 'head'), parts along dimension 0
The draws below stay inside these ranges and needn't reach their ends.
There are 2 independent parts, one for each index of `replica`. The reference program is written for one: setup_inputs(seed, part) draws one part's arguments, and reference() takes and returns one part's arrays. A program takes and returns all parts, laid end to end along the dimension named above; each array names one. Nothing has to cross between parts.
Inputs may be any that keep to these rules, and one draw needn't show every extreme that they name: `task_ids`: task t's prefix is task_keys[t]. The rows 2 * 16 * p to 2 * 16 * (p + 1) - 1 form aligned blocks; in each block no task is named more than 8 times, and one task, the same for all blocks, is named exactly 8 times in every block. `suffix_len`: each aligned block of 16 rows holds one length equal to 512.
All inputs are finite; a program needn't handle non-finite values.
Results may differ from the reference program's by a relative error of at most 0.005.
Values may be sent and summed in bfloat16 or wider, within the bound.
A program may use at most 64 MiB of HBM per device.

```python
import math
import jax
import jax.numpy as jnp
from jax import lax

QH = 64
KVH = 8
HD = 128
SEQ_DEV = 16
TASK = 4096
SUF = 512
CAP = 8
SEQS = 128
SYS = 1024
TASKS = 4


def draw_keys_like(key, tag_value, full_shape):
    own_key = jax.random.fold_in(key, tag_value)
    first_key = jax.random.fold_in(own_key, 0)
    drawn = jnp.clip(jax.random.normal(first_key, full_shape, jnp.float32), -5.0, 5.0)
    return drawn.astype(jnp.bfloat16)


def draw_queries(key, part):
    own_key = jax.random.fold_in(key, 11)
    first_key = jax.random.fold_in(own_key, 0)
    drawn = jax.random.normal(first_key, (SEQS, QH, HD), jnp.float32) * 2.5
    return jnp.clip(drawn, -12.0, 12.0).astype(jnp.bfloat16)


def draw_sys_keys(key, part):
    return draw_keys_like(key, 31, (KVH, SYS, HD))


def draw_task_keys(key, part):
    return draw_keys_like(key, 37, (TASKS, KVH, TASK, HD))


def draw_suffix_keys(key, part):
    return draw_keys_like(key, 41, (SEQS, KVH, SUF, HD))


def draw_task_ids(key, part):
    own_key = jax.random.fold_in(key, 23)
    pair_count = SEQS // (2 * SEQ_DEV)
    busiest = jax.random.randint(jax.random.fold_in(own_key, 1), (), 0, TASKS)
    tickets = jnp.repeat(jnp.arange(TASKS - 1, dtype=jnp.int32), CAP)
    others = tickets + (tickets >= busiest).astype(jnp.int32)

    def one_pair(pair_index):
        pair_key = jax.random.fold_in(own_key, pair_index + 2)
        chosen = jax.random.permutation(jax.random.fold_in(pair_key, 0), others)[:2 * SEQ_DEV - CAP]
        joined = jnp.concatenate([chosen, jnp.full((CAP,), busiest, jnp.int32)])
        return jax.random.permutation(jax.random.fold_in(pair_key, 1), joined)
    return jax.vmap(one_pair)(jnp.arange(pair_count, dtype=jnp.int32)).reshape(SEQS).astype(jnp.int32)


def draw_suffix_len(key, part):
    own_key = jax.random.fold_in(key, 29)
    lengths = jax.random.randint(jax.random.fold_in(own_key, 1), (SEQS,), SUF // 2, SUF + 1)
    picked = jax.random.randint(jax.random.fold_in(own_key, 2), (SEQS // SEQ_DEV,), 0, SEQ_DEV)
    within = jnp.arange(SEQS, dtype=jnp.int32) % SEQ_DEV
    return jnp.where(within == jnp.repeat(picked, SEQ_DEV), SUF, lengths).astype(jnp.int32)


def level_of(rng, extent, pieces, least, high):
    def one(dim, blocks):
        draws = jax.random.uniform(jax.random.fold_in(jax.random.fold_in(rng, 6), dim), (blocks,), jnp.float32, least / len(pieces), high / len(pieces))
        return jnp.repeat(jnp.exp(draws), extent[dim] // blocks).reshape((-1,) + (1,) * (len(extent) - dim - 1))

    gain = one(*pieces[0])
    for cut in pieces[1:]:
        gain = gain * one(*cut)
    return gain


def bell_draw(stream_key, shape, deviation, most, cuts=(), kind=jnp.bfloat16):
    level = level_of(stream_key, shape, cuts, -0.22, 0.18) if cuts else 1.0
    entries = jax.random.normal(stream_key, shape, jnp.float32) * deviation * level
    return jnp.minimum(jnp.maximum(entries, -most), most).astype(kind)


def setup_inputs(seed: int = 0, part: int = 0) -> dict:
    key_of = jax.random.split(jax.random.key(seed), 10)
    part_keys = jax.random.split(jax.random.fold_in(key_of[9], part), 10)
    return {
        "queries": draw_queries(jax.random.fold_in(jax.random.fold_in(key_of[9], part), 71), part),
        "sys_keys": draw_sys_keys(jax.random.fold_in(jax.random.fold_in(key_of[9], part), 71), part),
        "sys_values": bell_draw(part_keys[2], (KVH, SYS, HD), 1.0, 6.0, ((0, 2), (1, 8))),
        "task_keys": draw_task_keys(jax.random.fold_in(jax.random.fold_in(key_of[9], part), 71), part),
        "task_values": bell_draw(part_keys[4], (TASKS, KVH, TASK, HD), 1.0, 6.0, ((0, 4), (1, 2), (2, 2))),
        "suffix_keys": draw_suffix_keys(jax.random.fold_in(jax.random.fold_in(key_of[9], part), 71), part),
        "suffix_values": bell_draw(part_keys[6], (SEQS, KVH, SUF, HD), 1.0, 6.0, ((0, 8), (1, 2))),
        "task_ids": draw_task_ids(jax.random.fold_in(jax.random.fold_in(key_of[9], part), 71), part),
        "suffix_len": draw_suffix_len(jax.random.fold_in(jax.random.fold_in(key_of[9], part), 71), part),
    }


NEGATIVE = -1e+30

def level_partial(query_rows, level_keys, level_values, usable):
    score_scale = 1.0 / math.sqrt(HD)
    scores = jnp.einsum('kgd,kld->kgl', query_rows, level_keys.astype(jnp.float32)) * score_scale
    scores = jnp.where(usable[None, None, :], scores, NEGATIVE)
    maxima = lax.optimization_barrier(jnp.max(scores, axis=2))
    weights = jnp.where(usable[None, None, :], jnp.exp(scores - maxima[:, :, None]), 0.0)
    totals = lax.optimization_barrier(jnp.sum(weights, axis=2))
    rounded = lax.optimization_barrier(weights.astype(jnp.bfloat16))
    numerator = jnp.einsum('kgl,kld->kgd', rounded.astype(jnp.float32), level_values.astype(jnp.float32))
    return (maxima, totals, numerator)

def reference(queries, sys_keys, sys_values, task_keys, task_values, suffix_keys, suffix_values, task_ids, suffix_len):
    group_size = QH // KVH
    every_system = jnp.ones((SYS,), dtype=jnp.bool_)
    every_task = jnp.ones((TASK,), dtype=jnp.bool_)
    positions = jnp.arange(SUF, dtype=jnp.int32)

    def per_sequence(packed):
        query_row, task_index, length, own_keys, own_values = packed
        query_rows = query_row.astype(jnp.float32).reshape(KVH, group_size, HD)
        chosen_keys = lax.dynamic_index_in_dim(task_keys, task_index.astype(jnp.int32), 0, keepdims=False)
        chosen_values = lax.dynamic_index_in_dim(task_values, task_index.astype(jnp.int32), 0, keepdims=False)
        system_level = level_partial(query_rows, sys_keys, sys_values, every_system)
        task_level = level_partial(query_rows, chosen_keys, chosen_values, every_task)
        suffix_level = level_partial(query_rows, own_keys, own_values, positions < length)
        highest = jnp.maximum(jnp.maximum(system_level[0], task_level[0]), suffix_level[0])
        system_factor = jnp.exp(system_level[0] - highest)
        task_factor = jnp.exp(task_level[0] - highest)
        suffix_factor = jnp.exp(suffix_level[0] - highest)
        totals = system_level[1] * system_factor + task_level[1] * task_factor + suffix_level[1] * suffix_factor
        numerator = system_level[2] * system_factor[:, :, None] + task_level[2] * task_factor[:, :, None] + suffix_level[2] * suffix_factor[:, :, None]
        return (numerator / totals[:, :, None]).reshape(QH, HD).astype(jnp.bfloat16)
    return lax.map(per_sequence, (queries, task_ids, suffix_len, suffix_keys, suffix_values))
```

```python
import functools
import math

import jax
import jax.numpy as jnp
from jax import lax
from jax.experimental import pallas as pl
from jax.experimental.pallas import tpu as pltpu
from jax.sharding import PartitionSpec as P

CAP = 8
NEGATIVE = -1e30
MESH = pl.DeviceIdType.MESH
NT = (((1,), (1,)), ((), ()))
TN = (((0,), (0,)), ((), ()))
F32 = jnp.float32
BF16 = jnp.bfloat16


def dot(a, b, dims=(((1,), (0,)), ((), ()))):
    return lax.dot_general(a, b, dims, preferred_element_type=F32)


def merge(first, second):
    top = jnp.maximum(first[1], second[1])
    a = jnp.exp(first[1] - top)
    b = jnp.exp(second[1] - top)
    total = a + b
    inverse = 1.0 / total
    return first[0] * (a * inverse) + second[0] * (b * inverse), top + jnp.log(total)


def iota(shape, dim):
    return lax.broadcasted_iota(jnp.int32, shape, dim)


def selected(value, picks, pieces):
    out = None
    for _ in range(pieces):
        part = value.astype(BF16)
        value = value - part.astype(F32)
        term = dot(part, picks)
        out = term if out is None else out + term
    return out


def kernel(
    n,
    q_ref,
    sk_ref,
    sv_ref,
    tk_hbm,
    tv_hbm,
    uk_hbm,
    uv_hbm,
    ids_ref,
    len_ref,
    out_ref,
    tk,
    tv,
    uk,
    uv,
    qbuf,
    part_o,
    part_e,
    swap_o,
    swap_e,
    send_o,
    send_e,
    chain_o,
    chain_e,
    fin_o,
    fin_e,
    suf_o,
    suf_e,
    out32,
    task_sem,
    suf_sem,
    own_send,
    z_send,
    z_recv,
    d_send,
    d_recv,
    swap_send,
    swap_recv,
    chain_send,
    chain_recv,
    fin_send,
    fin_recv,
):
    rows, heads, width = q_ref.shape
    kv = sk_ref.shape[0]
    group = heads // kv
    own = uk.shape[0]
    lanes = qbuf.shape[2]
    half = lanes // 2
    task_rows = CAP * group
    scale = 1.0 / math.sqrt(width)
    j = lax.axis_index("kv")
    s = lax.axis_index("sub")
    other = 1 - s

    task_copies = []
    for index, (hbm, buf) in enumerate(((tk_hbm, tk), (tv_hbm, tv))):
        copy = pltpu.make_async_copy(hbm.at[0], buf, task_sem.at[index])
        copy.start()
        task_copies.append(copy)

    def suffix_copies(i):
        return (
            pltpu.make_async_copy(uk_hbm.at[i], uk.at[i], suf_sem.at[0, i]),
            pltpu.make_async_copy(uv_hbm.at[i], uv.at[i], suf_sem.at[1, i]),
        )

    @pl.loop(0, own)
    def _(i):
        for copy in suffix_copies(i):
            copy.start()

    barrier = pltpu.get_barrier_semaphore()
    pl.semaphore_signal(barrier, inc=1, device_id={"sub": other}, device_id_type=MESH)

    @pl.when(j > 0)
    def _():
        pl.semaphore_signal(barrier, inc=1, device_id={"kv": j - 1}, device_id_type=MESH)

    @pl.when(j < n - 1)
    def _():
        pl.semaphore_signal(barrier, inc=1, device_id={"kv": j + 1}, device_id_type=MESH)

    ids = ids_ref[...].astype(F32)
    wide = jnp.broadcast_to(ids, (rows, rows))
    down, across = iota((rows, rows), 0), iota((rows, rows), 1)
    ids_column = jnp.sum(jnp.where(down == across, wide, 0.0), axis=1, keepdims=True)
    same = jnp.where((ids_column == wide) & (down < across), 1.0, 0.0)
    places = ids * CAP + jnp.sum(same, axis=0, keepdims=True)
    places8 = jnp.broadcast_to(places, (8, rows)).astype(BF16)

    def spread(count, base):
        shape = (rows, count * group)
        pick = jnp.where(iota(shape, 0) == base + iota(shape, 1) // group, 1.0, 0.0).astype(BF16)
        row = dot(places8, pick)[0:1].astype(jnp.int32)
        shape = (lanes, count * group)
        down, across = iota(shape, 0), iota(shape, 1)
        hit = (down // group == row) & (down % group == across % group)
        return jnp.where(hit, 1.0, 0.0).astype(BF16)

    everyone = spread(rows, 0)
    wide_query = q_ref[...].astype(F32)
    for k in range(kv):
        mine = wide_query[:, k * group : (k + 1) * group, :].reshape(rows * group, width)
        qbuf[j, k] = dot(everyone, mine.astype(BF16)).astype(BF16)

    pl.semaphore_wait(
        barrier, 1 + jnp.where(j > 0, 1, 0) + jnp.where(j < n - 1, 1, 0)
    )

    def query_view(p, k, h):
        return qbuf.at[p, k, pl.ds(pl.multiple_of(h * half, 16), half), :]

    def query_copy(p, k, send_sem, recv_sem, device):
        return pltpu.make_async_remote_copy(
            src_ref=query_view(p, k, s),
            dst_ref=query_view(p, k, s),
            send_sem=send_sem,
            recv_sem=recv_sem,
            device_id=device,
            device_id_type=MESH,
        )

    def own_copy(k, d):
        return query_copy(j, k, own_send.at[d, k], z_recv.at[j, k], {"kv": j + 2 * d - 1})

    def relay_copy(p, k, d):
        return query_copy(p, k, z_send.at[p, k], z_recv.at[p, k], {"kv": j + 1 - 2 * d})

    def side_copy(p, k):
        return query_copy(p, k, d_send.at[p, k], d_recv.at[p, k], {"sub": other})

    def side_arrival(p, k):
        return pltpu.make_async_remote_copy(
            src_ref=query_view(p, k, other),
            dst_ref=query_view(p, k, other),
            send_sem=d_send.at[p, k],
            recv_sem=d_recv.at[p, k],
            device_id={"sub": other},
            device_id_type=MESH,
        )

    @pl.when(j < n - 1)
    def _():
        for k in range(kv):
            own_copy(k, 1).start()

    @pl.when(j > 0)
    def _():
        for k in range(kv):
            own_copy(k, 0).start()

    def swap_copies(p, k):
        return tuple(
            pltpu.make_async_remote_copy(
                src_ref=src.at[p, other, k],
                dst_ref=dst.at[p, k],
                send_sem=swap_send.at[index, p, k],
                recv_sem=swap_recv.at[index, p, k],
                device_id={"sub": other},
                device_id_type=MESH,
            )
            for index, (src, dst) in enumerate(((part_o, swap_o), (part_e, swap_e)))
        )

    def chain_copies(p, k, d, target=None):
        target = {"kv": j + 2 * d - 1} if target is None else target
        return tuple(
            pltpu.make_async_remote_copy(
                src_ref=src.at[p, k],
                dst_ref=dst.at[d, p, k],
                send_sem=chain_send.at[index, p, k],
                recv_sem=chain_recv.at[index, d, p, k],
                device_id=target,
                device_id_type=MESH,
            )
            for index, (src, dst) in enumerate(((send_o, chain_o), (send_e, chain_e)))
        )

    def fin_copies(k):
        return tuple(
            pltpu.make_async_remote_copy(
                src_ref=buf.at[s, k],
                dst_ref=buf.at[s, k],
                send_sem=fin_send.at[index, k],
                recv_sem=fin_recv.at[index, k],
                device_id={"sub": other},
                device_id_type=MESH,
            )
            for index, buf in enumerate((fin_o, fin_e))
        )

    def fin_arrivals(k):
        return tuple(
            pltpu.make_async_remote_copy(
                src_ref=buf.at[other, k],
                dst_ref=buf.at[other, k],
                send_sem=fin_send.at[index, k],
                recv_sem=fin_recv.at[index, k],
                device_id={"sub": other},
                device_id_type=MESH,
            )
            for index, buf in enumerate((fin_o, fin_e))
        )

    def attend(keys, values, query):
        scores = dot(keys, query, NT)
        maxima = jnp.max(scores, axis=0, keepdims=True)
        weights = jnp.exp((scores - maxima) * scale)
        totals = jnp.sum(weights, axis=0, keepdims=True)
        return maxima * scale, totals, dot(values, weights.astype(BF16), TN)

    def block(p, d):
        def arrive(k):
            @pl.when(jnp.logical_not(beyond(d)))
            def _():
                relay_copy(p, k, d).wait_recv()
                side_copy(p, k).start()

        for k in range(kv):
            if d is not None:
                for later in ([0, 1] if k == 0 else [k + 1]):
                    if later < kv:
                        arrive(later)
                side_arrival(p, k).wait_recv()
            top, total, numerator = attend(sk_ref[k], sv_ref[k], qbuf[p, k])
            system = (numerator * (1.0 / total), top + jnp.log(total))
            picked = qbuf[p, k, pl.ds(pl.multiple_of(j * task_rows, 16), task_rows), :]
            doubled = jnp.concatenate([picked, picked], axis=0)
            tokens = tk.shape[1]
            step = min(512, tokens)
            state = None
            for base in range(0, tokens, step):
                part = attend(
                    tk[k, base : base + step, :], tv[k, base : base + step, :], doubled
                )
                if state is None:
                    state = part
                else:
                    top = jnp.maximum(state[0], part[0])
                    a, b = jnp.exp(state[0] - top), jnp.exp(part[0] - top)
                    state = (top, state[1] * a + part[1] * b, state[2] * a + part[2] * b)
            top, total, numerator = state
            repeats = lanes // (2 * task_rows)
            place = iota((1, lanes), 1) // task_rows == j
            task = (
                jnp.concatenate([numerator * (1.0 / total)] * repeats, axis=1),
                jnp.where(
                    place, jnp.concatenate([top + jnp.log(total)] * repeats, axis=1), NEGATIVE
                ),
            )
            result, level = merge(system, task)
            for h in range(2):
                part_o[p, h, k] = result[:, h * half : (h + 1) * half]
                part_e[p, h, k] = jnp.broadcast_to(level[:, h * half : (h + 1) * half], (8, half))
            for copy in swap_copies(p, k):
                copy.start()

    def chip_part(p, k):
        return merge(
            (part_o[p, s, k], part_e[p, s, k][0:1]), (swap_o[p, k], swap_e[p, k][0:1])
        )

    def chain_part(d, p, k):
        return chain_o[d, p, k].astype(F32), chain_e[d, p, k][0:1]

    def finish(p, d, incoming):
        for k in range(kv):
            for copy in swap_copies(p, k):
                copy.wait_recv()
            state = chip_part(p, k)
            if incoming:
                for copy in chain_copies(p, k, d):
                    copy.wait_recv()
                state = merge(state, chain_part(d, p, k))
            send_o[p, k] = state[0].astype(BF16)
            send_e[p, k] = jnp.broadcast_to(state[1], (8, half))
            for copy in chain_copies(p, k, d):
                copy.start()

    def suffix(i):
        for copy in suffix_copies(i):
            copy.wait()
        query = q_ref[s * own + i].astype(F32)
        length = len_ref[i]
        scores = jnp.concatenate(
            [
                dot(query[k * group : (k + 1) * group].astype(BF16), uk[i, k], NT)
                for k in range(kv)
            ],
            axis=0,
        )
        usable = iota(scores.shape, 1) < length
        scores = jnp.where(usable, scores, NEGATIVE)
        maxima = jnp.max(scores, axis=1, keepdims=True)
        weights = jnp.where(usable, jnp.exp((scores - maxima) * scale), 0.0)
        totals = jnp.sum(weights, axis=1, keepdims=True)
        numerator = jnp.concatenate(
            [
                dot(weights[k * group : (k + 1) * group].astype(BF16), uv[i, k])
                for k in range(kv)
            ],
            axis=0,
        )
        suf_o[i] = numerator * (1.0 / totals)
        suf_e[i] = jnp.broadcast_to(maxima * scale + jnp.log(totals), (heads, width))

    def source(t, d):
        return j + (2 * d - 1) * t

    def valid(t, d):
        p = source(t, d)
        return (p >= 0) & (p < n)

    def beyond(d):
        return jnp.where(d == 0, j < n - 1, j > 0)

    early = own // 4
    late, turns = own - early, 2 * n - 2

    @pl.loop(0, early)
    def _(i):
        suffix(i)

    for copy in task_copies:
        copy.wait()

    @pl.loop(1, n)
    def _(t):
        for k in range(kv):
            for d in range(2):

                @pl.when(valid(t, d) & beyond(d))
                def _(d=d, k=k):
                    p = source(t, d)
                    relay_copy(p, k, d).wait_recv()
                    relay_copy(p, k, d).start()
                    side_copy(p, k).start()

        @pl.loop(0, 2)
        def _(d):
            @pl.when(valid(t, d))
            def _():
                block(source(t, d), d)

        for d in range(2):

            @pl.when(valid(t, d) & jnp.logical_not(beyond(d)))
            def _(d=d):
                finish(source(t, d), d, False)

    block(j, None)

    @pl.loop(1, 2 * n - 1)
    def _(turn):
        @pl.loop(early + (turn - 1) * late // turns, early + turn * late // turns)
        def _(i):
            suffix(i)

        low = 2 * (n - 1) - j - turn

        @pl.when((low >= 0) & (low < j) & (j < n - 1))
        def _():
            finish(low, 0, True)

        high = turn - j

        @pl.when((high > j) & (high < n) & (j > 0))
        def _():
            finish(high, 1, True)

    for k in range(kv):
        for copy in swap_copies(j, k):
            copy.wait_recv()
        value, level = chip_part(j, k)
        fin_o[s, k] = value
        fin_e[s, k] = jnp.broadcast_to(level, (8, half))
    chosen = spread(own, s * own)
    for k in range(kv):
        for d in range(2):

            @pl.when(j < n - 1 if d == 0 else j > 0)
            def _(d=d, k=k):
                for copy in chain_copies(j, k, d, {"kv": j + 1 - 2 * d}):
                    copy.wait_recv()
                state = merge((fin_o[s, k], fin_e[s, k][0:1]), chain_part(d, j, k))
                fin_o[s, k] = state[0]
                fin_e[s, k] = jnp.broadcast_to(state[1], (8, half))

        for copy in fin_copies(k):
            copy.start()
    for k in range(kv):
        for copy in fin_arrivals(k):
            copy.wait_recv()
        value = jnp.concatenate([fin_o[0, k], fin_o[1, k]], axis=1)
        level = jnp.concatenate([fin_e[0, k], fin_e[1, k]], axis=1)
        value = selected(value, chosen, 2).T
        level = jnp.broadcast_to(selected(level, chosen, 3)[0:1], (width, own * group)).T
        near = slice(k * group, (k + 1) * group)
        suffix_state = (
            suf_o[:, near, :].reshape(own * group, width),
            suf_e[:, near, :].reshape(own * group, width),
        )
        attended = merge((value, level), suffix_state)[0]
        out32[:, near, :] = attended.reshape(own, group, width)
    out_ref[...] = out32[...].astype(BF16)

    for k in range(kv):

        @pl.when(j < n - 1)
        def _(k=k):
            own_copy(k, 1).wait_send()

        @pl.when(j > 0)
        def _(k=k):
            own_copy(k, 0).wait_send()

        for copy in swap_copies(j, k) + fin_copies(k):
            copy.wait_send()

    @pl.loop(1, n)
    def _(t):
        for d in range(2):

            @pl.when(valid(t, d))
            def _(d=d):
                p = source(t, d)
                for k in range(kv):

                    @pl.when(beyond(d))
                    def _(k=k):
                        relay_copy(p, k, d).wait_send()

                    side_copy(p, k).wait_send()
                    for copy in swap_copies(p, k) + chain_copies(p, k, d):
                        copy.wait_send()


def exp2(x):
    return jnp.exp2(x)


def blend(parts):
    top = parts[0][1]
    for part in parts[1:]:
        top = jnp.maximum(top, part[1])
    factors = [exp2(part[1] - top) for part in parts]
    total = sum(factors[1:], factors[0])
    inverse = 1.0 / total
    value = parts[0][0] * (factors[0] * inverse)
    for part, factor in zip(parts[1:], factors[1:]):
        value = value + part[0] * (factor * inverse)
    return value, top + jnp.log2(total)


def paired(
    n,
    q_hbm,
    sk_hbm,
    sv_hbm,
    tk_hbm,
    tv_hbm,
    uk_hbm,
    uv_hbm,
    ids_hbm,
    len_hbm,
    out_hbm,
    qh,
    qo,
    ids_ref,
    len_ref,
    perm,
    qs,
    tq,
    qx,
    sysb,
    taskb,
    uk,
    uv,
    suf_o,
    suf_e,
    sib_o,
    sib_e,
    base_o,
    base_e,
    rs_o,
    rs_e,
    rr_o,
    rr_e,
    ps_o,
    ps_e,
    pr_o,
    pr_e,
    out32,
    outb,
    load_sem,
    sysl_sem,
    task_sem,
    suf_sem,
    tx_send,
    tx_recv,
    sys_send,
    sys_recv,
    q_send,
    q_recv,
    ret_send,
    ret_recv,
    sx_send,
    sx_recv,
    fin_sem,
    fin_send,
    fin_recv,
):
    rows = qh.shape[0]
    own, heads, width = qo.shape
    mine = qh.shape[1]
    kv = uk.shape[1]
    group = heads // kv
    per = kv // 2
    half_n = n // 2
    cell = CAP * group
    lanes = 2 * half_n * cell
    tile = 2 * cell
    shard = sk_hbm.shape[1]
    stretch = tk_hbm.shape[2]
    scale = math.log2(math.e) / math.sqrt(width)
    j = lax.axis_index("kv")
    s = lax.axis_index("sub")
    other = 1 - s
    side = j // half_n
    e = j % half_n
    mate = j + 1 - 2 * e
    far = (1 - side) * half_n

    barrier = pltpu.get_barrier_semaphore()
    pl.semaphore_signal(barrier, inc=1, device_id={"sub": other}, device_id_type=MESH)
    for d in range(1, n):
        target = lax.rem(j + d, n)
        for z in range(2):
            pl.semaphore_signal(
                barrier, inc=1, device_id={"kv": target, "sub": z}, device_id_type=MESH
            )

    def remote(src, dst, send_sem, recv_sem, device):
        return pltpu.make_async_remote_copy(
            src_ref=src,
            dst_ref=dst,
            send_sem=send_sem,
            recv_sem=recv_sem,
            device_id=device,
            device_id_type=MESH,
        )

    first = pl.multiple_of(s * mine, 16)
    loads = [
        pltpu.make_async_copy(ids_hbm, ids_ref, load_sem.at[0]),
        pltpu.make_async_copy(q_hbm.at[:, pl.ds(first, mine), :], qh, load_sem.at[1]),
        pltpu.make_async_copy(q_hbm.at[pl.ds(s * own, own)], qo, load_sem.at[2]),
        pltpu.make_async_copy(len_hbm, len_ref, load_sem.at[3]),
    ]
    for copy in loads:
        copy.start()

    def spot(chip, core):
        return pl.ds(pl.multiple_of((2 * chip + core) * shard, 128), shard)

    sys_local = [
        pltpu.make_async_copy(
            hbm.at[pl.ds(s * per, per)], sysb.at[kind, :, spot(e, s), :], sysl_sem.at[kind]
        )
        for kind, hbm in enumerate((sk_hbm, sv_hbm))
    ]
    for copy in sys_local:
        copy.start()

    def strip(core):
        return pl.ds(pl.multiple_of(core * stretch, 128), stretch)

    task_local = [
        [
            pltpu.make_async_copy(
                hbm.at[0, s * per + h], taskb.at[kind, h, strip(s), :], task_sem.at[kind, h]
            )
            for kind, hbm in enumerate((tk_hbm, tv_hbm))
        ]
        for h in range(per)
    ]
    for copies in task_local:
        for copy in copies:
            copy.start()

    def suffix_copies(i):
        return (
            pltpu.make_async_copy(uk_hbm.at[i], uk.at[i], suf_sem.at[0, i]),
            pltpu.make_async_copy(uv_hbm.at[i], uv.at[i], suf_sem.at[1, i]),
        )

    @pl.loop(0, own)
    def _(i):
        for copy in suffix_copies(i):
            copy.start()

    loads[0].wait()
    ids = ids_ref[...]
    names = ids.astype(F32)
    wide = jnp.broadcast_to(names, (rows, rows))
    down, across = iota((rows, rows), 0), iota((rows, rows), 1)
    column = jnp.sum(jnp.where(down == across, wide, 0.0), axis=1, keepdims=True)
    same = jnp.where((column == wide) & (down < across), 1.0, 0.0)
    seat = ids % half_n
    seat = jnp.where(ids // half_n == side, half_n - 1 - seat, half_n + seat)
    places = seat.astype(F32) * CAP + jnp.sum(same, axis=0, keepdims=True)
    places8 = jnp.broadcast_to(places, (8, rows)).astype(BF16)
    shape = (rows, rows * group)
    pick = jnp.where(iota(shape, 0) == iota(shape, 1) // group, 1.0, 0.0).astype(BF16)
    row = dot(places8, pick)[0:1].astype(jnp.int32)
    shape = (lanes, rows * group)
    down, across = iota(shape, 0), iota(shape, 1)
    hit = (down // group == row) & (down % group == across % group)
    perm[...] = jnp.where(hit, 1.0, 0.0).astype(BF16)
    loads[1].wait()
    wide_query = qh[...].astype(F32)
    for h in range(per):
        flat = wide_query[:, h * group : (h + 1) * group, :].reshape(rows * group, width)
        qs[h] = dot(perm[...], flat.astype(BF16)).astype(BF16)

    def cellat(base):
        return pl.ds(pl.multiple_of(base, 16), cell)

    for h in range(per):
        tq[h, cellat((1 - e) * cell), :] = qs[h, cellat((1 - e) * cell), :]

    def query_copies(h):
        copies = [
            remote(
                qs.at[h, cellat(e * cell), :],
                tq.at[h, cellat(tile + e * cell), :],
                q_send.at[h, 0],
                q_recv.at[h, 0],
                {"kv": mate},
            )
        ]
        for c in range(2):
            copies.append(
                remote(
                    qs.at[h, cellat(tile + c * cell), :],
                    tq.at[h, cellat(e * tile + c * cell), :],
                    q_send.at[h, 1 + c],
                    q_recv.at[h, 1 + e],
                    {"kv": far + c},
                )
            )
            copies.append(
                remote(
                    qs.at[h, cellat((1 - c) * cell), :],
                    qx.at[h, cellat(e * tile + (1 - c) * cell), :],
                    q_send.at[h, 3 + c],
                    q_recv.at[h, 3 + e],
                    {"kv": far + c},
                )
            )
        return copies

    def query_arrivals(h):
        places = [(tq, tile + (1 - e) * cell)]
        places += [(tq, i * tile + e * cell) for i in range(2)]
        places += [(qx, i * tile + (1 - e) * cell) for i in range(2)]
        return [
            remote(
                buf.at[h, cellat(base), :],
                buf.at[h, cellat(base), :],
                q_send.at[h, index],
                q_recv.at[h, index],
                {"kv": mate},
            )
            for index, (buf, base) in enumerate(places)
        ]

    def sys_copies(h):
        copies = []
        for kind, hbm in enumerate((sk_hbm, sv_hbm)):
            dst = sysb.at[kind, h, spot(e, s), :]
            copies.append(
                remote(
                    hbm.at[other * per + h],
                    dst,
                    sys_send.at[kind, h, 0],
                    sys_recv.at[kind, h, 0],
                    {"sub": other},
                )
            )
            for z in range(2):
                copies.append(
                    remote(
                        hbm.at[z * per + h],
                        dst,
                        sys_send.at[kind, h, 1 + z],
                        sys_recv.at[kind, h, 1 + s],
                        {"kv": mate, "sub": z},
                    )
                )
        return copies

    def sys_arrivals(h):
        out = []
        for kind in range(2):
            for index, (chip, core) in enumerate(((e, other), (1 - e, 0), (1 - e, 1))):
                ref = sysb.at[kind, h, spot(chip, core), :]
                out.append(
                    remote(
                        ref,
                        ref,
                        sys_send.at[kind, h, index],
                        sys_recv.at[kind, h, index],
                        {"sub": other},
                    )
                )
        return out

    def task_copies(h):
        return [
            remote(
                hbm.at[0, other * per + h],
                taskb.at[kind, h, strip(s), :],
                tx_send.at[kind, h],
                tx_recv.at[kind, h],
                {"sub": other},
            )
            for kind, hbm in enumerate((tk_hbm, tv_hbm))
        ]

    def task_arrivals(h):
        return [
            remote(
                taskb.at[kind, h, strip(other), :],
                taskb.at[kind, h, strip(other), :],
                tx_send.at[kind, h],
                tx_recv.at[kind, h],
                {"sub": other},
            )
            for kind in range(2)
        ]

    pl.semaphore_wait(barrier, 2 * n - 1)
    for h in range(per):
        for copy in query_copies(h) + sys_copies(h) + task_copies(h):
            copy.start()

    def suffix(i):
        for copy in suffix_copies(i):
            copy.wait()
        query = qo[i].astype(F32)
        length = len_ref[i]
        scores = jnp.concatenate(
            [
                dot(query[k * group : (k + 1) * group].astype(BF16), uk[i, k], NT)
                for k in range(kv)
            ],
            axis=0,
        )
        usable = iota(scores.shape, 1) < length
        scores = jnp.where(usable, scores, NEGATIVE)
        maxima = jnp.max(scores, axis=1, keepdims=True)
        weights = jnp.where(usable, exp2((scores - maxima) * scale), 0.0)
        totals = jnp.sum(weights, axis=1, keepdims=True)
        numerator = jnp.concatenate(
            [
                dot(weights[k * group : (k + 1) * group].astype(BF16), uv[i, k])
                for k in range(kv)
            ],
            axis=0,
        )
        value = numerator * (1.0 / totals)
        level = jnp.broadcast_to(maxima * scale + jnp.log2(totals), (heads, width))
        for z in range(2):
            suf_o[z, i] = value[z * mine : (z + 1) * mine]
            suf_e[z, i] = level[z * mine : (z + 1) * mine]

    def sweep(pairs, query):
        state = None
        scores = dot(pairs[0][0](), query, NT)
        for index, (_, values) in enumerate(pairs):
            later = dot(pairs[index + 1][0](), query, NT) if index + 1 < len(pairs) else None
            top = jnp.max(scores, axis=0, keepdims=True)
            weights = exp2((scores - top) * scale)
            total = jnp.sum(weights, axis=0, keepdims=True)
            part = (top * scale, total, dot(values(), weights.astype(BF16), TN))
            if state is None:
                state = part
            else:
                top = jnp.maximum(state[0], part[0])
                a, b = exp2(state[0] - top), exp2(part[0] - top)
                state = (top, state[1] * a + part[1] * b, state[2] * a + part[2] * b)
            scores = later
        top, total, numerator = state
        return numerator * (1.0 / total), top + jnp.log2(total)

    def pieces(buf, h, step):
        tokens = buf.shape[2]
        step = min(step, tokens)
        return [
            (
                lambda base=base: buf[0, h, base : base + step, :],
                lambda base=base: buf[1, h, base : base + step, :],
            )
            for base in range(0, tokens, step)
        ]

    zone = iota((1, tile), 1) // cell

    def ret_copies(h, i):
        return [
            remote(
                src.at[h, i],
                dst.at[h, e],
                ret_send.at[index, h, i],
                ret_recv.at[index, h, e],
                {"kv": far + i},
            )
            for index, (src, dst) in enumerate(((rs_o, rr_o), (rs_e, rr_e)))
        ]

    def ret_arrivals(h, i):
        return [
            remote(
                dst.at[h, i],
                dst.at[h, i],
                ret_send.at[index, h, i],
                ret_recv.at[index, h, i],
                {"kv": far + i},
            )
            for index, dst in enumerate((rr_o, rr_e))
        ]

    def mate_copies(h):
        return [
            remote(
                src.at[h],
                dst.at[h],
                ret_send.at[index, h, 2],
                ret_recv.at[index, h, 2],
                {"kv": mate},
            )
            for index, (src, dst) in enumerate(((ps_o, pr_o), (ps_e, pr_e)))
        ]

    def head(h):
        for copy in task_local[h] + ([] if h else sys_local):
            copy.wait()
        for copy in query_arrivals(h) + task_arrivals(h):
            copy.wait_recv()
        for i in range(2):
            qx[h, cellat(i * tile + e * cell), :] = tq[h, cellat(i * tile + e * cell), :]
        value, level = sweep(pieces(taskb, h, 512), tq[h])
        near = value[:, tile:]
        packed = jnp.where(
            zone == 1 - e,
            near[: width // 2],
            pltpu.roll(near[width // 2 :], cell, 1),
        )
        ps_o[h] = packed.astype(BF16)
        ps_e[h] = jnp.broadcast_to(level[:, tile:], (8, tile))
        for copy in mate_copies(h):
            copy.start()
        for copy in sys_arrivals(h):
            copy.wait_recv()
        cross, cross_level = sweep(pieces(sysb, h, 512), qx[h])
        for i in range(2):
            cut = slice(i * tile, (i + 1) * tile)
            task_level = jnp.where(zone == e, level[:, cut], NEGATIVE)
            merged = blend([(cross[:, cut], cross_level[:, cut]), (value[:, cut], task_level)])
            rs_o[h, i] = merged[0].astype(BF16)
            rs_e[h, i] = jnp.broadcast_to(merged[1], (8, tile))
            for copy in ret_copies(h, i):
                copy.start()
        home, home_level = sweep(pieces(sysb, h, 512), qs[h])
        task_level = jnp.where(zone == 1 - e, level[:, :tile], NEGATIVE)
        merged = blend([(home[:, :tile], home_level[:, :tile]), (value[:, :tile], task_level)])
        base_o[h] = jnp.concatenate([merged[0], home[:, tile:]], axis=1)
        base_e[h] = jnp.broadcast_to(
            jnp.concatenate([merged[1], home_level[:, tile:]], axis=1), (8, lanes)
        )

    def exchange():
        return [
            remote(
                src.at[other],
                dst,
                sx_send.at[index],
                sx_recv.at[index],
                {"sub": other},
            )
            for index, (src, dst) in enumerate(((suf_o, sib_o), (suf_e, sib_e)))
        ]

    def span(core):
        return pl.ds(pl.multiple_of(core * own * group, 128), own * group)

    def fold(h):
        value, level = None, None
        for core, o_ref, e_ref in ((s, suf_o.at[s], suf_e.at[s]), (other, sib_o, sib_e)):
            near = slice(h * group, (h + 1) * group)
            rest = o_ref[:, near, :].reshape(own * group, width)
            tall = e_ref[:, near, :].reshape(own * group, width)
            chosen = perm[:, span(core)]
            for _ in range(2):
                piece = rest.astype(BF16)
                rest = rest - piece.astype(F32)
                term = dot(piece, chosen, (((0,), (1,)), ((), ())))
                value = term if value is None else value + term
            tall = tall.T[0:1]
            term = jnp.sum(jnp.where(chosen.astype(F32) > 0.5, tall, 0.0), axis=1, keepdims=True)
            level = term if level is None else level + term
        level = jnp.broadcast_to(level, (lanes, width)).T[0:1]
        merged = blend([(base_o[h], base_e[h][0:1]), (value, level)])
        base_o[h] = merged[0]
        base_e[h] = jnp.broadcast_to(merged[1], (8, lanes))

    def finish(h):
        for copy in ret_arrivals(h, 0) + ret_arrivals(h, 1) + mate_copies(h):
            copy.wait_recv()
        low = zone == 0
        far_o = [rr_o[h, c].astype(F32) for c in range(2)]
        far_e = [rr_e[h, c][0:1] for c in range(2)]
        crossed = [
            (jnp.where(low, far_o[1], far_o[0]), jnp.where(low, far_e[1], far_e[0])),
            (jnp.where(low, far_o[0], far_o[1]), jnp.where(low, far_e[0], far_e[1])),
        ]
        packed = pr_o[h].astype(F32)
        near = jnp.concatenate([packed, pltpu.roll(packed, cell, 1)], axis=0)
        near_level = jnp.where(zone == e, pr_e[h][0:1], NEGATIVE)
        results = []
        for i in range(2):
            cut = slice(i * tile, (i + 1) * tile)
            parts = [(base_o[h, :, cut], base_e[h, 0:1, cut]), crossed[i]]
            if i == 0:
                parts.append((near, near_level))
            results.append(blend(parts)[0])
        done = jnp.concatenate(results, axis=1).astype(BF16)
        for index, core in enumerate((other, s)):
            chosen = perm[:, span(core)]
            ordered = dot(chosen, done, (((0,), (1,)), ((), ())))
            out32[index, :, h * group : (h + 1) * group, :] = ordered.reshape(own, group, width)

    for copy in loads[2:]:
        copy.wait()
    early = own
    @pl.loop(0, early)
    def _(i):
        suffix(i)

    for copy in exchange():
        copy.start()
    for h in range(per):
        head(h)
    for copy in exchange():
        copy.wait_recv()
    for h in range(per):
        fold(h)
    for h in range(per):
        finish(h)
    outb[0] = out32[0].astype(BF16)
    mine_cut = out_hbm.at[:, pl.ds(first, mine), :]
    give = remote(outb.at[0], mine_cut, fin_send, fin_recv, {"sub": other})
    give.start()
    outb[1] = out32[1].astype(BF16)
    keep = pltpu.make_async_copy(outb.at[1], mine_cut, fin_sem)
    keep.start()

    for h in range(per):
        for copy in query_copies(h) + sys_copies(h) + task_copies(h):
            copy.wait_send()
        for copy in mate_copies(h) + ret_copies(h, 0) + ret_copies(h, 1):
            copy.wait_send()
    for copy in exchange():
        copy.wait_send()
    keep.wait()
    give.wait_send()
    theirs = out_hbm.at[:, pl.ds(pl.multiple_of(other * mine, 16), mine), :]
    remote(outb.at[0], theirs, fin_send, fin_recv, {"sub": other}).wait_recv()


def paired_call(n, args, out_shape):
    queries, sys_keys, _, task_keys, _, suffix_keys, _, task_ids, _ = args
    rows, heads, width = queries.shape
    kv = sys_keys.shape[0]
    group = heads // kv
    own = suffix_keys.shape[0]
    per = kv // 2
    mine = heads // 2
    cell = CAP * group
    tile = 2 * cell
    lanes = n * cell
    anywhere = pl.BlockSpec(memory_space=pl.ANY)
    dma = pltpu.SemaphoreType.DMA
    return pl.pallas_call(
        functools.partial(paired, n),
        out_shape=out_shape,
        in_specs=[anywhere] * 9,
        out_specs=anywhere,
        scratch_shapes=[
            pltpu.VMEM((rows, mine, width), BF16),
            pltpu.VMEM((own, heads, width), BF16),
            pltpu.VMEM((1, rows), jnp.int32),
            pltpu.SMEM((own,), jnp.int32),
            pltpu.VMEM((lanes, rows * group), BF16),
            pltpu.VMEM((per, lanes, width), BF16),
            pltpu.VMEM((per, lanes, width), BF16),
            pltpu.VMEM((per, lanes, width), BF16),
            pltpu.VMEM((2, per, n * sys_keys.shape[1], width), BF16),
            pltpu.VMEM((2, per, 2 * task_keys.shape[2], width), BF16),
            pltpu.VMEM(suffix_keys.shape, BF16),
            pltpu.VMEM(suffix_keys.shape, BF16),
            pltpu.VMEM((2, own, mine, width), F32),
            pltpu.VMEM((2, own, mine, width), F32),
            pltpu.VMEM((own, mine, width), F32),
            pltpu.VMEM((own, mine, width), F32),
            pltpu.VMEM((per, width, lanes), F32),
            pltpu.VMEM((per, 8, lanes), F32),
            pltpu.VMEM((per, 2, width, tile), BF16),
            pltpu.VMEM((per, 2, 8, tile), F32),
            pltpu.VMEM((per, 2, width, tile), BF16),
            pltpu.VMEM((per, 2, 8, tile), F32),
            pltpu.VMEM((per, width // 2, tile), BF16),
            pltpu.VMEM((per, 8, tile), F32),
            pltpu.VMEM((per, width // 2, tile), BF16),
            pltpu.VMEM((per, 8, tile), F32),
            pltpu.VMEM((2, own, mine, width), F32),
            pltpu.VMEM((2, own, mine, width), BF16),
            dma((4,)),
            dma((2,)),
            dma((2, per)),
            dma((2, own)),
            dma((2, per)),
            dma((2, per)),
            dma((2, per, 3)),
            dma((2, per, 3)),
            dma((per, 5)),
            dma((per, 5)),
            dma((2, per, 3)),
            dma((2, per, 3)),
            dma((2,)),
            dma((2,)),
            dma,
            dma,
            dma,
        ],
        compiler_params=pltpu.CompilerParams(
            collective_id=0, has_side_effects=True, vmem_limit_bytes=60 * 1024 * 1024
        ),
        name="cascade",
    )(*args[:7], task_ids.reshape(1, rows), args[8])


def body(
    queries,
    sys_keys,
    sys_values,
    task_keys,
    task_values,
    suffix_keys,
    suffix_values,
    task_ids,
    suffix_len,
):
    n = lax.axis_size("kv")
    rows, heads, width = queries.shape
    kv = sys_keys.shape[0]
    group = heads // kv
    own = suffix_keys.shape[0]
    lanes = n * CAP * group
    half = lanes // 2
    out_shape = jax.ShapeDtypeStruct((own, heads, width), BF16)
    if n == 4 and rows == n * CAP and kv % 2 == 0 and 2 * CAP * group == width:
        args = (
            queries,
            sys_keys,
            sys_values,
            task_keys,
            task_values,
            suffix_keys,
            suffix_values,
            task_ids,
            suffix_len,
        )
        return paired_call(n, args, out_shape)
    vmem = pl.BlockSpec(memory_space=pltpu.VMEM)
    anywhere = pl.BlockSpec(memory_space=pl.ANY)
    dma = pltpu.SemaphoreType.DMA
    return pl.pallas_call(
        functools.partial(kernel, n),
        out_shape=out_shape,
        in_specs=[vmem] * 3 + [anywhere] * 4 + [vmem, pl.BlockSpec(memory_space=pltpu.SMEM)],
        out_specs=vmem,
        scratch_shapes=[
            pltpu.VMEM(task_keys.shape[1:], BF16),
            pltpu.VMEM(task_values.shape[1:], BF16),
            pltpu.VMEM(suffix_keys.shape, BF16),
            pltpu.VMEM(suffix_values.shape, BF16),
            pltpu.VMEM((n, kv, lanes, width), BF16),
            pltpu.VMEM((n, 2, kv, width, half), F32),
            pltpu.VMEM((n, 2, kv, 8, half), F32),
            pltpu.VMEM((n, kv, width, half), F32),
            pltpu.VMEM((n, kv, 8, half), F32),
            pltpu.VMEM((n, kv, width, half), BF16),
            pltpu.VMEM((n, kv, 8, half), F32),
            pltpu.VMEM((2, n, kv, width, half), BF16),
            pltpu.VMEM((2, n, kv, 8, half), F32),
            pltpu.VMEM((2, kv, width, half), F32),
            pltpu.VMEM((2, kv, 8, half), F32),
            pltpu.VMEM((own, heads, width), F32),
            pltpu.VMEM((own, heads, width), F32),
            pltpu.VMEM((own, heads, width), F32),
            dma((2,)),
            dma((2, own)),
            dma((2, kv)),
            dma((n, kv)),
            dma((n, kv)),
            dma((n, kv)),
            dma((n, kv)),
            dma((2, n, kv)),
            dma((2, n, kv)),
            dma((2, n, kv)),
            dma((2, 2, n, kv)),
            dma((2, kv)),
            dma((2, kv)),
        ],
        compiler_params=pltpu.CompilerParams(
            collective_id=0, has_side_effects=True, vmem_limit_bytes=60 * 1024 * 1024
        ),
        name="cascade",
    )(
        queries,
        sys_keys,
        sys_values,
        task_keys,
        task_values,
        suffix_keys,
        suffix_values,
        task_ids.reshape(1, rows),
        suffix_len,
    )


def solution(mesh):
    in_specs = (
        P(("replica", "kv"), "head", None),
        P(("replica", "head"), ("kv", "sub"), None),
        P(("replica", "head"), ("kv", "sub"), None),
        P(("replica", "kv"), "head", "sub", None),
        P(("replica", "kv"), "head", "sub", None),
        P(("replica", "kv", "sub"), "head", None, None),
        P(("replica", "kv", "sub"), "head", None, None),
        P(("replica", "kv")),
        P(("replica", "kv", "sub")),
    )
    out_specs = P(("replica", "kv", "sub"), "head", None)
    return jax.shard_map(body, mesh=mesh, in_specs=in_specs, out_specs=out_specs, check_vma=False)
```

```python
import functools
import math

import jax
import jax.numpy as jnp
from jax import lax
from jax.experimental import pallas as pl
from jax.experimental.pallas import tpu as pltpu
from jax.sharding import PartitionSpec as P

CAP = 8
NEGATIVE = -1e30
MESH = pl.DeviceIdType.MESH
NT = (((1,), (1,)), ((), ()))
TN = (((0,), (0,)), ((), ()))
F32 = jnp.float32
BF16 = jnp.bfloat16


def dot(a, b, dims=(((1,), (0,)), ((), ()))):
    return lax.dot_general(a, b, dims, preferred_element_type=F32)


def merge(first, second):
    top = jnp.maximum(first[1], second[1])
    a = jnp.exp(first[1] - top)
    b = jnp.exp(second[1] - top)
    total = a + b
    inverse = 1.0 / total
    return first[0] * (a * inverse) + second[0] * (b * inverse), top + jnp.log(total)


def iota(shape, dim):
    return lax.broadcasted_iota(jnp.int32, shape, dim)


def selected(value, picks, pieces):
    out = None
    for _ in range(pieces):
        part = value.astype(BF16)
        value = value - part.astype(F32)
        term = dot(part, picks)
        out = term if out is None else out + term
    return out


def kernel(
    n,
    q_ref,
    sk_ref,
    sv_ref,
    tk_hbm,
    tv_hbm,
    uk_hbm,
    uv_hbm,
    ids_ref,
    len_ref,
    out_ref,
    tk,
    tv,
    uk,
    uv,
    qbuf,
    part_o,
    part_e,
    swap_o,
    swap_e,
    send_o,
    send_e,
    chain_o,
    chain_e,
    fin_o,
    fin_e,
    suf_o,
    suf_e,
    out32,
    task_sem,
    suf_sem,
    own_send,
    z_send,
    z_recv,
    d_send,
    d_recv,
    swap_send,
    swap_recv,
    chain_send,
    chain_recv,
    fin_send,
    fin_recv,
):
    rows, heads, width = q_ref.shape
    kv = sk_ref.shape[0]
    group = heads // kv
    own = uk.shape[0]
    lanes = qbuf.shape[2]
    half = lanes // 2
    task_rows = CAP * group
    scale = 1.0 / math.sqrt(width)
    j = lax.axis_index("kv")
    s = lax.axis_index("sub")
    other = 1 - s

    task_copies = []
    for index, (hbm, buf) in enumerate(((tk_hbm, tk), (tv_hbm, tv))):
        copy = pltpu.make_async_copy(hbm.at[0], buf, task_sem.at[index])
        copy.start()
        task_copies.append(copy)

    def suffix_copies(i):
        return (
            pltpu.make_async_copy(uk_hbm.at[i], uk.at[i], suf_sem.at[0, i]),
            pltpu.make_async_copy(uv_hbm.at[i], uv.at[i], suf_sem.at[1, i]),
        )

    @pl.loop(0, own)
    def _(i):
        for copy in suffix_copies(i):
            copy.start()

    barrier = pltpu.get_barrier_semaphore()
    pl.semaphore_signal(barrier, inc=1, device_id={"sub": other}, device_id_type=MESH)

    @pl.when(j > 0)
    def _():
        pl.semaphore_signal(barrier, inc=1, device_id={"kv": j - 1}, device_id_type=MESH)

    @pl.when(j < n - 1)
    def _():
        pl.semaphore_signal(barrier, inc=1, device_id={"kv": j + 1}, device_id_type=MESH)

    ids = ids_ref[...].astype(F32)
    wide = jnp.broadcast_to(ids, (rows, rows))
    down, across = iota((rows, rows), 0), iota((rows, rows), 1)
    ids_column = jnp.sum(jnp.where(down == across, wide, 0.0), axis=1, keepdims=True)
    same = jnp.where((ids_column == wide) & (down < across), 1.0, 0.0)
    places = ids * CAP + jnp.sum(same, axis=0, keepdims=True)
    places8 = jnp.broadcast_to(places, (8, rows)).astype(BF16)

    def spread(count, base):
        shape = (rows, count * group)
        pick = jnp.where(iota(shape, 0) == base + iota(shape, 1) // group, 1.0, 0.0).astype(BF16)
        row = dot(places8, pick)[0:1].astype(jnp.int32)
        shape = (lanes, count * group)
        down, across = iota(shape, 0), iota(shape, 1)
        hit = (down // group == row) & (down % group == across % group)
        return jnp.where(hit, 1.0, 0.0).astype(BF16)

    everyone = spread(rows, 0)
    wide_query = q_ref[...].astype(F32)
    for k in range(kv):
        mine = wide_query[:, k * group : (k + 1) * group, :].reshape(rows * group, width)
        qbuf[j, k] = dot(everyone, mine.astype(BF16)).astype(BF16)

    pl.semaphore_wait(
        barrier, 1 + jnp.where(j > 0, 1, 0) + jnp.where(j < n - 1, 1, 0)
    )

    def query_view(p, k, h):
        return qbuf.at[p, k, pl.ds(pl.multiple_of(h * half, 16), half), :]

    def query_copy(p, k, send_sem, recv_sem, device):
        return pltpu.make_async_remote_copy(
            src_ref=query_view(p, k, s),
            dst_ref=query_view(p, k, s),
            send_sem=send_sem,
            recv_sem=recv_sem,
            device_id=device,
            device_id_type=MESH,
        )

    def own_copy(k, d):
        return query_copy(j, k, own_send.at[d, k], z_recv.at[j, k], {"kv": j + 2 * d - 1})

    def relay_copy(p, k, d):
        return query_copy(p, k, z_send.at[p, k], z_recv.at[p, k], {"kv": j + 1 - 2 * d})

    def side_copy(p, k):
        return query_copy(p, k, d_send.at[p, k], d_recv.at[p, k], {"sub": other})

    def side_arrival(p, k):
        return pltpu.make_async_remote_copy(
            src_ref=query_view(p, k, other),
            dst_ref=query_view(p, k, other),
            send_sem=d_send.at[p, k],
            recv_sem=d_recv.at[p, k],
            device_id={"sub": other},
            device_id_type=MESH,
        )

    @pl.when(j < n - 1)
    def _():
        for k in range(kv):
            own_copy(k, 1).start()

    @pl.when(j > 0)
    def _():
        for k in range(kv):
            own_copy(k, 0).start()

    def swap_copies(p, k):
        return tuple(
            pltpu.make_async_remote_copy(
                src_ref=src.at[p, other, k],
                dst_ref=dst.at[p, k],
                send_sem=swap_send.at[index, p, k],
                recv_sem=swap_recv.at[index, p, k],
                device_id={"sub": other},
                device_id_type=MESH,
            )
            for index, (src, dst) in enumerate(((part_o, swap_o), (part_e, swap_e)))
        )

    def chain_copies(p, k, d, target=None):
        target = {"kv": j + 2 * d - 1} if target is None else target
        return tuple(
            pltpu.make_async_remote_copy(
                src_ref=src.at[p, k],
                dst_ref=dst.at[d, p, k],
                send_sem=chain_send.at[index, p, k],
                recv_sem=chain_recv.at[index, d, p, k],
                device_id=target,
                device_id_type=MESH,
            )
            for index, (src, dst) in enumerate(((send_o, chain_o), (send_e, chain_e)))
        )

    def fin_copies(k):
        return tuple(
            pltpu.make_async_remote_copy(
                src_ref=buf.at[s, k],
                dst_ref=buf.at[s, k],
                send_sem=fin_send.at[index, k],
                recv_sem=fin_recv.at[index, k],
                device_id={"sub": other},
                device_id_type=MESH,
            )
            for index, buf in enumerate((fin_o, fin_e))
        )

    def fin_arrivals(k):
        return tuple(
            pltpu.make_async_remote_copy(
                src_ref=buf.at[other, k],
                dst_ref=buf.at[other, k],
                send_sem=fin_send.at[index, k],
                recv_sem=fin_recv.at[index, k],
                device_id={"sub": other},
                device_id_type=MESH,
            )
            for index, buf in enumerate((fin_o, fin_e))
        )

    def attend(keys, values, query):
        scores = dot(keys, query, NT)
        maxima = jnp.max(scores, axis=0, keepdims=True)
        weights = jnp.exp((scores - maxima) * scale)
        totals = jnp.sum(weights, axis=0, keepdims=True)
        return maxima * scale, totals, dot(values, weights.astype(BF16), TN)

    def block(p, d):
        def arrive(k):
            @pl.when(jnp.logical_not(beyond(d)))
            def _():
                relay_copy(p, k, d).wait_recv()
                side_copy(p, k).start()

        for k in range(kv):
            if d is not None:
                for later in ([0, 1] if k == 0 else [k + 1]):
                    if later < kv:
                        arrive(later)
                side_arrival(p, k).wait_recv()
            top, total, numerator = attend(sk_ref[k], sv_ref[k], qbuf[p, k])
            system = (numerator * (1.0 / total), top + jnp.log(total))
            picked = qbuf[p, k, pl.ds(pl.multiple_of(j * task_rows, 16), task_rows), :]
            doubled = jnp.concatenate([picked, picked], axis=0)
            tokens = tk.shape[1]
            step = min(512, tokens)
            state = None
            for base in range(0, tokens, step):
                part = attend(
                    tk[k, base : base + step, :], tv[k, base : base + step, :], doubled
                )
                if state is None:
                    state = part
                else:
                    top = jnp.maximum(state[0], part[0])
                    a, b = jnp.exp(state[0] - top), jnp.exp(part[0] - top)
                    state = (top, state[1] * a + part[1] * b, state[2] * a + part[2] * b)
            top, total, numerator = state
            repeats = lanes // (2 * task_rows)
            place = iota((1, lanes), 1) // task_rows == j
            task = (
                jnp.concatenate([numerator * (1.0 / total)] * repeats, axis=1),
                jnp.where(
                    place, jnp.concatenate([top + jnp.log(total)] * repeats, axis=1), NEGATIVE
                ),
            )
            result, level = merge(system, task)
            for h in range(2):
                part_o[p, h, k] = result[:, h * half : (h + 1) * half]
                part_e[p, h, k] = jnp.broadcast_to(level[:, h * half : (h + 1) * half], (8, half))
            for copy in swap_copies(p, k):
                copy.start()

    def chip_part(p, k):
        return merge(
            (part_o[p, s, k], part_e[p, s, k][0:1]), (swap_o[p, k], swap_e[p, k][0:1])
        )

    def chain_part(d, p, k):
        return chain_o[d, p, k].astype(F32), chain_e[d, p, k][0:1]

    def finish(p, d, incoming):
        for k in range(kv):
            for copy in swap_copies(p, k):
                copy.wait_recv()
            state = chip_part(p, k)
            if incoming:
                for copy in chain_copies(p, k, d):
                    copy.wait_recv()
                state = merge(state, chain_part(d, p, k))
            send_o[p, k] = state[0].astype(BF16)
            send_e[p, k] = jnp.broadcast_to(state[1], (8, half))
            for copy in chain_copies(p, k, d):
                copy.start()

    def suffix(i):
        for copy in suffix_copies(i):
            copy.wait()
        query = q_ref[s * own + i].astype(F32)
        length = len_ref[i]
        scores = jnp.concatenate(
            [
                dot(query[k * group : (k + 1) * group].astype(BF16), uk[i, k], NT)
                for k in range(kv)
            ],
            axis=0,
        )
        usable = iota(scores.shape, 1) < length
        scores = jnp.where(usable, scores, NEGATIVE)
        maxima = jnp.max(scores, axis=1, keepdims=True)
        weights = jnp.where(usable, jnp.exp((scores - maxima) * scale), 0.0)
        totals = jnp.sum(weights, axis=1, keepdims=True)
        numerator = jnp.concatenate(
            [
                dot(weights[k * group : (k + 1) * group].astype(BF16), uv[i, k])
                for k in range(kv)
            ],
            axis=0,
        )
        suf_o[i] = numerator * (1.0 / totals)
        suf_e[i] = jnp.broadcast_to(maxima * scale + jnp.log(totals), (heads, width))

    def source(t, d):
        return j + (2 * d - 1) * t

    def valid(t, d):
        p = source(t, d)
        return (p >= 0) & (p < n)

    def beyond(d):
        return jnp.where(d == 0, j < n - 1, j > 0)

    early = own // 4
    late, turns = own - early, 2 * n - 2

    @pl.loop(0, early)
    def _(i):
        suffix(i)

    for copy in task_copies:
        copy.wait()

    @pl.loop(1, n)
    def _(t):
        for k in range(kv):
            for d in range(2):

                @pl.when(valid(t, d) & beyond(d))
                def _(d=d, k=k):
                    p = source(t, d)
                    relay_copy(p, k, d).wait_recv()
                    relay_copy(p, k, d).start()
                    side_copy(p, k).start()

        @pl.loop(0, 2)
        def _(d):
            @pl.when(valid(t, d))
            def _():
                block(source(t, d), d)

        for d in range(2):

            @pl.when(valid(t, d) & jnp.logical_not(beyond(d)))
            def _(d=d):
                finish(source(t, d), d, False)

    block(j, None)

    @pl.loop(1, 2 * n - 1)
    def _(turn):
        @pl.loop(early + (turn - 1) * late // turns, early + turn * late // turns)
        def _(i):
            suffix(i)

        low = 2 * (n - 1) - j - turn

        @pl.when((low >= 0) & (low < j) & (j < n - 1))
        def _():
            finish(low, 0, True)

        high = turn - j

        @pl.when((high > j) & (high < n) & (j > 0))
        def _():
            finish(high, 1, True)

    for k in range(kv):
        for copy in swap_copies(j, k):
            copy.wait_recv()
        value, level = chip_part(j, k)
        fin_o[s, k] = value
        fin_e[s, k] = jnp.broadcast_to(level, (8, half))
    chosen = spread(own, s * own)
    for k in range(kv):
        for d in range(2):

            @pl.when(j < n - 1 if d == 0 else j > 0)
            def _(d=d, k=k):
                for copy in chain_copies(j, k, d, {"kv": j + 1 - 2 * d}):
                    copy.wait_recv()
                state = merge((fin_o[s, k], fin_e[s, k][0:1]), chain_part(d, j, k))
                fin_o[s, k] = state[0]
                fin_e[s, k] = jnp.broadcast_to(state[1], (8, half))

        for copy in fin_copies(k):
            copy.start()
    for k in range(kv):
        for copy in fin_arrivals(k):
            copy.wait_recv()
        value = jnp.concatenate([fin_o[0, k], fin_o[1, k]], axis=1)
        level = jnp.concatenate([fin_e[0, k], fin_e[1, k]], axis=1)
        value = selected(value, chosen, 2).T
        level = jnp.broadcast_to(selected(level, chosen, 3)[0:1], (width, own * group)).T
        near = slice(k * group, (k + 1) * group)
        suffix_state = (
            suf_o[:, near, :].reshape(own * group, width),
            suf_e[:, near, :].reshape(own * group, width),
        )
        attended = merge((value, level), suffix_state)[0]
        out32[:, near, :] = attended.reshape(own, group, width)
    out_ref[...] = out32[...].astype(BF16)

    for k in range(kv):

        @pl.when(j < n - 1)
        def _(k=k):
            own_copy(k, 1).wait_send()

        @pl.when(j > 0)
        def _(k=k):
            own_copy(k, 0).wait_send()

        for copy in swap_copies(j, k) + fin_copies(k):
            copy.wait_send()

    @pl.loop(1, n)
    def _(t):
        for d in range(2):

            @pl.when(valid(t, d))
            def _(d=d):
                p = source(t, d)
                for k in range(kv):

                    @pl.when(beyond(d))
                    def _(k=k):
                        relay_copy(p, k, d).wait_send()

                    side_copy(p, k).wait_send()
                    for copy in swap_copies(p, k) + chain_copies(p, k, d):
                        copy.wait_send()


exp2 = jnp.exp2
scope = jax.named_scope


def blend(parts):
    top = parts[0][1]
    for part in parts[1:]:
        top = jnp.maximum(top, part[1])
    factors = [exp2(part[1] - top) for part in parts]
    total = sum(factors[1:], factors[0])
    inverse = 1.0 / total
    value = parts[0][0] * (factors[0] * inverse)
    for part, factor in zip(parts[1:], factors[1:]):
        value = value + part[0] * (factor * inverse)
    return value, top + jnp.log2(total)


def paired(
    n,
    q_hbm,
    sk_hbm,
    sv_hbm,
    tk_hbm,
    tv_hbm,
    uk_hbm,
    uv_hbm,
    ids_hbm,
    len_hbm,
    out_hbm,
    qh,
    qo,
    ids_ref,
    len_ref,
    perm,
    qs,
    tq,
    qx,
    sysb,
    taskb,
    uk,
    uv,
    suf_o,
    suf_e,
    sib_o,
    sib_e,
    base_o,
    base_e,
    rs_o,
    rs_e,
    rr_o,
    rr_e,
    ps_o,
    ps_e,
    pr_o,
    pr_e,
    out32,
    outb,
    load_sem,
    sysl_sem,
    task_sem,
    suf_sem,
    tx_send,
    tx_recv,
    sys_send,
    sys_recv,
    q_send,
    q_recv,
    ret_send,
    ret_recv,
    sx_send,
    sx_recv,
    fin_sem,
    fin_send,
    fin_recv,
):
    rows = qh.shape[0]
    own, heads, width = qo.shape
    mine = qh.shape[1]
    kv = uk.shape[1]
    group = heads // kv
    per = kv // 2
    half_n = n // 2
    cell = CAP * group
    lanes = 2 * half_n * cell
    tile = 2 * cell
    shard = sk_hbm.shape[1]
    stretch = tk_hbm.shape[2]
    scale = math.log2(math.e) / math.sqrt(width)
    j = lax.axis_index("kv")
    s = lax.axis_index("sub")
    other = 1 - s
    side = j // half_n
    e = j % half_n
    mate = j + 1 - 2 * e
    far = (1 - side) * half_n

    barrier = pltpu.get_barrier_semaphore()
    pl.semaphore_signal(barrier, inc=1, device_id={"sub": other}, device_id_type=MESH)
    for d in range(1, n):
        target = lax.rem(j + d, n)
        for z in range(2):
            pl.semaphore_signal(
                barrier, inc=1, device_id={"kv": target, "sub": z}, device_id_type=MESH
            )

    def remote(src, dst, send_sem, recv_sem, device):
        return pltpu.make_async_remote_copy(
            src_ref=src,
            dst_ref=dst,
            send_sem=send_sem,
            recv_sem=recv_sem,
            device_id=device,
            device_id_type=MESH,
        )

    first = pl.multiple_of(s * mine, 16)
    loads = [
        pltpu.make_async_copy(ids_hbm, ids_ref, load_sem.at[0]),
        pltpu.make_async_copy(q_hbm.at[:, pl.ds(first, mine), :], qh, load_sem.at[1]),
        pltpu.make_async_copy(q_hbm.at[pl.ds(s * own, own)], qo, load_sem.at[2]),
        pltpu.make_async_copy(len_hbm, len_ref, load_sem.at[3]),
    ]
    for copy in loads:
        copy.start()

    def spot(chip, core):
        return pl.ds(pl.multiple_of((2 * chip + core) * shard, 128), shard)

    sys_local = [
        pltpu.make_async_copy(
            hbm.at[pl.ds(s * per, per)], sysb.at[kind, :, spot(e, s), :], sysl_sem.at[kind]
        )
        for kind, hbm in enumerate((sk_hbm, sv_hbm))
    ]
    for copy in sys_local:
        copy.start()

    def strip(core):
        return pl.ds(pl.multiple_of(core * stretch, 128), stretch)

    task_local = [
        [
            pltpu.make_async_copy(
                hbm.at[0, s * per + h], taskb.at[kind, h, strip(s), :], task_sem.at[kind, h]
            )
            for kind, hbm in enumerate((tk_hbm, tv_hbm))
        ]
        for h in range(per)
    ]
    def suffix_copies(i):
        return (
            pltpu.make_async_copy(uk_hbm.at[i], uk.at[i], suf_sem.at[0, i]),
            pltpu.make_async_copy(uv_hbm.at[i], uv.at[i], suf_sem.at[1, i]),
        )

    def fetch(low, high):
        @pl.loop(low, high)
        def _(i):
            for copy in suffix_copies(i):
                copy.start()

    fetch(0, own // 4)
    for copies in task_local:
        for copy in copies:
            copy.start()
    fetch(own // 4, own)

    with scope("ids"):
        loads[0].wait()
    ids = ids_ref[...]
    names = ids.astype(F32)
    wide = jnp.broadcast_to(names, (rows, rows))
    down, across = iota((rows, rows), 0), iota((rows, rows), 1)
    column = jnp.sum(jnp.where(down == across, wide, 0.0), axis=1, keepdims=True)
    same = jnp.where((column == wide) & (down < across), 1.0, 0.0)
    seat = ids % half_n
    seat = jnp.where(ids // half_n == side, half_n - 1 - seat, half_n + seat)
    places = seat.astype(F32) * CAP + jnp.sum(same, axis=0, keepdims=True)
    places8 = jnp.broadcast_to(places, (8, rows)).astype(BF16)
    shape = (rows, rows * group)
    pick = jnp.where(iota(shape, 0) == iota(shape, 1) // group, 1.0, 0.0).astype(BF16)
    row = dot(places8, pick)[0:1].astype(jnp.int32)
    shape = (lanes, rows * group)
    down, across = iota(shape, 0), iota(shape, 1)
    hit = (down // group == row) & (down % group == across % group)
    perm[...] = jnp.where(hit, 1.0, 0.0).astype(BF16)
    loads[1].wait()
    wide_query = qh[...].astype(F32)
    for h in range(per):
        flat = wide_query[:, h * group : (h + 1) * group, :].reshape(rows * group, width)
        qs[h] = dot(perm[...], flat.astype(BF16)).astype(BF16)

    def cellat(base):
        return pl.ds(pl.multiple_of(base, 16), cell)

    for h in range(per):
        tq[h, cellat((1 - e) * cell), :] = qs[h, cellat((1 - e) * cell), :]

    def query_copies(h):
        copies = [
            remote(
                qs.at[h, cellat(e * cell), :],
                tq.at[h, cellat(tile + e * cell), :],
                q_send.at[h, 0],
                q_recv.at[h, 0],
                {"kv": mate},
            )
        ]
        for c in range(2):
            copies.append(
                remote(
                    qs.at[h, cellat(tile + c * cell), :],
                    tq.at[h, cellat(e * tile + c * cell), :],
                    q_send.at[h, 1 + c],
                    q_recv.at[h, 1 + e],
                    {"kv": far + c},
                )
            )
            copies.append(
                remote(
                    qs.at[h, cellat((1 - c) * cell), :],
                    qx.at[h, cellat(e * tile + (1 - c) * cell), :],
                    q_send.at[h, 3 + c],
                    q_recv.at[h, 3 + e],
                    {"kv": far + c},
                )
            )
        return copies

    def query_arrivals(h):
        places = [(tq, tile + (1 - e) * cell)]
        places += [(tq, i * tile + e * cell) for i in range(2)]
        places += [(qx, i * tile + (1 - e) * cell) for i in range(2)]
        return [
            remote(
                buf.at[h, cellat(base), :],
                buf.at[h, cellat(base), :],
                q_send.at[h, index],
                q_recv.at[h, index],
                {"kv": mate},
            )
            for index, (buf, base) in enumerate(places)
        ]

    def sys_copies(h):
        copies = []
        for kind, hbm in enumerate((sk_hbm, sv_hbm)):
            dst = sysb.at[kind, h, spot(e, s), :]
            copies.append(
                remote(
                    hbm.at[other * per + h],
                    dst,
                    sys_send.at[kind, h, 0],
                    sys_recv.at[kind, h, 0],
                    {"sub": other},
                )
            )
            for z in range(2):
                copies.append(
                    remote(
                        hbm.at[z * per + h],
                        dst,
                        sys_send.at[kind, h, 1 + z],
                        sys_recv.at[kind, h, 1 + s],
                        {"kv": mate, "sub": z},
                    )
                )
        return copies

    def sys_arrivals(h):
        out = []
        for kind in range(2):
            for index, (chip, core) in enumerate(((e, other), (1 - e, 0), (1 - e, 1))):
                ref = sysb.at[kind, h, spot(chip, core), :]
                out.append(
                    remote(
                        ref,
                        ref,
                        sys_send.at[kind, h, index],
                        sys_recv.at[kind, h, index],
                        {"sub": other},
                    )
                )
        return out

    def task_copies(h):
        return [
            remote(
                hbm.at[0, other * per + h],
                taskb.at[kind, h, strip(s), :],
                tx_send.at[kind, h],
                tx_recv.at[kind, h],
                {"sub": other},
            )
            for kind, hbm in enumerate((tk_hbm, tv_hbm))
        ]

    def task_arrivals(h):
        return [
            remote(
                taskb.at[kind, h, strip(other), :],
                taskb.at[kind, h, strip(other), :],
                tx_send.at[kind, h],
                tx_recv.at[kind, h],
                {"sub": other},
            )
            for kind in range(2)
        ]

    def suffix(base):
        picks = range(4)
        for r in picks:
            for copy in suffix_copies(base + r):
                copy.wait()
        scores = []
        for r in picks:
            query = qo[base + r].astype(F32)
            scores.append(
                jnp.concatenate(
                    [
                        dot(
                            query[k * group : (k + 1) * group].astype(BF16),
                            uk[base + r, k],
                            NT,
                        )
                        for k in range(kv)
                    ],
                    axis=0,
                )
            )
        states = []
        for r in picks:
            usable = iota(scores[r].shape, 1) < len_ref[base + r]
            masked = jnp.where(usable, scores[r], NEGATIVE)
            maxima = jnp.max(masked, axis=1, keepdims=True)
            weights = jnp.where(usable, exp2((masked - maxima) * scale), 0.0)
            states.append((maxima, weights, jnp.sum(weights, axis=1, keepdims=True)))
        for r in picks:
            maxima, weights, totals = states[r]
            numerator = jnp.concatenate(
                [
                    dot(weights[k * group : (k + 1) * group].astype(BF16), uv[base + r, k])
                    for k in range(kv)
                ],
                axis=0,
            )
            value = numerator * (1.0 / totals)
            level = jnp.broadcast_to(maxima * scale + jnp.log2(totals), (heads, width))
            for z in range(2):
                suf_o[z, base + r] = value[z * mine : (z + 1) * mine]
                suf_e[z, base + r] = level[z * mine : (z + 1) * mine]

    def sweep(items):
        states = {}
        ahead = [dot(item[1](), item[3], NT) for item in items[:1]]
        for index, (name, _, values, _) in enumerate(items):
            scores = ahead.pop(0)
            if index + 1 < len(items):
                item = items[index + 1]
                ahead.append(dot(item[1](), item[3], NT))
            top = jnp.max(scores, axis=0, keepdims=True)
            weights = exp2((scores - top) * scale)
            total = jnp.sum(weights, axis=0, keepdims=True)
            part = (top * scale, total, dot(values(), weights.astype(BF16), TN))
            if name in states:
                state = states[name]
                top = jnp.maximum(state[0], part[0])
                a, b = exp2(state[0] - top), exp2(part[0] - top)
                part = (top, state[1] * a + part[1] * b, state[2] * a + part[2] * b)
            states[name] = part
        return {
            name: (numerator * (1.0 / total), top + jnp.log2(total))
            for name, (top, total, numerator) in states.items()
        }

    def pieces(name, buf, h, step, query):
        tokens = buf.shape[2]
        step = min(step, tokens)
        return [
            (
                name,
                lambda base=base: buf[0, h, base : base + step, :],
                lambda base=base: buf[1, h, base : base + step, :],
                query,
            )
            for base in range(0, tokens, step)
        ]

    zone = iota((1, tile), 1) // cell

    slim = (slice(None), pl.ds(0, 1))

    def ret_copies(h, i):
        return [
            remote(
                src.at[h, i, slim[index]],
                dst.at[h, e, slim[index]],
                ret_send.at[index, h, i],
                ret_recv.at[index, h, e],
                {"kv": far + i},
            )
            for index, (src, dst) in enumerate(((rs_o, rr_o), (rs_e, rr_e)))
        ]

    def ret_arrivals(h, i):
        return [
            remote(
                dst.at[h, i, slim[index]],
                dst.at[h, i, slim[index]],
                ret_send.at[index, h, i],
                ret_recv.at[index, h, i],
                {"kv": far + i},
            )
            for index, dst in enumerate((rr_o, rr_e))
        ]

    def mate_copies(h):
        return [
            remote(
                src.at[h, slim[index]],
                dst.at[h, slim[index]],
                ret_send.at[index, h, 2],
                ret_recv.at[index, h, 2],
                {"kv": mate},
            )
            for index, (src, dst) in enumerate(((ps_o, pr_o), (ps_e, pr_e)))
        ]

    def arrive(h):
        with scope("local"):
            for copy in task_local[h]:
                copy.wait()
        with scope("queries"):
            for copy in query_arrivals(h):
                copy.wait_recv()
        with scope("taskwait"):
            for copy in task_arrivals(h):
                copy.wait_recv()

    def system(h):
        with scope("syswait"):
            if h == 0:
                for copy in sys_local:
                    copy.wait()
            for copy in sys_arrivals(h):
                copy.wait_recv()

    def gather(h):
        for i in range(2):
            qx[h, cellat(i * tile + e * cell), :] = tq[h, cellat(i * tile + e * cell), :]

    def task_items(h):
        return pieces("task", taskb, h, 1024, tq[h])

    def cross_items(h):
        return pieces("cross", sysb, h, 1024, qx[h])

    def keep_task(h, found):
        value, level = found
        base_o[h] = value
        base_e[h] = jnp.broadcast_to(level, (8, lanes))
        near = value[:, tile:]
        packed = jnp.where(
            zone == 1 - e,
            near[: width // 2],
            pltpu.roll(near[width // 2 :], cell, 1),
        )
        ps_o[h] = packed.astype(BF16)
        ps_e[h] = jnp.broadcast_to(level[:, tile:], (8, tile))

    def keep_cross(h, found, task):
        value, level = found
        for i in range(2):
            cut = slice(i * tile, (i + 1) * tile)
            task_level = jnp.where(zone == e, task[1][:, cut], NEGATIVE)
            merged = blend([(value[:, cut], level[:, cut]), (task[0][:, cut], task_level)])
            rs_o[h, i] = merged[0].astype(BF16)
            rs_e[h, i] = jnp.broadcast_to(merged[1], (8, tile))

    def home():
        items = []
        for h in range(per):
            items += pieces(h, sysb, h, 1024, qs[h])
        found = sweep(items)
        for h in range(per):
            value, level = found[h]
            task_level = jnp.where(zone == 1 - e, base_e[h, 0:1, :tile], NEGATIVE)
            merged = blend([(value[:, :tile], level[:, :tile]), (base_o[h, :, :tile], task_level)])
            base_o[h] = jnp.concatenate([merged[0], value[:, tile:]], axis=1)
            base_e[h] = jnp.broadcast_to(
                jnp.concatenate([merged[1], level[:, tile:]], axis=1), (8, lanes)
            )

    def exchange():
        return [
            remote(
                src.at[other],
                dst,
                sx_send.at[index],
                sx_recv.at[index],
                {"sub": other},
            )
            for index, (src, dst) in enumerate(((suf_o, sib_o), (suf_e, sib_e)))
        ]

    def span(core):
        return pl.ds(pl.multiple_of(core * own * group, 128), own * group)

    def fold(h):
        value, level = None, None
        for core, o_ref, e_ref in ((s, suf_o.at[s], suf_e.at[s]), (other, sib_o, sib_e)):
            near = slice(h * group, (h + 1) * group)
            rest = o_ref[:, near, :].reshape(own * group, width)
            tall = e_ref[:, near, :].reshape(own * group, width)
            chosen = perm[:, span(core)]
            for _ in range(2):
                piece = rest.astype(BF16)
                rest = rest - piece.astype(F32)
                term = dot(piece, chosen, (((0,), (1,)), ((), ())))
                value = term if value is None else value + term
            tall = tall.T[0:1]
            term = jnp.sum(jnp.where(chosen.astype(F32) > 0.5, tall, 0.0), axis=1, keepdims=True)
            level = term if level is None else level + term
        level = jnp.broadcast_to(level, (lanes, width)).T[0:1]
        merged = blend([(base_o[h], base_e[h][0:1]), (value, level)])
        base_o[h] = merged[0]
        base_e[h] = jnp.broadcast_to(merged[1], (8, lanes))

    def finish(h):
        with scope("retwait"):
            for copy in ret_arrivals(h, 0) + ret_arrivals(h, 1) + mate_copies(h):
                copy.wait_recv()
        low = zone == 0
        far_o = [rr_o[h, c].astype(F32) for c in range(2)]
        far_e = [rr_e[h, c][0:1] for c in range(2)]
        crossed = [
            (jnp.where(low, far_o[1], far_o[0]), jnp.where(low, far_e[1], far_e[0])),
            (jnp.where(low, far_o[0], far_o[1]), jnp.where(low, far_e[0], far_e[1])),
        ]
        packed = pr_o[h].astype(F32)
        near = jnp.concatenate([packed, pltpu.roll(packed, cell, 1)], axis=0)
        near_level = jnp.where(zone == e, pr_e[h][0:1], NEGATIVE)
        results = []
        for i in range(2):
            cut = slice(i * tile, (i + 1) * tile)
            parts = [(base_o[h, :, cut], base_e[h, 0:1, cut]), crossed[i]]
            if i == 0:
                parts.append((near, near_level))
            results.append(blend(parts)[0])
        done = jnp.concatenate(results, axis=1).astype(BF16)
        for index, core in enumerate((other, s)):
            chosen = perm[:, span(core)]
            ordered = dot(chosen, done, (((0,), (1,)), ((), ())))
            out32[index, :, h * group : (h + 1) * group, :] = ordered.reshape(own, group, width)

    for copy in loads[2:]:
        copy.wait()

    def suffixes(low, high):
        with scope("suffix"):

            @pl.loop(low, high)
            def _(i):
                suffix(i * 4)

    ahead = (3 * own * (n - 1 - j)) // (32 * n)
    suffixes(0, ahead)
    with scope("barrier"):
        pl.semaphore_wait(barrier, 2 * n - 1)
    for copy in query_copies(0) + sys_copies(0) + task_copies(0):
        copy.start()
    suffixes(ahead, 2)
    with scope("drain"):
        for copy in query_copies(0):
            copy.wait_send()
    for copy in query_copies(1) + sys_copies(1) + task_copies(1):
        copy.start()
    suffixes(2, own // 4)
    for copy in exchange():
        copy.start()
    arrive(0)
    system(0)
    with scope("block"):
        gather(0)
        found = sweep(task_items(0) + cross_items(0))
        keep_cross(0, found["cross"], found["task"])
        keep_task(0, found["task"])
        for copy in ret_copies(0, 0) + ret_copies(0, 1) + mate_copies(0):
            copy.start()
    arrive(1)
    with scope("task"):
        gather(1)
        keep_task(1, sweep(task_items(1))["task"])
        for copy in mate_copies(1):
            copy.start()
    system(1)
    with scope("cross"):
        task = (base_o[1], base_e[1, 0:1])
        keep_cross(1, sweep(cross_items(1))["cross"], task)
        for copy in ret_copies(1, 0) + ret_copies(1, 1):
            copy.start()
    with scope("home"):
        home()
    with scope("sxwait"):
        for copy in exchange():
            copy.wait_recv()
    with scope("fold"):
        for h in range(per):
            fold(h)
    for h in range(per):
        with scope("finish"):
            finish(h)
    outb[0] = out32[0].astype(BF16)
    mine_cut = out_hbm.at[:, pl.ds(first, mine), :]
    give = remote(outb.at[0], mine_cut, fin_send, fin_recv, {"sub": other})
    give.start()
    outb[1] = out32[1].astype(BF16)
    keep = pltpu.make_async_copy(outb.at[1], mine_cut, fin_sem)
    keep.start()

    for copy in sys_copies(0) + task_copies(0) + query_copies(1) + sys_copies(1) + task_copies(1):
        copy.wait_send()
    for h in range(per):
        for copy in mate_copies(h) + ret_copies(h, 0) + ret_copies(h, 1):
            copy.wait_send()
    for copy in exchange():
        copy.wait_send()
    with scope("tail"):
        keep.wait()
        give.wait_send()
        theirs = out_hbm.at[:, pl.ds(pl.multiple_of(other * mine, 16), mine), :]
        remote(outb.at[0], theirs, fin_send, fin_recv, {"sub": other}).wait_recv()


def paired_call(n, args, out_shape):
    queries, sys_keys, _, task_keys, _, suffix_keys, _, task_ids, _ = args
    rows, heads, width = queries.shape
    kv = sys_keys.shape[0]
    group = heads // kv
    own = suffix_keys.shape[0]
    per = kv // 2
    mine = heads // 2
    cell = CAP * group
    tile = 2 * cell
    lanes = n * cell
    dma = pltpu.SemaphoreType.DMA
    return pl.pallas_call(
        functools.partial(paired, n),
        out_shape=out_shape,
        in_specs=[pl.BlockSpec(memory_space=pl.ANY)] * 9,
        out_specs=pl.BlockSpec(memory_space=pl.ANY),
        scratch_shapes=[
            pltpu.VMEM((rows, mine, width), BF16),
            pltpu.VMEM((own, heads, width), BF16),
            pltpu.VMEM((1, rows), jnp.int32),
            pltpu.SMEM((own,), jnp.int32),
            pltpu.VMEM((lanes, rows * group), BF16),
            pltpu.VMEM((per, lanes, width), BF16),
            pltpu.VMEM((per, lanes, width), BF16),
            pltpu.VMEM((per, lanes, width), BF16),
            pltpu.VMEM((2, per, n * sys_keys.shape[1], width), BF16),
            pltpu.VMEM((2, per, 2 * task_keys.shape[2], width), BF16),
            pltpu.VMEM(suffix_keys.shape, BF16),
            pltpu.VMEM(suffix_keys.shape, BF16),
            pltpu.VMEM((2, own, mine, width), F32),
            pltpu.VMEM((2, own, mine, width), F32),
            pltpu.VMEM((own, mine, width), F32),
            pltpu.VMEM((own, mine, width), F32),
            pltpu.VMEM((per, width, lanes), F32),
            pltpu.VMEM((per, 8, lanes), F32),
            pltpu.VMEM((per, 2, width, tile), BF16),
            pltpu.VMEM((per, 2, 8, tile), F32),
            pltpu.VMEM((per, 2, width, tile), BF16),
            pltpu.VMEM((per, 2, 8, tile), F32),
            pltpu.VMEM((per, width // 2, tile), BF16),
            pltpu.VMEM((per, 8, tile), F32),
            pltpu.VMEM((per, width // 2, tile), BF16),
            pltpu.VMEM((per, 8, tile), F32),
            pltpu.VMEM((2, own, mine, width), F32),
            pltpu.VMEM((2, own, mine, width), BF16),
            dma((4,)),
            dma((2,)),
            dma((2, per)),
            dma((2, own)),
            dma((2, per)),
            dma((2, per)),
            dma((2, per, 3)),
            dma((2, per, 3)),
            dma((per, 5)),
            dma((per, 5)),
            dma((2, per, 3)),
            dma((2, per, 3)),
            dma((2,)),
            dma((2,)),
            dma,
            dma,
            dma,
        ],
        compiler_params=pltpu.CompilerParams(
            collective_id=0, has_side_effects=True, vmem_limit_bytes=60 * 1024 * 1024
        ),
        name="cascade",
    )(*args[:7], task_ids.reshape(1, rows), args[8])


def body(
    queries,
    sys_keys,
    sys_values,
    task_keys,
    task_values,
    suffix_keys,
    suffix_values,
    task_ids,
    suffix_len,
):
    n = lax.axis_size("kv")
    rows, heads, width = queries.shape
    kv = sys_keys.shape[0]
    group = heads // kv
    own = suffix_keys.shape[0]
    lanes = n * CAP * group
    half = lanes // 2
    out_shape = jax.ShapeDtypeStruct((own, heads, width), BF16)
    if n == 4 and rows == n * CAP and kv % 2 == 0 and 2 * CAP * group == width:
        args = (
            queries,
            sys_keys,
            sys_values,
            task_keys,
            task_values,
            suffix_keys,
            suffix_values,
            task_ids,
            suffix_len,
        )
        return paired_call(n, args, out_shape)
    vmem = pl.BlockSpec(memory_space=pltpu.VMEM)
    anywhere = pl.BlockSpec(memory_space=pl.ANY)
    dma = pltpu.SemaphoreType.DMA
    return pl.pallas_call(
        functools.partial(kernel, n),
        out_shape=out_shape,
        in_specs=[vmem] * 3 + [anywhere] * 4 + [vmem, pl.BlockSpec(memory_space=pltpu.SMEM)],
        out_specs=vmem,
        scratch_shapes=[
            pltpu.VMEM(task_keys.shape[1:], BF16),
            pltpu.VMEM(task_values.shape[1:], BF16),
            pltpu.VMEM(suffix_keys.shape, BF16),
            pltpu.VMEM(suffix_values.shape, BF16),
            pltpu.VMEM((n, kv, lanes, width), BF16),
            pltpu.VMEM((n, 2, kv, width, half), F32),
            pltpu.VMEM((n, 2, kv, 8, half), F32),
            pltpu.VMEM((n, kv, width, half), F32),
            pltpu.VMEM((n, kv, 8, half), F32),
            pltpu.VMEM((n, kv, width, half), BF16),
            pltpu.VMEM((n, kv, 8, half), F32),
            pltpu.VMEM((2, n, kv, width, half), BF16),
            pltpu.VMEM((2, n, kv, 8, half), F32),
            pltpu.VMEM((2, kv, width, half), F32),
            pltpu.VMEM((2, kv, 8, half), F32),
            pltpu.VMEM((own, heads, width), F32),
            pltpu.VMEM((own, heads, width), F32),
            pltpu.VMEM((own, heads, width), F32),
            dma((2,)),
            dma((2, own)),
            dma((2, kv)),
            dma((n, kv)),
            dma((n, kv)),
            dma((n, kv)),
            dma((n, kv)),
            dma((2, n, kv)),
            dma((2, n, kv)),
            dma((2, n, kv)),
            dma((2, 2, n, kv)),
            dma((2, kv)),
            dma((2, kv)),
        ],
        compiler_params=pltpu.CompilerParams(
            collective_id=0, has_side_effects=True, vmem_limit_bytes=60 * 1024 * 1024
        ),
        name="cascade",
    )(
        queries,
        sys_keys,
        sys_values,
        task_keys,
        task_values,
        suffix_keys,
        suffix_values,
        task_ids.reshape(1, rows),
        suffix_len,
    )


def solution(mesh):
    in_specs = (
        P(("replica", "kv"), "head", None),
        P(("replica", "head"), ("kv", "sub"), None),
        P(("replica", "head"), ("kv", "sub"), None),
        P(("replica", "kv"), "head", "sub", None),
        P(("replica", "kv"), "head", "sub", None),
        P(("replica", "kv", "sub"), "head", None, None),
        P(("replica", "kv", "sub"), "head", None, None),
        P(("replica", "kv")),
        P(("replica", "kv", "sub")),
    )
    out_specs = P(("replica", "kv", "sub"), "head", None)
    return jax.shard_map(body, mesh=mesh, in_specs=in_specs, out_specs=out_specs, check_vma=False)
```

```python
import functools
import math

import jax
import jax.numpy as jnp
from jax import lax
from jax.experimental import pallas as pl
from jax.experimental.pallas import tpu as pltpu
from jax.sharding import PartitionSpec as P

CAP = 8
NEGATIVE = -1e30
MESH = pl.DeviceIdType.MESH
NT = (((1,), (1,)), ((), ()))
TN = (((0,), (0,)), ((), ()))
F32 = jnp.float32
BF16 = jnp.bfloat16


def dot(a, b, dims=(((1,), (0,)), ((), ()))):
    return lax.dot_general(a, b, dims, preferred_element_type=F32)


def merge(first, second):
    top = jnp.maximum(first[1], second[1])
    a = jnp.exp(first[1] - top)
    b = jnp.exp(second[1] - top)
    total = a + b
    inverse = 1.0 / total
    return first[0] * (a * inverse) + second[0] * (b * inverse), top + jnp.log(total)


def iota(shape, dim):
    return lax.broadcasted_iota(jnp.int32, shape, dim)


def selected(value, picks, pieces):
    out = None
    for _ in range(pieces):
        part = value.astype(BF16)
        value = value - part.astype(F32)
        term = dot(part, picks)
        out = term if out is None else out + term
    return out


def kernel(
    n,
    q_ref,
    sk_ref,
    sv_ref,
    tk_hbm,
    tv_hbm,
    uk_hbm,
    uv_hbm,
    ids_ref,
    len_ref,
    out_ref,
    tk,
    tv,
    uk,
    uv,
    qbuf,
    part_o,
    part_e,
    swap_o,
    swap_e,
    send_o,
    send_e,
    chain_o,
    chain_e,
    fin_o,
    fin_e,
    suf_o,
    suf_e,
    out32,
    task_sem,
    suf_sem,
    own_send,
    z_send,
    z_recv,
    d_send,
    d_recv,
    swap_send,
    swap_recv,
    chain_send,
    chain_recv,
    fin_send,
    fin_recv,
):
    rows, heads, width = q_ref.shape
    kv = sk_ref.shape[0]
    group = heads // kv
    own = uk.shape[0]
    lanes = qbuf.shape[2]
    half = lanes // 2
    task_rows = CAP * group
    scale = 1.0 / math.sqrt(width)
    j = lax.axis_index("kv")
    s = lax.axis_index("sub")
    other = 1 - s

    task_copies = []
    for index, (hbm, buf) in enumerate(((tk_hbm, tk), (tv_hbm, tv))):
        copy = pltpu.make_async_copy(hbm.at[0], buf, task_sem.at[index])
        copy.start()
        task_copies.append(copy)

    def suffix_copies(i):
        return (
            pltpu.make_async_copy(uk_hbm.at[i], uk.at[i], suf_sem.at[0, i]),
            pltpu.make_async_copy(uv_hbm.at[i], uv.at[i], suf_sem.at[1, i]),
        )

    @pl.loop(0, own)
    def _(i):
        for copy in suffix_copies(i):
            copy.start()

    barrier = pltpu.get_barrier_semaphore()
    pl.semaphore_signal(barrier, inc=1, device_id={"sub": other}, device_id_type=MESH)

    @pl.when(j > 0)
    def _():
        pl.semaphore_signal(barrier, inc=1, device_id={"kv": j - 1}, device_id_type=MESH)

    @pl.when(j < n - 1)
    def _():
        pl.semaphore_signal(barrier, inc=1, device_id={"kv": j + 1}, device_id_type=MESH)

    ids = ids_ref[...].astype(F32)
    wide = jnp.broadcast_to(ids, (rows, rows))
    down, across = iota((rows, rows), 0), iota((rows, rows), 1)
    ids_column = jnp.sum(jnp.where(down == across, wide, 0.0), axis=1, keepdims=True)
    same = jnp.where((ids_column == wide) & (down < across), 1.0, 0.0)
    places = ids * CAP + jnp.sum(same, axis=0, keepdims=True)
    places8 = jnp.broadcast_to(places, (8, rows)).astype(BF16)

    def spread(count, base):
        shape = (rows, count * group)
        pick = jnp.where(iota(shape, 0) == base + iota(shape, 1) // group, 1.0, 0.0).astype(BF16)
        row = dot(places8, pick)[0:1].astype(jnp.int32)
        shape = (lanes, count * group)
        down, across = iota(shape, 0), iota(shape, 1)
        hit = (down // group == row) & (down % group == across % group)
        return jnp.where(hit, 1.0, 0.0).astype(BF16)

    everyone = spread(rows, 0)
    wide_query = q_ref[...].astype(F32)
    for k in range(kv):
        mine = wide_query[:, k * group : (k + 1) * group, :].reshape(rows * group, width)
        qbuf[j, k] = dot(everyone, mine.astype(BF16)).astype(BF16)

    pl.semaphore_wait(
        barrier, 1 + jnp.where(j > 0, 1, 0) + jnp.where(j < n - 1, 1, 0)
    )

    def query_view(p, k, h):
        return qbuf.at[p, k, pl.ds(pl.multiple_of(h * half, 16), half), :]

    def query_copy(p, k, send_sem, recv_sem, device):
        return pltpu.make_async_remote_copy(
            src_ref=query_view(p, k, s),
            dst_ref=query_view(p, k, s),
            send_sem=send_sem,
            recv_sem=recv_sem,
            device_id=device,
            device_id_type=MESH,
        )

    def own_copy(k, d):
        return query_copy(j, k, own_send.at[d, k], z_recv.at[j, k], {"kv": j + 2 * d - 1})

    def relay_copy(p, k, d):
        return query_copy(p, k, z_send.at[p, k], z_recv.at[p, k], {"kv": j + 1 - 2 * d})

    def side_copy(p, k):
        return query_copy(p, k, d_send.at[p, k], d_recv.at[p, k], {"sub": other})

    def side_arrival(p, k):
        return pltpu.make_async_remote_copy(
            src_ref=query_view(p, k, other),
            dst_ref=query_view(p, k, other),
            send_sem=d_send.at[p, k],
            recv_sem=d_recv.at[p, k],
            device_id={"sub": other},
            device_id_type=MESH,
        )

    @pl.when(j < n - 1)
    def _():
        for k in range(kv):
            own_copy(k, 1).start()

    @pl.when(j > 0)
    def _():
        for k in range(kv):
            own_copy(k, 0).start()

    def swap_copies(p, k):
        return tuple(
            pltpu.make_async_remote_copy(
                src_ref=src.at[p, other, k],
                dst_ref=dst.at[p, k],
                send_sem=swap_send.at[index, p, k],
                recv_sem=swap_recv.at[index, p, k],
                device_id={"sub": other},
                device_id_type=MESH,
            )
            for index, (src, dst) in enumerate(((part_o, swap_o), (part_e, swap_e)))
        )

    def chain_copies(p, k, d, target=None):
        target = {"kv": j + 2 * d - 1} if target is None else target
        return tuple(
            pltpu.make_async_remote_copy(
                src_ref=src.at[p, k],
                dst_ref=dst.at[d, p, k],
                send_sem=chain_send.at[index, p, k],
                recv_sem=chain_recv.at[index, d, p, k],
                device_id=target,
                device_id_type=MESH,
            )
            for index, (src, dst) in enumerate(((send_o, chain_o), (send_e, chain_e)))
        )

    def fin_copies(k):
        return tuple(
            pltpu.make_async_remote_copy(
                src_ref=buf.at[s, k],
                dst_ref=buf.at[s, k],
                send_sem=fin_send.at[index, k],
                recv_sem=fin_recv.at[index, k],
                device_id={"sub": other},
                device_id_type=MESH,
            )
            for index, buf in enumerate((fin_o, fin_e))
        )

    def fin_arrivals(k):
        return tuple(
            pltpu.make_async_remote_copy(
                src_ref=buf.at[other, k],
                dst_ref=buf.at[other, k],
                send_sem=fin_send.at[index, k],
                recv_sem=fin_recv.at[index, k],
                device_id={"sub": other},
                device_id_type=MESH,
            )
            for index, buf in enumerate((fin_o, fin_e))
        )

    def attend(keys, values, query):
        scores = dot(keys, query, NT)
        maxima = jnp.max(scores, axis=0, keepdims=True)
        weights = jnp.exp((scores - maxima) * scale)
        totals = jnp.sum(weights, axis=0, keepdims=True)
        return maxima * scale, totals, dot(values, weights.astype(BF16), TN)

    def block(p, d):
        def arrive(k):
            @pl.when(jnp.logical_not(beyond(d)))
            def _():
                relay_copy(p, k, d).wait_recv()
                side_copy(p, k).start()

        for k in range(kv):
            if d is not None:
                for later in ([0, 1] if k == 0 else [k + 1]):
                    if later < kv:
                        arrive(later)
                side_arrival(p, k).wait_recv()
            top, total, numerator = attend(sk_ref[k], sv_ref[k], qbuf[p, k])
            system = (numerator * (1.0 / total), top + jnp.log(total))
            picked = qbuf[p, k, pl.ds(pl.multiple_of(j * task_rows, 16), task_rows), :]
            doubled = jnp.concatenate([picked, picked], axis=0)
            tokens = tk.shape[1]
            step = min(512, tokens)
            state = None
            for base in range(0, tokens, step):
                part = attend(
                    tk[k, base : base + step, :], tv[k, base : base + step, :], doubled
                )
                if state is None:
                    state = part
                else:
                    top = jnp.maximum(state[0], part[0])
                    a, b = jnp.exp(state[0] - top), jnp.exp(part[0] - top)
                    state = (top, state[1] * a + part[1] * b, state[2] * a + part[2] * b)
            top, total, numerator = state
            repeats = lanes // (2 * task_rows)
            place = iota((1, lanes), 1) // task_rows == j
            task = (
                jnp.concatenate([numerator * (1.0 / total)] * repeats, axis=1),
                jnp.where(
                    place, jnp.concatenate([top + jnp.log(total)] * repeats, axis=1), NEGATIVE
                ),
            )
            result, level = merge(system, task)
            for h in range(2):
                part_o[p, h, k] = result[:, h * half : (h + 1) * half]
                part_e[p, h, k] = jnp.broadcast_to(level[:, h * half : (h + 1) * half], (8, half))
            for copy in swap_copies(p, k):
                copy.start()

    def chip_part(p, k):
        return merge(
            (part_o[p, s, k], part_e[p, s, k][0:1]), (swap_o[p, k], swap_e[p, k][0:1])
        )

    def chain_part(d, p, k):
        return chain_o[d, p, k].astype(F32), chain_e[d, p, k][0:1]

    def finish(p, d, incoming):
        for k in range(kv):
            for copy in swap_copies(p, k):
                copy.wait_recv()
            state = chip_part(p, k)
            if incoming:
                for copy in chain_copies(p, k, d):
                    copy.wait_recv()
                state = merge(state, chain_part(d, p, k))
            send_o[p, k] = state[0].astype(BF16)
            send_e[p, k] = jnp.broadcast_to(state[1], (8, half))
            for copy in chain_copies(p, k, d):
                copy.start()

    def suffix(i):
        for copy in suffix_copies(i):
            copy.wait()
        query = q_ref[s * own + i].astype(F32)
        length = len_ref[i]
        scores = jnp.concatenate(
            [
                dot(query[k * group : (k + 1) * group].astype(BF16), uk[i, k], NT)
                for k in range(kv)
            ],
            axis=0,
        )
        usable = iota(scores.shape, 1) < length
        scores = jnp.where(usable, scores, NEGATIVE)
        maxima = jnp.max(scores, axis=1, keepdims=True)
        weights = jnp.where(usable, jnp.exp((scores - maxima) * scale), 0.0)
        totals = jnp.sum(weights, axis=1, keepdims=True)
        numerator = jnp.concatenate(
            [
                dot(weights[k * group : (k + 1) * group].astype(BF16), uv[i, k])
                for k in range(kv)
            ],
            axis=0,
        )
        suf_o[i] = numerator * (1.0 / totals)
        suf_e[i] = jnp.broadcast_to(maxima * scale + jnp.log(totals), (heads, width))

    def source(t, d):
        return j + (2 * d - 1) * t

    def valid(t, d):
        p = source(t, d)
        return (p >= 0) & (p < n)

    def beyond(d):
        return jnp.where(d == 0, j < n - 1, j > 0)

    early = own // 4
    late, turns = own - early, 2 * n - 2

    @pl.loop(0, early)
    def _(i):
        suffix(i)

    for copy in task_copies:
        copy.wait()

    @pl.loop(1, n)
    def _(t):
        for k in range(kv):
            for d in range(2):

                @pl.when(valid(t, d) & beyond(d))
                def _(d=d, k=k):
                    p = source(t, d)
                    relay_copy(p, k, d).wait_recv()
                    relay_copy(p, k, d).start()
                    side_copy(p, k).start()

        @pl.loop(0, 2)
        def _(d):
            @pl.when(valid(t, d))
            def _():
                block(source(t, d), d)

        for d in range(2):

            @pl.when(valid(t, d) & jnp.logical_not(beyond(d)))
            def _(d=d):
                finish(source(t, d), d, False)

    block(j, None)

    @pl.loop(1, 2 * n - 1)
    def _(turn):
        @pl.loop(early + (turn - 1) * late // turns, early + turn * late // turns)
        def _(i):
            suffix(i)

        low = 2 * (n - 1) - j - turn

        @pl.when((low >= 0) & (low < j) & (j < n - 1))
        def _():
            finish(low, 0, True)

        high = turn - j

        @pl.when((high > j) & (high < n) & (j > 0))
        def _():
            finish(high, 1, True)

    for k in range(kv):
        for copy in swap_copies(j, k):
            copy.wait_recv()
        value, level = chip_part(j, k)
        fin_o[s, k] = value
        fin_e[s, k] = jnp.broadcast_to(level, (8, half))
    chosen = spread(own, s * own)
    for k in range(kv):
        for d in range(2):

            @pl.when(j < n - 1 if d == 0 else j > 0)
            def _(d=d, k=k):
                for copy in chain_copies(j, k, d, {"kv": j + 1 - 2 * d}):
                    copy.wait_recv()
                state = merge((fin_o[s, k], fin_e[s, k][0:1]), chain_part(d, j, k))
                fin_o[s, k] = state[0]
                fin_e[s, k] = jnp.broadcast_to(state[1], (8, half))

        for copy in fin_copies(k):
            copy.start()
    for k in range(kv):
        for copy in fin_arrivals(k):
            copy.wait_recv()
        value = jnp.concatenate([fin_o[0, k], fin_o[1, k]], axis=1)
        level = jnp.concatenate([fin_e[0, k], fin_e[1, k]], axis=1)
        value = selected(value, chosen, 2).T
        level = jnp.broadcast_to(selected(level, chosen, 3)[0:1], (width, own * group)).T
        near = slice(k * group, (k + 1) * group)
        suffix_state = (
            suf_o[:, near, :].reshape(own * group, width),
            suf_e[:, near, :].reshape(own * group, width),
        )
        attended = merge((value, level), suffix_state)[0]
        out32[:, near, :] = attended.reshape(own, group, width)
    out_ref[...] = out32[...].astype(BF16)

    for k in range(kv):

        @pl.when(j < n - 1)
        def _(k=k):
            own_copy(k, 1).wait_send()

        @pl.when(j > 0)
        def _(k=k):
            own_copy(k, 0).wait_send()

        for copy in swap_copies(j, k) + fin_copies(k):
            copy.wait_send()

    @pl.loop(1, n)
    def _(t):
        for d in range(2):

            @pl.when(valid(t, d))
            def _(d=d):
                p = source(t, d)
                for k in range(kv):

                    @pl.when(beyond(d))
                    def _(k=k):
                        relay_copy(p, k, d).wait_send()

                    side_copy(p, k).wait_send()
                    for copy in swap_copies(p, k) + chain_copies(p, k, d):
                        copy.wait_send()


exp2 = jnp.exp2
scope = jax.named_scope


def blend(parts):
    top = parts[0][1]
    for part in parts[1:]:
        top = jnp.maximum(top, part[1])
    factors = [exp2(part[1] - top) for part in parts]
    total = sum(factors[1:], factors[0])
    inverse = 1.0 / total
    value = parts[0][0] * (factors[0] * inverse)
    for part, factor in zip(parts[1:], factors[1:]):
        value = value + part[0] * (factor * inverse)
    return value, top + jnp.log2(total)


def paired(
    n,
    q_hbm,
    sk_hbm,
    sv_hbm,
    tk_hbm,
    tv_hbm,
    uk_hbm,
    uv_hbm,
    ids_hbm,
    len_hbm,
    out_ref,
    qh,
    qo,
    ids_ref,
    len_ref,
    perm,
    qs,
    tq,
    qx,
    sysb,
    taskb,
    uk,
    uv,
    suf_o,
    suf_e,
    sib_o,
    sib_e,
    base_o,
    base_e,
    rs_o,
    rs_e,
    rr_o,
    rr_e,
    ps_o,
    ps_e,
    pr_o,
    pr_e,
    out32,
    outb,
    load_sem,
    sysl_sem,
    task_sem,
    suf_sem,
    tx_send,
    tx_recv,
    sys_send,
    sys_recv,
    q_send,
    q_recv,
    ret_send,
    ret_recv,
    sx_send,
    sx_recv,
    fin_send,
    fin_recv,
):
    rows = qh.shape[0]
    own, heads, width = qo.shape
    mine = qh.shape[1]
    kv = uk.shape[1]
    group = heads // kv
    per = kv // 2
    half_n = n // 2
    cell = CAP * group
    lanes = 2 * half_n * cell
    tile = 2 * cell
    shard = sk_hbm.shape[1]
    stretch = tk_hbm.shape[2]
    scale = math.log2(math.e) / math.sqrt(width)
    j = lax.axis_index("kv")
    s = lax.axis_index("sub")
    other = 1 - s
    side = j // half_n
    e = j % half_n
    mate = j + 1 - 2 * e
    far = (1 - side) * half_n

    barrier = pltpu.get_barrier_semaphore()
    pl.semaphore_signal(barrier, inc=1, device_id={"sub": other}, device_id_type=MESH)
    for d in range(1, n):
        target = lax.rem(j + d, n)
        for z in range(2):
            pl.semaphore_signal(
                barrier, inc=1, device_id={"kv": target, "sub": z}, device_id_type=MESH
            )

    def remote(src, dst, send_sem, recv_sem, device):
        return pltpu.make_async_remote_copy(
            src_ref=src,
            dst_ref=dst,
            send_sem=send_sem,
            recv_sem=recv_sem,
            device_id=device,
            device_id_type=MESH,
        )

    first = pl.multiple_of(s * mine, 16)
    loads = [
        pltpu.make_async_copy(ids_hbm, ids_ref, load_sem.at[0]),
        pltpu.make_async_copy(q_hbm.at[:, pl.ds(first, mine), :], qh, load_sem.at[1]),
        pltpu.make_async_copy(q_hbm.at[pl.ds(s * own, own)], qo, load_sem.at[2]),
        pltpu.make_async_copy(len_hbm, len_ref, load_sem.at[3]),
    ]
    for copy in loads:
        copy.start()

    def spot(chip, core):
        return pl.ds(pl.multiple_of((2 * chip + core) * shard, 128), shard)

    sys_local = [
        pltpu.make_async_copy(
            hbm.at[pl.ds(s * per, per)], sysb.at[kind, :, spot(e, s), :], sysl_sem.at[kind]
        )
        for kind, hbm in enumerate((sk_hbm, sv_hbm))
    ]
    for copy in sys_local:
        copy.start()

    def strip(core):
        return pl.ds(pl.multiple_of(core * stretch, 128), stretch)

    task_local = [
        [
            pltpu.make_async_copy(
                hbm.at[0, s * per + h], taskb.at[kind, h, strip(s), :], task_sem.at[kind, h]
            )
            for kind, hbm in enumerate((tk_hbm, tv_hbm))
        ]
        for h in range(per)
    ]
    def suffix_copies(i):
        return (
            pltpu.make_async_copy(uk_hbm.at[i], uk.at[i], suf_sem.at[0, i]),
            pltpu.make_async_copy(uv_hbm.at[i], uv.at[i], suf_sem.at[1, i]),
        )

    def fetch(low, high):
        @pl.loop(low, high)
        def _(i):
            for copy in suffix_copies(i):
                copy.start()

    fetch(0, own // 4)
    for copies in task_local:
        for copy in copies:
            copy.start()
    fetch(own // 4, own)

    with scope("ids"):
        loads[0].wait()
    ids = ids_ref[...]
    names = ids.astype(F32)
    wide = jnp.broadcast_to(names, (rows, rows))
    down, across = iota((rows, rows), 0), iota((rows, rows), 1)
    column = jnp.sum(jnp.where(down == across, wide, 0.0), axis=1, keepdims=True)
    same = jnp.where((column == wide) & (down < across), 1.0, 0.0)
    seat = ids % half_n
    seat = jnp.where(ids // half_n == side, half_n - 1 - seat, half_n + seat)
    places = seat.astype(F32) * CAP + jnp.sum(same, axis=0, keepdims=True)
    places8 = jnp.broadcast_to(places, (8, rows)).astype(BF16)
    shape = (rows, rows * group)
    pick = jnp.where(iota(shape, 0) == iota(shape, 1) // group, 1.0, 0.0).astype(BF16)
    row = dot(places8, pick)[0:1].astype(jnp.int32)
    shape = (lanes, rows * group)
    down, across = iota(shape, 0), iota(shape, 1)
    hit = (down // group == row) & (down % group == across % group)
    perm[...] = jnp.where(hit, 1.0, 0.0).astype(BF16)
    loads[1].wait()
    wide_query = qh[...].astype(F32)
    for h in range(per):
        flat = wide_query[:, h * group : (h + 1) * group, :].reshape(rows * group, width)
        qs[h] = dot(perm[...], flat.astype(BF16)).astype(BF16)

    def cellat(base):
        return pl.ds(pl.multiple_of(base, 16), cell)

    for h in range(per):
        tq[h, cellat((1 - e) * cell), :] = qs[h, cellat((1 - e) * cell), :]

    def query_copies(h):
        copies = [
            remote(
                qs.at[h, cellat(e * cell), :],
                tq.at[h, cellat(tile + e * cell), :],
                q_send.at[h, 0],
                q_recv.at[h, 0],
                {"kv": mate},
            )
        ]
        for c in range(2):
            copies.append(
                remote(
                    qs.at[h, cellat(tile + c * cell), :],
                    tq.at[h, cellat(e * tile + c * cell), :],
                    q_send.at[h, 1 + c],
                    q_recv.at[h, 1 + e],
                    {"kv": far + c},
                )
            )
            copies.append(
                remote(
                    qs.at[h, cellat((1 - c) * cell), :],
                    qx.at[h, cellat(e * tile + (1 - c) * cell), :],
                    q_send.at[h, 3 + c],
                    q_recv.at[h, 3 + e],
                    {"kv": far + c},
                )
            )
        return copies

    def query_arrivals(h):
        places = [(tq, tile + (1 - e) * cell)]
        places += [(tq, i * tile + e * cell) for i in range(2)]
        places += [(qx, i * tile + (1 - e) * cell) for i in range(2)]
        return [
            remote(
                buf.at[h, cellat(base), :],
                buf.at[h, cellat(base), :],
                q_send.at[h, index],
                q_recv.at[h, index],
                {"kv": mate},
            )
            for index, (buf, base) in enumerate(places)
        ]

    def sys_copies(h):
        copies = []
        for kind, hbm in enumerate((sk_hbm, sv_hbm)):
            dst = sysb.at[kind, h, spot(e, s), :]
            copies.append(
                remote(
                    hbm.at[other * per + h],
                    dst,
                    sys_send.at[kind, h, 0],
                    sys_recv.at[kind, h, 0],
                    {"sub": other},
                )
            )
            for z in range(2):
                copies.append(
                    remote(
                        hbm.at[z * per + h],
                        dst,
                        sys_send.at[kind, h, 1 + z],
                        sys_recv.at[kind, h, 1 + s],
                        {"kv": mate, "sub": z},
                    )
                )
        return copies

    def sys_arrivals(h):
        out = []
        for kind in range(2):
            for index, (chip, core) in enumerate(((e, other), (1 - e, 0), (1 - e, 1))):
                ref = sysb.at[kind, h, spot(chip, core), :]
                out.append(
                    remote(
                        ref,
                        ref,
                        sys_send.at[kind, h, index],
                        sys_recv.at[kind, h, index],
                        {"sub": other},
                    )
                )
        return out

    def task_copies(h):
        return [
            remote(
                hbm.at[0, other * per + h],
                taskb.at[kind, h, strip(s), :],
                tx_send.at[kind, h],
                tx_recv.at[kind, h],
                {"sub": other},
            )
            for kind, hbm in enumerate((tk_hbm, tv_hbm))
        ]

    def task_arrivals(h):
        return [
            remote(
                taskb.at[kind, h, strip(other), :],
                taskb.at[kind, h, strip(other), :],
                tx_send.at[kind, h],
                tx_recv.at[kind, h],
                {"sub": other},
            )
            for kind in range(2)
        ]

    def suffix(base):
        picks = range(4)
        for r in picks:
            for copy in suffix_copies(base + r):
                copy.wait()
        scores = []
        for r in picks:
            query = qo[base + r].astype(F32)
            scores.append(
                jnp.concatenate(
                    [
                        dot(
                            query[k * group : (k + 1) * group].astype(BF16),
                            uk[base + r, k],
                            NT,
                        )
                        for k in range(kv)
                    ],
                    axis=0,
                )
            )
        states = []
        for r in picks:
            usable = iota(scores[r].shape, 1) < len_ref[base + r]
            masked = jnp.where(usable, scores[r], NEGATIVE)
            maxima = jnp.max(masked, axis=1, keepdims=True)
            weights = jnp.where(usable, exp2((masked - maxima) * scale), 0.0)
            states.append((maxima, weights, jnp.sum(weights, axis=1, keepdims=True)))
        for r in picks:
            maxima, weights, totals = states[r]
            numerator = jnp.concatenate(
                [
                    dot(weights[k * group : (k + 1) * group].astype(BF16), uv[base + r, k])
                    for k in range(kv)
                ],
                axis=0,
            )
            value = numerator * (1.0 / totals)
            level = jnp.broadcast_to(maxima * scale + jnp.log2(totals), (heads, width))
            for z in range(2):
                suf_o[z, base + r] = value[z * mine : (z + 1) * mine]
                suf_e[z, base + r] = level[z * mine : (z + 1) * mine]

    def sweep(items):
        states = {}
        ahead = [dot(item[1](), item[3], NT) for item in items[:1]]
        for index, (name, _, values, _) in enumerate(items):
            scores = ahead.pop(0)
            if index + 1 < len(items):
                item = items[index + 1]
                ahead.append(dot(item[1](), item[3], NT))
            top = jnp.max(scores, axis=0, keepdims=True)
            weights = exp2((scores - top) * scale)
            total = jnp.sum(weights, axis=0, keepdims=True)
            part = (top * scale, total, dot(values(), weights.astype(BF16), TN))
            if name in states:
                state = states[name]
                top = jnp.maximum(state[0], part[0])
                a, b = exp2(state[0] - top), exp2(part[0] - top)
                part = (top, state[1] * a + part[1] * b, state[2] * a + part[2] * b)
            states[name] = part
        return {
            name: (numerator * (1.0 / total), top + jnp.log2(total))
            for name, (top, total, numerator) in states.items()
        }

    def pieces(name, buf, h, step, query):
        tokens = buf.shape[2]
        step = min(step, tokens)
        return [
            (
                name,
                lambda base=base: buf[0, h, base : base + step, :],
                lambda base=base: buf[1, h, base : base + step, :],
                query,
            )
            for base in range(0, tokens, step)
        ]

    zone = iota((1, tile), 1) // cell

    slim = (slice(None), pl.ds(0, 1))

    def ret_copies(h, i):
        return [
            remote(
                src.at[h, i, slim[index]],
                dst.at[h, e, slim[index]],
                ret_send.at[index, h, i],
                ret_recv.at[index, h, e],
                {"kv": far + i},
            )
            for index, (src, dst) in enumerate(((rs_o, rr_o), (rs_e, rr_e)))
        ]

    def ret_arrivals(h, i):
        return [
            remote(
                dst.at[h, i, slim[index]],
                dst.at[h, i, slim[index]],
                ret_send.at[index, h, i],
                ret_recv.at[index, h, i],
                {"kv": far + i},
            )
            for index, dst in enumerate((rr_o, rr_e))
        ]

    def mate_copies(h):
        return [
            remote(
                src.at[h, slim[index]],
                dst.at[h, slim[index]],
                ret_send.at[index, h, 2],
                ret_recv.at[index, h, 2],
                {"kv": mate},
            )
            for index, (src, dst) in enumerate(((ps_o, pr_o), (ps_e, pr_e)))
        ]

    def arrive(h):
        with scope("local"):
            for copy in task_local[h]:
                copy.wait()
        with scope("queries"):
            for copy in query_arrivals(h):
                copy.wait_recv()
        with scope("taskwait"):
            for copy in task_arrivals(h):
                copy.wait_recv()

    def system(h):
        with scope("syswait"):
            if h == 0:
                for copy in sys_local:
                    copy.wait()
            for copy in sys_arrivals(h):
                copy.wait_recv()

    def gather(h):
        for i in range(2):
            qx[h, cellat(i * tile + e * cell), :] = tq[h, cellat(i * tile + e * cell), :]

    def task_items(h):
        return pieces("task", taskb, h, 1024, tq[h])

    def cross_items(h):
        return pieces("cross", sysb, h, 1024, qx[h])

    def keep_task(h, found):
        value, level = found
        base_o[h] = value
        base_e[h] = jnp.broadcast_to(level, (8, lanes))
        near = value[:, tile:]
        packed = jnp.where(
            zone == 1 - e,
            near[: width // 2],
            pltpu.roll(near[width // 2 :], cell, 1),
        )
        ps_o[h] = packed.astype(BF16)
        ps_e[h] = jnp.broadcast_to(level[:, tile:], (8, tile))

    def keep_cross(h, found, task):
        value, level = found
        for i in range(2):
            cut = slice(i * tile, (i + 1) * tile)
            task_level = jnp.where(zone == e, task[1][:, cut], NEGATIVE)
            merged = blend([(value[:, cut], level[:, cut]), (task[0][:, cut], task_level)])
            rs_o[h, i] = merged[0].astype(BF16)
            rs_e[h, i] = jnp.broadcast_to(merged[1], (8, tile))

    def home():
        items = []
        for h in range(per):
            items += pieces(h, sysb, h, 1024, qs[h])
        found = sweep(items)
        for h in range(per):
            value, level = found[h]
            task_level = jnp.where(zone == 1 - e, base_e[h, 0:1, :tile], NEGATIVE)
            merged = blend([(value[:, :tile], level[:, :tile]), (base_o[h, :, :tile], task_level)])
            base_o[h] = jnp.concatenate([merged[0], value[:, tile:]], axis=1)
            base_e[h] = jnp.broadcast_to(
                jnp.concatenate([merged[1], level[:, tile:]], axis=1), (8, lanes)
            )

    def exchange():
        return [
            remote(
                src.at[other],
                dst,
                sx_send.at[index],
                sx_recv.at[index],
                {"sub": other},
            )
            for index, (src, dst) in enumerate(((suf_o, sib_o), (suf_e, sib_e)))
        ]

    def span(core):
        return pl.ds(pl.multiple_of(core * own * group, 128), own * group)

    def fold(h):
        value, level = None, None
        for core, o_ref, e_ref in ((s, suf_o.at[s], suf_e.at[s]), (other, sib_o, sib_e)):
            near = slice(h * group, (h + 1) * group)
            rest = o_ref[:, near, :].reshape(own * group, width)
            tall = e_ref[:, near, :].reshape(own * group, width)
            chosen = perm[:, span(core)]
            for _ in range(2):
                piece = rest.astype(BF16)
                rest = rest - piece.astype(F32)
                term = dot(piece, chosen, (((0,), (1,)), ((), ())))
                value = term if value is None else value + term
            tall = tall.T[0:1]
            term = jnp.sum(jnp.where(chosen.astype(F32) > 0.5, tall, 0.0), axis=1, keepdims=True)
            level = term if level is None else level + term
        level = jnp.broadcast_to(level, (lanes, width)).T[0:1]
        merged = blend([(base_o[h], base_e[h][0:1]), (value, level)])
        base_o[h] = merged[0]
        base_e[h] = jnp.broadcast_to(merged[1], (8, lanes))

    def finish(h):
        with scope("retwait"):
            for copy in ret_arrivals(h, 0) + ret_arrivals(h, 1) + mate_copies(h):
                copy.wait_recv()
        low = zone == 0
        far_o = [rr_o[h, c].astype(F32) for c in range(2)]
        far_e = [rr_e[h, c][0:1] for c in range(2)]
        crossed = [
            (jnp.where(low, far_o[1], far_o[0]), jnp.where(low, far_e[1], far_e[0])),
            (jnp.where(low, far_o[0], far_o[1]), jnp.where(low, far_e[0], far_e[1])),
        ]
        packed = pr_o[h].astype(F32)
        near = jnp.concatenate([packed, pltpu.roll(packed, cell, 1)], axis=0)
        near_level = jnp.where(zone == e, pr_e[h][0:1], NEGATIVE)
        results = []
        for i in range(2):
            cut = slice(i * tile, (i + 1) * tile)
            parts = [(base_o[h, :, cut], base_e[h, 0:1, cut]), crossed[i]]
            if i == 0:
                parts.append((near, near_level))
            results.append(blend(parts)[0])
        done = jnp.concatenate(results, axis=1).astype(BF16)
        for index, core in enumerate((other, s)):
            chosen = perm[:, span(core)]
            ordered = dot(chosen, done, (((0,), (1,)), ((), ())))
            out32[index, :, h * group : (h + 1) * group, :] = ordered.reshape(own, group, width)

    for copy in loads[2:]:
        copy.wait()

    def suffixes(low, high):
        with scope("suffix"):

            @pl.loop(low, high)
            def _(i):
                suffix(i * 4)

    ahead = (3 * own * (n - 1 - j)) // (32 * n)
    suffixes(0, ahead)
    with scope("barrier"):
        pl.semaphore_wait(barrier, 2 * n - 1)
    for copy in query_copies(0) + sys_copies(0) + task_copies(0):
        copy.start()
    suffixes(ahead, 1)
    for copy in query_copies(1):
        copy.start()
    suffixes(1, 2)
    with scope("drain"):
        for copy in query_copies(0):
            copy.wait_send()
    for copy in sys_copies(1) + task_copies(1):
        copy.start()
    suffixes(2, own // 4 - 1)
    arrive(0)
    system(0)
    with scope("block"):
        gather(0)
        found = sweep(task_items(0) + cross_items(0))
        keep_cross(0, found["cross"], found["task"])
        keep_task(0, found["task"])
        for copy in ret_copies(0, 0) + ret_copies(0, 1) + mate_copies(0):
            copy.start()
    arrive(1)
    with scope("task"):
        gather(1)
        keep_task(1, sweep(task_items(1))["task"])
        for copy in mate_copies(1):
            copy.start()
    system(1)
    with scope("cross"):
        task = (base_o[1], base_e[1, 0:1])
        keep_cross(1, sweep(cross_items(1))["cross"], task)
        for copy in ret_copies(1, 0) + ret_copies(1, 1):
            copy.start()
    suffixes(own // 4 - 1, own // 4)
    for copy in exchange():
        copy.start()
    with scope("home"):
        home()
    with scope("sxwait"):
        for copy in exchange():
            copy.wait_recv()
    with scope("fold"):
        for h in range(per):
            fold(h)
    for h in range(per):
        with scope("finish"):
            finish(h)
    outb[...] = out32[0].astype(BF16)
    give = remote(outb, out_ref.at[:, pl.ds(first, mine), :], fin_send, fin_recv, {"sub": other})
    give.start()
    out_ref[:, pl.ds(first, mine), :] = out32[1].astype(BF16)

    for copy in sys_copies(0) + task_copies(0) + query_copies(1) + sys_copies(1) + task_copies(1):
        copy.wait_send()
    for h in range(per):
        for copy in mate_copies(h) + ret_copies(h, 0) + ret_copies(h, 1):
            copy.wait_send()
    for copy in exchange():
        copy.wait_send()
    with scope("tail"):
        give.wait_send()
        theirs = out_ref.at[:, pl.ds(pl.multiple_of(other * mine, 16), mine), :]
        remote(outb, theirs, fin_send, fin_recv, {"sub": other}).wait_recv()


def paired_call(n, args, out_shape):
    queries, sys_keys, _, task_keys, _, suffix_keys, _, task_ids, _ = args
    rows, heads, width = queries.shape
    kv = sys_keys.shape[0]
    group = heads // kv
    own = suffix_keys.shape[0]
    per = kv // 2
    mine = heads // 2
    cell = CAP * group
    tile = 2 * cell
    lanes = n * cell
    dma = pltpu.SemaphoreType.DMA
    inputs = (*args[:7], task_ids.reshape(1, rows), args[8])
    return pl.pallas_call(
        functools.partial(paired, n),
        out_shape=out_shape,
        in_specs=[pl.BlockSpec(memory_space=pl.ANY)] * 9,
        out_specs=pl.BlockSpec(memory_space=pltpu.VMEM),
        scratch_shapes=[
            pltpu.VMEM((rows, mine, width), BF16),
            pltpu.VMEM((own, heads, width), BF16),
            pltpu.VMEM((1, rows), jnp.int32),
            pltpu.SMEM((own,), jnp.int32),
            pltpu.VMEM((lanes, rows * group), BF16),
            pltpu.VMEM((per, lanes, width), BF16),
            pltpu.VMEM((per, lanes, width), BF16),
            pltpu.VMEM((per, lanes, width), BF16),
            pltpu.VMEM((2, per, n * sys_keys.shape[1], width), BF16),
            pltpu.VMEM((2, per, 2 * task_keys.shape[2], width), BF16),
            pltpu.VMEM(suffix_keys.shape, BF16),
            pltpu.VMEM(suffix_keys.shape, BF16),
            pltpu.VMEM((2, own, mine, width), F32),
            pltpu.VMEM((2, own, mine, width), F32),
            pltpu.VMEM((own, mine, width), F32),
            pltpu.VMEM((own, mine, width), F32),
            pltpu.VMEM((per, width, lanes), F32),
            pltpu.VMEM((per, 8, lanes), F32),
            pltpu.VMEM((per, 2, width, tile), BF16),
            pltpu.VMEM((per, 2, 8, tile), F32),
            pltpu.VMEM((per, 2, width, tile), BF16),
            pltpu.VMEM((per, 2, 8, tile), F32),
            pltpu.VMEM((per, width // 2, tile), BF16),
            pltpu.VMEM((per, 8, tile), F32),
            pltpu.VMEM((per, width // 2, tile), BF16),
            pltpu.VMEM((per, 8, tile), F32),
            pltpu.VMEM((2, own, mine, width), F32),
            pltpu.VMEM((own, mine, width), BF16),
            dma((4,)),
            dma((2,)),
            dma((2, per)),
            dma((2, own)),
            dma((2, per)),
            dma((2, per)),
            dma((2, per, 3)),
            dma((2, per, 3)),
            dma((per, 5)),
            dma((per, 5)),
            dma((2, per, 3)),
            dma((2, per, 3)),
            dma((2,)),
            dma((2,)),
            dma,
            dma,
        ],
        compiler_params=pltpu.CompilerParams(
            collective_id=0, has_side_effects=True, vmem_limit_bytes=48 * 1024 * 1024
        ),
        name="cascade",
    )(*(pltpu.with_memory_space_constraint(x, pltpu.HBM) for x in inputs))


def body(
    queries,
    sys_keys,
    sys_values,
    task_keys,
    task_values,
    suffix_keys,
    suffix_values,
    task_ids,
    suffix_len,
):
    n = lax.axis_size("kv")
    rows, heads, width = queries.shape
    kv = sys_keys.shape[0]
    group = heads // kv
    own = suffix_keys.shape[0]
    lanes = n * CAP * group
    half = lanes // 2
    out_shape = jax.ShapeDtypeStruct((own, heads, width), BF16)
    if n == 4 and rows == n * CAP and kv % 2 == 0 and 2 * CAP * group == width:
        args = (
            queries,
            sys_keys,
            sys_values,
            task_keys,
            task_values,
            suffix_keys,
            suffix_values,
            task_ids,
            suffix_len,
        )
        return paired_call(n, args, out_shape)
    vmem = pl.BlockSpec(memory_space=pltpu.VMEM)
    anywhere = pl.BlockSpec(memory_space=pl.ANY)
    dma = pltpu.SemaphoreType.DMA
    return pl.pallas_call(
        functools.partial(kernel, n),
        out_shape=out_shape,
        in_specs=[vmem] * 3 + [anywhere] * 4 + [vmem, pl.BlockSpec(memory_space=pltpu.SMEM)],
        out_specs=vmem,
        scratch_shapes=[
            pltpu.VMEM(task_keys.shape[1:], BF16),
            pltpu.VMEM(task_values.shape[1:], BF16),
            pltpu.VMEM(suffix_keys.shape, BF16),
            pltpu.VMEM(suffix_values.shape, BF16),
            pltpu.VMEM((n, kv, lanes, width), BF16),
            pltpu.VMEM((n, 2, kv, width, half), F32),
            pltpu.VMEM((n, 2, kv, 8, half), F32),
            pltpu.VMEM((n, kv, width, half), F32),
            pltpu.VMEM((n, kv, 8, half), F32),
            pltpu.VMEM((n, kv, width, half), BF16),
            pltpu.VMEM((n, kv, 8, half), F32),
            pltpu.VMEM((2, n, kv, width, half), BF16),
            pltpu.VMEM((2, n, kv, 8, half), F32),
            pltpu.VMEM((2, kv, width, half), F32),
            pltpu.VMEM((2, kv, 8, half), F32),
            pltpu.VMEM((own, heads, width), F32),
            pltpu.VMEM((own, heads, width), F32),
            pltpu.VMEM((own, heads, width), F32),
            dma((2,)),
            dma((2, own)),
            dma((2, kv)),
            dma((n, kv)),
            dma((n, kv)),
            dma((n, kv)),
            dma((n, kv)),
            dma((2, n, kv)),
            dma((2, n, kv)),
            dma((2, n, kv)),
            dma((2, 2, n, kv)),
            dma((2, kv)),
            dma((2, kv)),
        ],
        compiler_params=pltpu.CompilerParams(
            collective_id=0, has_side_effects=True, vmem_limit_bytes=60 * 1024 * 1024
        ),
        name="cascade",
    )(
        queries,
        sys_keys,
        sys_values,
        task_keys,
        task_values,
        suffix_keys,
        suffix_values,
        task_ids.reshape(1, rows),
        suffix_len,
    )


def solution(mesh):
    in_specs = (
        P(("replica", "kv"), "head", None),
        P(("replica", "head"), ("kv", "sub"), None),
        P(("replica", "head"), ("kv", "sub"), None),
        P(("replica", "kv"), "head", "sub", None),
        P(("replica", "kv"), "head", "sub", None),
        P(("replica", "kv", "sub"), "head", None, None),
        P(("replica", "kv", "sub"), "head", None, None),
        P(("replica", "kv")),
        P(("replica", "kv", "sub")),
    )
    out_specs = P(("replica", "kv", "sub"), "head", None)
    return jax.shard_map(body, mesh=mesh, in_specs=in_specs, out_specs=out_specs, check_vma=False)
```

```python
import functools
import math

import jax
import jax.numpy as jnp
from jax import lax
from jax.experimental import pallas as pl
from jax.experimental.pallas import tpu as pltpu
from jax.sharding import PartitionSpec as P

CAP = 8
NEGATIVE = -1e30
MESH = pl.DeviceIdType.MESH
NT = (((1,), (1,)), ((), ()))
TN = (((0,), (0,)), ((), ()))
F32 = jnp.float32
BF16 = jnp.bfloat16


def dot(a, b, dims=(((1,), (0,)), ((), ()))):
    return lax.dot_general(a, b, dims, preferred_element_type=F32)


def merge(first, second):
    top = jnp.maximum(first[1], second[1])
    a = jnp.exp(first[1] - top)
    b = jnp.exp(second[1] - top)
    total = a + b
    inverse = 1.0 / total
    return first[0] * (a * inverse) + second[0] * (b * inverse), top + jnp.log(total)


def iota(shape, dim):
    return lax.broadcasted_iota(jnp.int32, shape, dim)


def selected(value, picks, pieces):
    out = None
    for _ in range(pieces):
        part = value.astype(BF16)
        value = value - part.astype(F32)
        term = dot(part, picks)
        out = term if out is None else out + term
    return out


def kernel(
    n,
    q_ref,
    sk_ref,
    sv_ref,
    tk_hbm,
    tv_hbm,
    uk_hbm,
    uv_hbm,
    ids_ref,
    len_ref,
    out_ref,
    tk,
    tv,
    uk,
    uv,
    qbuf,
    part_o,
    part_e,
    swap_o,
    swap_e,
    send_o,
    send_e,
    chain_o,
    chain_e,
    fin_o,
    fin_e,
    suf_o,
    suf_e,
    out32,
    task_sem,
    suf_sem,
    own_send,
    z_send,
    z_recv,
    d_send,
    d_recv,
    swap_send,
    swap_recv,
    chain_send,
    chain_recv,
    fin_send,
    fin_recv,
):
    rows, heads, width = q_ref.shape
    kv = sk_ref.shape[0]
    group = heads // kv
    own = uk.shape[0]
    lanes = qbuf.shape[2]
    half = lanes // 2
    task_rows = CAP * group
    scale = 1.0 / math.sqrt(width)
    j = lax.axis_index("kv")
    s = lax.axis_index("sub")
    other = 1 - s

    task_copies = []
    for index, (hbm, buf) in enumerate(((tk_hbm, tk), (tv_hbm, tv))):
        copy = pltpu.make_async_copy(hbm.at[0], buf, task_sem.at[index])
        copy.start()
        task_copies.append(copy)

    def suffix_copies(i):
        return (
            pltpu.make_async_copy(uk_hbm.at[i], uk.at[i], suf_sem.at[0, i]),
            pltpu.make_async_copy(uv_hbm.at[i], uv.at[i], suf_sem.at[1, i]),
        )

    @pl.loop(0, own)
    def _(i):
        for copy in suffix_copies(i):
            copy.start()

    barrier = pltpu.get_barrier_semaphore()
    pl.semaphore_signal(barrier, inc=1, device_id={"sub": other}, device_id_type=MESH)

    @pl.when(j > 0)
    def _():
        pl.semaphore_signal(barrier, inc=1, device_id={"kv": j - 1}, device_id_type=MESH)

    @pl.when(j < n - 1)
    def _():
        pl.semaphore_signal(barrier, inc=1, device_id={"kv": j + 1}, device_id_type=MESH)

    ids = ids_ref[...].astype(F32)
    wide = jnp.broadcast_to(ids, (rows, rows))
    down, across = iota((rows, rows), 0), iota((rows, rows), 1)
    ids_column = jnp.sum(jnp.where(down == across, wide, 0.0), axis=1, keepdims=True)
    same = jnp.where((ids_column == wide) & (down < across), 1.0, 0.0)
    places = ids * CAP + jnp.sum(same, axis=0, keepdims=True)
    places8 = jnp.broadcast_to(places, (8, rows)).astype(BF16)

    def spread(count, base):
        shape = (rows, count * group)
        pick = jnp.where(iota(shape, 0) == base + iota(shape, 1) // group, 1.0, 0.0).astype(BF16)
        row = dot(places8, pick)[0:1].astype(jnp.int32)
        shape = (lanes, count * group)
        down, across = iota(shape, 0), iota(shape, 1)
        hit = (down // group == row) & (down % group == across % group)
        return jnp.where(hit, 1.0, 0.0).astype(BF16)

    everyone = spread(rows, 0)
    wide_query = q_ref[...].astype(F32)
    for k in range(kv):
        mine = wide_query[:, k * group : (k + 1) * group, :].reshape(rows * group, width)
        qbuf[j, k] = dot(everyone, mine.astype(BF16)).astype(BF16)

    pl.semaphore_wait(
        barrier, 1 + jnp.where(j > 0, 1, 0) + jnp.where(j < n - 1, 1, 0)
    )

    def query_view(p, k, h):
        return qbuf.at[p, k, pl.ds(pl.multiple_of(h * half, 16), half), :]

    def query_copy(p, k, send_sem, recv_sem, device):
        return pltpu.make_async_remote_copy(
            src_ref=query_view(p, k, s),
            dst_ref=query_view(p, k, s),
            send_sem=send_sem,
            recv_sem=recv_sem,
            device_id=device,
            device_id_type=MESH,
        )

    def own_copy(k, d):
        return query_copy(j, k, own_send.at[d, k], z_recv.at[j, k], {"kv": j + 2 * d - 1})

    def relay_copy(p, k, d):
        return query_copy(p, k, z_send.at[p, k], z_recv.at[p, k], {"kv": j + 1 - 2 * d})

    def side_copy(p, k):
        return query_copy(p, k, d_send.at[p, k], d_recv.at[p, k], {"sub": other})

    def side_arrival(p, k):
        return pltpu.make_async_remote_copy(
            src_ref=query_view(p, k, other),
            dst_ref=query_view(p, k, other),
            send_sem=d_send.at[p, k],
            recv_sem=d_recv.at[p, k],
            device_id={"sub": other},
            device_id_type=MESH,
        )

    @pl.when(j < n - 1)
    def _():
        for k in range(kv):
            own_copy(k, 1).start()

    @pl.when(j > 0)
    def _():
        for k in range(kv):
            own_copy(k, 0).start()

    def swap_copies(p, k):
        return tuple(
            pltpu.make_async_remote_copy(
                src_ref=src.at[p, other, k],
                dst_ref=dst.at[p, k],
                send_sem=swap_send.at[index, p, k],
                recv_sem=swap_recv.at[index, p, k],
                device_id={"sub": other},
                device_id_type=MESH,
            )
            for index, (src, dst) in enumerate(((part_o, swap_o), (part_e, swap_e)))
        )

    def chain_copies(p, k, d, target=None):
        target = {"kv": j + 2 * d - 1} if target is None else target
        return tuple(
            pltpu.make_async_remote_copy(
                src_ref=src.at[p, k],
                dst_ref=dst.at[d, p, k],
                send_sem=chain_send.at[index, p, k],
                recv_sem=chain_recv.at[index, d, p, k],
                device_id=target,
                device_id_type=MESH,
            )
            for index, (src, dst) in enumerate(((send_o, chain_o), (send_e, chain_e)))
        )

    def fin_copies(k):
        return tuple(
            pltpu.make_async_remote_copy(
                src_ref=buf.at[s, k],
                dst_ref=buf.at[s, k],
                send_sem=fin_send.at[index, k],
                recv_sem=fin_recv.at[index, k],
                device_id={"sub": other},
                device_id_type=MESH,
            )
            for index, buf in enumerate((fin_o, fin_e))
        )

    def fin_arrivals(k):
        return tuple(
            pltpu.make_async_remote_copy(
                src_ref=buf.at[other, k],
                dst_ref=buf.at[other, k],
                send_sem=fin_send.at[index, k],
                recv_sem=fin_recv.at[index, k],
                device_id={"sub": other},
                device_id_type=MESH,
            )
            for index, buf in enumerate((fin_o, fin_e))
        )

    def attend(keys, values, query):
        scores = dot(keys, query, NT)
        maxima = jnp.max(scores, axis=0, keepdims=True)
        weights = jnp.exp((scores - maxima) * scale)
        totals = jnp.sum(weights, axis=0, keepdims=True)
        return maxima * scale, totals, dot(values, weights.astype(BF16), TN)

    def block(p, d):
        def arrive(k):
            @pl.when(jnp.logical_not(beyond(d)))
            def _():
                relay_copy(p, k, d).wait_recv()
                side_copy(p, k).start()

        for k in range(kv):
            if d is not None:
                for later in ([0, 1] if k == 0 else [k + 1]):
                    if later < kv:
                        arrive(later)
                side_arrival(p, k).wait_recv()
            top, total, numerator = attend(sk_ref[k], sv_ref[k], qbuf[p, k])
            system = (numerator * (1.0 / total), top + jnp.log(total))
            picked = qbuf[p, k, pl.ds(pl.multiple_of(j * task_rows, 16), task_rows), :]
            doubled = jnp.concatenate([picked, picked], axis=0)
            tokens = tk.shape[1]
            step = min(512, tokens)
            state = None
            for base in range(0, tokens, step):
                part = attend(
                    tk[k, base : base + step, :], tv[k, base : base + step, :], doubled
                )
                if state is None:
                    state = part
                else:
                    top = jnp.maximum(state[0], part[0])
                    a, b = jnp.exp(state[0] - top), jnp.exp(part[0] - top)
                    state = (top, state[1] * a + part[1] * b, state[2] * a + part[2] * b)
            top, total, numerator = state
            repeats = lanes // (2 * task_rows)
            place = iota((1, lanes), 1) // task_rows == j
            task = (
                jnp.concatenate([numerator * (1.0 / total)] * repeats, axis=1),
                jnp.where(
                    place, jnp.concatenate([top + jnp.log(total)] * repeats, axis=1), NEGATIVE
                ),
            )
            result, level = merge(system, task)
            for h in range(2):
                part_o[p, h, k] = result[:, h * half : (h + 1) * half]
                part_e[p, h, k] = jnp.broadcast_to(level[:, h * half : (h + 1) * half], (8, half))
            for copy in swap_copies(p, k):
                copy.start()

    def chip_part(p, k):
        return merge(
            (part_o[p, s, k], part_e[p, s, k][0:1]), (swap_o[p, k], swap_e[p, k][0:1])
        )

    def chain_part(d, p, k):
        return chain_o[d, p, k].astype(F32), chain_e[d, p, k][0:1]

    def finish(p, d, incoming):
        for k in range(kv):
            for copy in swap_copies(p, k):
                copy.wait_recv()
            state = chip_part(p, k)
            if incoming:
                for copy in chain_copies(p, k, d):
                    copy.wait_recv()
                state = merge(state, chain_part(d, p, k))
            send_o[p, k] = state[0].astype(BF16)
            send_e[p, k] = jnp.broadcast_to(state[1], (8, half))
            for copy in chain_copies(p, k, d):
                copy.start()

    def suffix(i):
        for copy in suffix_copies(i):
            copy.wait()
        query = q_ref[s * own + i].astype(F32)
        length = len_ref[i]
        scores = jnp.concatenate(
            [
                dot(query[k * group : (k + 1) * group].astype(BF16), uk[i, k], NT)
                for k in range(kv)
            ],
            axis=0,
        )
        usable = iota(scores.shape, 1) < length
        scores = jnp.where(usable, scores, NEGATIVE)
        maxima = jnp.max(scores, axis=1, keepdims=True)
        weights = jnp.where(usable, jnp.exp((scores - maxima) * scale), 0.0)
        totals = jnp.sum(weights, axis=1, keepdims=True)
        numerator = jnp.concatenate(
            [
                dot(weights[k * group : (k + 1) * group].astype(BF16), uv[i, k])
                for k in range(kv)
            ],
            axis=0,
        )
        suf_o[i] = numerator * (1.0 / totals)
        suf_e[i] = jnp.broadcast_to(maxima * scale + jnp.log(totals), (heads, width))

    def source(t, d):
        return j + (2 * d - 1) * t

    def valid(t, d):
        p = source(t, d)
        return (p >= 0) & (p < n)

    def beyond(d):
        return jnp.where(d == 0, j < n - 1, j > 0)

    early = own // 4
    late, turns = own - early, 2 * n - 2

    @pl.loop(0, early)
    def _(i):
        suffix(i)

    for copy in task_copies:
        copy.wait()

    @pl.loop(1, n)
    def _(t):
        for k in range(kv):
            for d in range(2):

                @pl.when(valid(t, d) & beyond(d))
                def _(d=d, k=k):
                    p = source(t, d)
                    relay_copy(p, k, d).wait_recv()
                    relay_copy(p, k, d).start()
                    side_copy(p, k).start()

        @pl.loop(0, 2)
        def _(d):
            @pl.when(valid(t, d))
            def _():
                block(source(t, d), d)

        for d in range(2):

            @pl.when(valid(t, d) & jnp.logical_not(beyond(d)))
            def _(d=d):
                finish(source(t, d), d, False)

    block(j, None)

    @pl.loop(1, 2 * n - 1)
    def _(turn):
        @pl.loop(early + (turn - 1) * late // turns, early + turn * late // turns)
        def _(i):
            suffix(i)

        low = 2 * (n - 1) - j - turn

        @pl.when((low >= 0) & (low < j) & (j < n - 1))
        def _():
            finish(low, 0, True)

        high = turn - j

        @pl.when((high > j) & (high < n) & (j > 0))
        def _():
            finish(high, 1, True)

    for k in range(kv):
        for copy in swap_copies(j, k):
            copy.wait_recv()
        value, level = chip_part(j, k)
        fin_o[s, k] = value
        fin_e[s, k] = jnp.broadcast_to(level, (8, half))
    chosen = spread(own, s * own)
    for k in range(kv):
        for d in range(2):

            @pl.when(j < n - 1 if d == 0 else j > 0)
            def _(d=d, k=k):
                for copy in chain_copies(j, k, d, {"kv": j + 1 - 2 * d}):
                    copy.wait_recv()
                state = merge((fin_o[s, k], fin_e[s, k][0:1]), chain_part(d, j, k))
                fin_o[s, k] = state[0]
                fin_e[s, k] = jnp.broadcast_to(state[1], (8, half))

        for copy in fin_copies(k):
            copy.start()
    for k in range(kv):
        for copy in fin_arrivals(k):
            copy.wait_recv()
        value = jnp.concatenate([fin_o[0, k], fin_o[1, k]], axis=1)
        level = jnp.concatenate([fin_e[0, k], fin_e[1, k]], axis=1)
        value = selected(value, chosen, 2).T
        level = jnp.broadcast_to(selected(level, chosen, 3)[0:1], (width, own * group)).T
        near = slice(k * group, (k + 1) * group)
        suffix_state = (
            suf_o[:, near, :].reshape(own * group, width),
            suf_e[:, near, :].reshape(own * group, width),
        )
        attended = merge((value, level), suffix_state)[0]
        out32[:, near, :] = attended.reshape(own, group, width)
    out_ref[...] = out32[...].astype(BF16)

    for k in range(kv):

        @pl.when(j < n - 1)
        def _(k=k):
            own_copy(k, 1).wait_send()

        @pl.when(j > 0)
        def _(k=k):
            own_copy(k, 0).wait_send()

        for copy in swap_copies(j, k) + fin_copies(k):
            copy.wait_send()

    @pl.loop(1, n)
    def _(t):
        for d in range(2):

            @pl.when(valid(t, d))
            def _(d=d):
                p = source(t, d)
                for k in range(kv):

                    @pl.when(beyond(d))
                    def _(k=k):
                        relay_copy(p, k, d).wait_send()

                    side_copy(p, k).wait_send()
                    for copy in swap_copies(p, k) + chain_copies(p, k, d):
                        copy.wait_send()


exp2 = jnp.exp2
scope = jax.named_scope


def blend(parts):
    top = parts[0][1]
    for part in parts[1:]:
        top = jnp.maximum(top, part[1])
    factors = [exp2(part[1] - top) for part in parts]
    total = sum(factors[1:], factors[0])
    inverse = 1.0 / total
    value = parts[0][0] * (factors[0] * inverse)
    for part, factor in zip(parts[1:], factors[1:]):
        value = value + part[0] * (factor * inverse)
    return value, top + jnp.log2(total)


def paired(
    n,
    q_hbm,
    sk_hbm,
    sv_hbm,
    tk_hbm,
    tv_hbm,
    uk_hbm,
    uv_hbm,
    ids_hbm,
    len_hbm,
    out_ref,
    qh,
    qo,
    ids_ref,
    len_ref,
    perm,
    qs,
    tq,
    qx,
    sysb,
    taskb,
    uk,
    uv,
    suf_o,
    suf_e,
    sib_o,
    sib_e,
    base_o,
    base_e,
    rs_o,
    rs_e,
    rr_o,
    rr_e,
    ps_o,
    ps_e,
    pr_o,
    pr_e,
    out32,
    outb,
    load_sem,
    sysl_sem,
    task_sem,
    suf_sem,
    tx_send,
    tx_recv,
    sys_send,
    sys_recv,
    q_send,
    q_recv,
    ret_send,
    ret_recv,
    sx_send,
    sx_recv,
    fin_send,
    fin_recv,
):
    rows = qh.shape[0]
    own, heads, width = qo.shape
    mine = qh.shape[1]
    kv = uk.shape[1]
    group = heads // kv
    per = kv // 2
    half_n = n // 2
    cell = CAP * group
    lanes = 2 * half_n * cell
    tile = 2 * cell
    shard = sk_hbm.shape[1]
    stretch = tk_hbm.shape[2]
    scale = math.log2(math.e) / math.sqrt(width)
    j = lax.axis_index("kv")
    s = lax.axis_index("sub")
    other = 1 - s
    side = j // half_n
    e = j % half_n
    mate = j + 1 - 2 * e
    far = (1 - side) * half_n

    barrier = pltpu.get_barrier_semaphore()
    pl.semaphore_signal(barrier, inc=1, device_id={"sub": other}, device_id_type=MESH)
    for d in range(1, n):
        target = lax.rem(j + d, n)
        for z in range(2):
            pl.semaphore_signal(
                barrier, inc=1, device_id={"kv": target, "sub": z}, device_id_type=MESH
            )

    def remote(src, dst, send_sem, recv_sem, device):
        return pltpu.make_async_remote_copy(
            src_ref=src,
            dst_ref=dst,
            send_sem=send_sem,
            recv_sem=recv_sem,
            device_id=device,
            device_id_type=MESH,
        )

    first = pl.multiple_of(s * mine, 16)
    loads = [
        pltpu.make_async_copy(ids_hbm, ids_ref, load_sem.at[0]),
        pltpu.make_async_copy(q_hbm.at[:, pl.ds(first, mine), :], qh, load_sem.at[1]),
        pltpu.make_async_copy(q_hbm.at[pl.ds(s * own, own)], qo, load_sem.at[2]),
        pltpu.make_async_copy(len_hbm, len_ref, load_sem.at[3]),
    ]
    for copy in loads:
        copy.start()

    def spot(chip, core):
        return pl.ds(pl.multiple_of((2 * chip + core) * shard, 128), shard)

    sys_local = [
        pltpu.make_async_copy(
            hbm.at[pl.ds(s * per, per)], sysb.at[kind, :, spot(e, s), :], sysl_sem.at[kind]
        )
        for kind, hbm in enumerate((sk_hbm, sv_hbm))
    ]
    for copy in sys_local:
        copy.start()

    def strip(core):
        return pl.ds(pl.multiple_of(core * stretch, 128), stretch)

    task_local = [
        [
            pltpu.make_async_copy(
                hbm.at[0, s * per + h], taskb.at[kind, h, strip(s), :], task_sem.at[kind, h]
            )
            for kind, hbm in enumerate((tk_hbm, tv_hbm))
        ]
        for h in range(per)
    ]
    def suffix_copies(i):
        return (
            pltpu.make_async_copy(uk_hbm.at[i], uk.at[i], suf_sem.at[0, i]),
            pltpu.make_async_copy(uv_hbm.at[i], uv.at[i], suf_sem.at[1, i]),
        )

    def fetch(low, high):
        @pl.loop(low, high)
        def _(i):
            for copy in suffix_copies(i):
                copy.start()

    fetch(0, own // 4)
    for copies in task_local:
        for copy in copies:
            copy.start()
    fetch(own // 4, own)

    with scope("ids"):
        loads[0].wait()
    ids = ids_ref[...]
    names = ids.astype(F32)
    wide = jnp.broadcast_to(names, (rows, rows))
    down, across = iota((rows, rows), 0), iota((rows, rows), 1)
    column = jnp.sum(jnp.where(down == across, wide, 0.0), axis=1, keepdims=True)
    same = jnp.where((column == wide) & (down < across), 1.0, 0.0)
    seat = ids % half_n
    seat = jnp.where(ids // half_n == side, half_n - 1 - seat, half_n + seat)
    places = seat.astype(F32) * CAP + jnp.sum(same, axis=0, keepdims=True)
    places8 = jnp.broadcast_to(places, (8, rows)).astype(BF16)
    shape = (rows, rows * group)
    pick = jnp.where(iota(shape, 0) == iota(shape, 1) // group, 1.0, 0.0).astype(BF16)
    row = dot(places8, pick)[0:1].astype(jnp.int32)
    shape = (lanes, rows * group)
    down, across = iota(shape, 0), iota(shape, 1)
    hit = (down // group == row) & (down % group == across % group)
    perm[...] = jnp.where(hit, 1.0, 0.0).astype(BF16)
    loads[1].wait()
    wide_query = qh[...].astype(F32)
    for h in range(per):
        flat = wide_query[:, h * group : (h + 1) * group, :].reshape(rows * group, width)
        qs[h] = dot(perm[...], flat.astype(BF16)).astype(BF16)

    def cellat(base):
        return pl.ds(pl.multiple_of(base, 16), cell)

    for h in range(per):
        tq[h, cellat((1 - e) * cell), :] = qs[h, cellat((1 - e) * cell), :]

    def query_copies(h):
        copies = [
            remote(
                qs.at[h, cellat(e * cell), :],
                tq.at[h, cellat(tile + e * cell), :],
                q_send.at[h, 0],
                q_recv.at[h, 0],
                {"kv": mate},
            )
        ]
        for c in range(2):
            copies.append(
                remote(
                    qs.at[h, cellat(tile + c * cell), :],
                    tq.at[h, cellat(e * tile + c * cell), :],
                    q_send.at[h, 1 + c],
                    q_recv.at[h, 1 + e],
                    {"kv": far + c},
                )
            )
            copies.append(
                remote(
                    qs.at[h, cellat((1 - c) * cell), :],
                    qx.at[h, cellat(e * tile + (1 - c) * cell), :],
                    q_send.at[h, 3 + c],
                    q_recv.at[h, 3 + e],
                    {"kv": far + c},
                )
            )
        return copies

    def query_arrivals(h):
        places = [(tq, tile + (1 - e) * cell)]
        places += [(tq, i * tile + e * cell) for i in range(2)]
        places += [(qx, i * tile + (1 - e) * cell) for i in range(2)]
        return [
            remote(
                buf.at[h, cellat(base), :],
                buf.at[h, cellat(base), :],
                q_send.at[h, index],
                q_recv.at[h, index],
                {"kv": mate},
            )
            for index, (buf, base) in enumerate(places)
        ]

    def sys_copies(h):
        copies = []
        for kind, hbm in enumerate((sk_hbm, sv_hbm)):
            dst = sysb.at[kind, h, spot(e, s), :]
            copies.append(
                remote(
                    hbm.at[other * per + h],
                    dst,
                    sys_send.at[kind, h, 0],
                    sys_recv.at[kind, h, 0],
                    {"sub": other},
                )
            )
            for z in range(2):
                copies.append(
                    remote(
                        hbm.at[z * per + h],
                        dst,
                        sys_send.at[kind, h, 1 + z],
                        sys_recv.at[kind, h, 1 + s],
                        {"kv": mate, "sub": z},
                    )
                )
        return copies

    def sys_arrivals(h):
        out = []
        for kind in range(2):
            for index, (chip, core) in enumerate(((e, other), (1 - e, 0), (1 - e, 1))):
                ref = sysb.at[kind, h, spot(chip, core), :]
                out.append(
                    remote(
                        ref,
                        ref,
                        sys_send.at[kind, h, index],
                        sys_recv.at[kind, h, index],
                        {"sub": other},
                    )
                )
        return out

    def task_copies(h):
        return [
            remote(
                hbm.at[0, other * per + h],
                taskb.at[kind, h, strip(s), :],
                tx_send.at[kind, h],
                tx_recv.at[kind, h],
                {"sub": other},
            )
            for kind, hbm in enumerate((tk_hbm, tv_hbm))
        ]

    def task_arrivals(h):
        return [
            remote(
                taskb.at[kind, h, strip(other), :],
                taskb.at[kind, h, strip(other), :],
                tx_send.at[kind, h],
                tx_recv.at[kind, h],
                {"sub": other},
            )
            for kind in range(2)
        ]

    def suffix(base):
        picks = range(4)
        for r in picks:
            for copy in suffix_copies(base + r):
                copy.wait()
        scores = []
        for r in picks:
            query = qo[base + r].astype(F32)
            scores.append(
                jnp.concatenate(
                    [
                        dot(
                            query[k * group : (k + 1) * group].astype(BF16),
                            uk[base + r, k],
                            NT,
                        )
                        for k in range(kv)
                    ],
                    axis=0,
                )
            )
        states = []
        for r in picks:
            usable = iota(scores[r].shape, 1) < len_ref[base + r]
            masked = jnp.where(usable, scores[r], NEGATIVE)
            maxima = jnp.max(masked, axis=1, keepdims=True)
            weights = jnp.where(usable, exp2((masked - maxima) * scale), 0.0)
            states.append((maxima, weights, jnp.sum(weights, axis=1, keepdims=True)))
        for r in picks:
            maxima, weights, totals = states[r]
            numerator = jnp.concatenate(
                [
                    dot(weights[k * group : (k + 1) * group].astype(BF16), uv[base + r, k])
                    for k in range(kv)
                ],
                axis=0,
            )
            value = numerator * (1.0 / totals)
            level = jnp.broadcast_to(maxima * scale + jnp.log2(totals), (heads, width))
            for z in range(2):
                suf_o[z, base + r] = value[z * mine : (z + 1) * mine]
                suf_e[z, base + r] = level[z * mine : (z + 1) * mine]

    def sweep(items):
        states = {}
        ahead = [dot(item[1](), item[3], NT) for item in items[:1]]
        for index, (name, _, values, _) in enumerate(items):
            scores = ahead.pop(0)
            if index + 1 < len(items):
                item = items[index + 1]
                ahead.append(dot(item[1](), item[3], NT))
            top = jnp.max(scores, axis=0, keepdims=True)
            weights = exp2((scores - top) * scale)
            total = jnp.sum(weights, axis=0, keepdims=True)
            part = (top * scale, total, dot(values(), weights.astype(BF16), TN))
            if name in states:
                state = states[name]
                top = jnp.maximum(state[0], part[0])
                a, b = exp2(state[0] - top), exp2(part[0] - top)
                part = (top, state[1] * a + part[1] * b, state[2] * a + part[2] * b)
            states[name] = part
        return {
            name: (numerator * (1.0 / total), top + jnp.log2(total))
            for name, (top, total, numerator) in states.items()
        }

    def pieces(name, buf, h, step, query):
        tokens = buf.shape[2]
        step = min(step, tokens)
        return [
            (
                name,
                lambda base=base: buf[0, h, base : base + step, :],
                lambda base=base: buf[1, h, base : base + step, :],
                query,
            )
            for base in range(0, tokens, step)
        ]

    zone = iota((1, tile), 1) // cell

    slim = (slice(None), pl.ds(0, 1))

    def ret_copies(h, i):
        return [
            remote(
                src.at[h, i, slim[index]],
                dst.at[h, e, slim[index]],
                ret_send.at[index, h, i],
                ret_recv.at[index, h, e],
                {"kv": far + i},
            )
            for index, (src, dst) in enumerate(((rs_o, rr_o), (rs_e, rr_e)))
        ]

    def ret_arrivals(h, i):
        return [
            remote(
                dst.at[h, i, slim[index]],
                dst.at[h, i, slim[index]],
                ret_send.at[index, h, i],
                ret_recv.at[index, h, i],
                {"kv": far + i},
            )
            for index, dst in enumerate((rr_o, rr_e))
        ]

    def mate_copies(h):
        return [
            remote(
                src.at[h, slim[index]],
                dst.at[h, slim[index]],
                ret_send.at[index, h, 2],
                ret_recv.at[index, h, 2],
                {"kv": mate},
            )
            for index, (src, dst) in enumerate(((ps_o, pr_o), (ps_e, pr_e)))
        ]

    def arrive(h):
        with scope("local"):
            for copy in task_local[h]:
                copy.wait()
        with scope("queries"):
            for copy in query_arrivals(h):
                copy.wait_recv()
        with scope("taskwait"):
            for copy in task_arrivals(h):
                copy.wait_recv()

    def system(h):
        with scope("syswait"):
            if h == 0:
                for copy in sys_local:
                    copy.wait()
            for copy in sys_arrivals(h):
                copy.wait_recv()

    def gather(h):
        for i in range(2):
            qx[h, cellat(i * tile + e * cell), :] = tq[h, cellat(i * tile + e * cell), :]

    def task_items(h):
        return pieces("task", taskb, h, 1024, tq[h])

    def cross_items(h):
        return pieces("cross", sysb, h, 1024, qx[h])

    def keep_task(h, found):
        value, level = found
        base_o[h] = value
        base_e[h] = jnp.broadcast_to(level, (8, lanes))
        near = value[:, tile:]
        packed = jnp.where(
            zone == 1 - e,
            near[: width // 2],
            pltpu.roll(near[width // 2 :], cell, 1),
        )
        ps_o[h] = packed.astype(BF16)
        ps_e[h] = jnp.broadcast_to(level[:, tile:], (8, tile))

    def keep_cross(h, found, task):
        value, level = found
        for i in range(2):
            cut = slice(i * tile, (i + 1) * tile)
            task_level = jnp.where(zone == e, task[1][:, cut], NEGATIVE)
            merged = blend([(value[:, cut], level[:, cut]), (task[0][:, cut], task_level)])
            rs_o[h, i] = merged[0].astype(BF16)
            rs_e[h, i] = jnp.broadcast_to(merged[1], (8, tile))

    def home():
        items = []
        for h in range(per):
            items += pieces(h, sysb, h, 1024, qs[h])
        found = sweep(items)
        for h in range(per):
            value, level = found[h]
            task_level = jnp.where(zone == 1 - e, base_e[h, 0:1, :tile], NEGATIVE)
            merged = blend([(value[:, :tile], level[:, :tile]), (base_o[h, :, :tile], task_level)])
            base_o[h] = jnp.concatenate([merged[0], value[:, tile:]], axis=1)
            base_e[h] = jnp.broadcast_to(
                jnp.concatenate([merged[1], level[:, tile:]], axis=1), (8, lanes)
            )

    def exchange():
        return [
            remote(
                src.at[other],
                dst,
                sx_send.at[index],
                sx_recv.at[index],
                {"sub": other},
            )
            for index, (src, dst) in enumerate(((suf_o, sib_o), (suf_e, sib_e)))
        ]

    def span(core):
        return pl.ds(pl.multiple_of(core * own * group, 128), own * group)

    def fold(h):
        value, level = None, None
        for core, o_ref, e_ref in ((s, suf_o.at[s], suf_e.at[s]), (other, sib_o, sib_e)):
            near = slice(h * group, (h + 1) * group)
            rest = o_ref[:, near, :].reshape(own * group, width)
            tall = e_ref[:, near, :].reshape(own * group, width)
            chosen = perm[:, span(core)]
            for _ in range(2):
                piece = rest.astype(BF16)
                rest = rest - piece.astype(F32)
                term = dot(piece, chosen, (((0,), (1,)), ((), ())))
                value = term if value is None else value + term
            tall = tall.T[0:1]
            term = jnp.sum(jnp.where(chosen.astype(F32) > 0.5, tall, 0.0), axis=1, keepdims=True)
            level = term if level is None else level + term
        level = jnp.broadcast_to(level, (lanes, width)).T[0:1]
        merged = blend([(base_o[h], base_e[h][0:1]), (value, level)])
        base_o[h] = merged[0]
        base_e[h] = jnp.broadcast_to(merged[1], (8, lanes))

    def finish(h):
        with scope("retwait"):
            for copy in ret_arrivals(h, 0) + ret_arrivals(h, 1) + mate_copies(h):
                copy.wait_recv()
        low = zone == 0
        far_o = [rr_o[h, c].astype(F32) for c in range(2)]
        far_e = [rr_e[h, c][0:1] for c in range(2)]
        crossed = [
            (jnp.where(low, far_o[1], far_o[0]), jnp.where(low, far_e[1], far_e[0])),
            (jnp.where(low, far_o[0], far_o[1]), jnp.where(low, far_e[0], far_e[1])),
        ]
        packed = pr_o[h].astype(F32)
        near = jnp.concatenate([packed, pltpu.roll(packed, cell, 1)], axis=0)
        near_level = jnp.where(zone == e, pr_e[h][0:1], NEGATIVE)
        results = []
        for i in range(2):
            cut = slice(i * tile, (i + 1) * tile)
            parts = [(base_o[h, :, cut], base_e[h, 0:1, cut]), crossed[i]]
            if i == 0:
                parts.append((near, near_level))
            results.append(blend(parts)[0])
        done = jnp.concatenate(results, axis=1).astype(BF16)
        for index, core in enumerate((other, s)):
            chosen = perm[:, span(core)]
            ordered = dot(chosen, done, (((0,), (1,)), ((), ())))
            out32[index, :, h * group : (h + 1) * group, :] = ordered.reshape(own, group, width)

    for copy in loads[2:]:
        copy.wait()

    def suffixes(low, high):
        with scope("suffix"):

            @pl.loop(low, high)
            def _(i):
                suffix(i * 4)

    ahead = (3 * own * (n - 1 - j)) // (32 * n)
    suffixes(0, ahead)
    with scope("barrier"):
        pl.semaphore_wait(barrier, 2 * n - 1)
    rank = e + side

    @pl.when(rank != 9)
    def _():
        for copy in query_copies(0):
            copy.start()

    @pl.when(rank == 0)
    def _():
        for copy in query_copies(1):
            copy.start()

    for copy in sys_copies(0) + task_copies(0):
        copy.start()

    @pl.when(rank == 9)
    def _():
        for copy in query_copies(0):
            copy.start()

    suffixes(ahead, 2)
    @pl.when(rank != 0)
    def _():
        for copy in query_copies(1):
            copy.start()

    suffixes(2, 2)
    for copy in sys_copies(1) + task_copies(1):
        copy.start()
    suffixes(2, own // 4 - 1)
    arrive(0)
    system(0)
    with scope("block"):
        gather(0)
        found = sweep(task_items(0) + cross_items(0))
        keep_cross(0, found["cross"], found["task"])
        keep_task(0, found["task"])
        for copy in ret_copies(0, 0) + ret_copies(0, 1) + mate_copies(0):
            copy.start()
    arrive(1)
    with scope("task"):
        gather(1)
        keep_task(1, sweep(task_items(1))["task"])
        for copy in mate_copies(1):
            copy.start()
    system(1)
    with scope("cross"):
        task = (base_o[1], base_e[1, 0:1])
        keep_cross(1, sweep(cross_items(1))["cross"], task)
        for copy in ret_copies(1, 0) + ret_copies(1, 1):
            copy.start()
    suffixes(own // 4 - 1, own // 4)
    for copy in exchange():
        copy.start()
    with scope("home"):
        home()
    with scope("sxwait"):
        for copy in exchange():
            copy.wait_recv()
    with scope("fold"):
        for h in range(per):
            fold(h)
    for h in range(per):
        with scope("finish"):
            finish(h)
    outb[...] = out32[0].astype(BF16)
    give = remote(outb, out_ref.at[:, pl.ds(first, mine), :], fin_send, fin_recv, {"sub": other})
    give.start()
    out_ref[:, pl.ds(first, mine), :] = out32[1].astype(BF16)

    for copy in query_copies(0) + sys_copies(0) + task_copies(0) + query_copies(1) + sys_copies(1) + task_copies(1):
        copy.wait_send()
    for h in range(per):
        for copy in mate_copies(h) + ret_copies(h, 0) + ret_copies(h, 1):
            copy.wait_send()
    for copy in exchange():
        copy.wait_send()
    with scope("tail"):
        give.wait_send()
        theirs = out_ref.at[:, pl.ds(pl.multiple_of(other * mine, 16), mine), :]
        remote(outb, theirs, fin_send, fin_recv, {"sub": other}).wait_recv()


def paired_call(n, args, out_shape):
    queries, sys_keys, _, task_keys, _, suffix_keys, _, task_ids, _ = args
    rows, heads, width = queries.shape
    kv = sys_keys.shape[0]
    group = heads // kv
    own = suffix_keys.shape[0]
    per = kv // 2
    mine = heads // 2
    cell = CAP * group
    tile = 2 * cell
    lanes = n * cell
    dma = pltpu.SemaphoreType.DMA
    inputs = (*args[:7], task_ids.reshape(1, rows), args[8])
    return pl.pallas_call(
        functools.partial(paired, n),
        out_shape=out_shape,
        in_specs=[pl.BlockSpec(memory_space=pl.ANY)] * 9,
        out_specs=pl.BlockSpec(memory_space=pltpu.VMEM),
        scratch_shapes=[
            pltpu.VMEM((rows, mine, width), BF16),
            pltpu.VMEM((own, heads, width), BF16),
            pltpu.VMEM((1, rows), jnp.int32),
            pltpu.SMEM((own,), jnp.int32),
            pltpu.VMEM((lanes, rows * group), BF16),
            pltpu.VMEM((per, lanes, width), BF16),
            pltpu.VMEM((per, lanes, width), BF16),
            pltpu.VMEM((per, lanes, width), BF16),
            pltpu.VMEM((2, per, n * sys_keys.shape[1], width), BF16),
            pltpu.VMEM((2, per, 2 * task_keys.shape[2], width), BF16),
            pltpu.VMEM(suffix_keys.shape, BF16),
            pltpu.VMEM(suffix_keys.shape, BF16),
            pltpu.VMEM((2, own, mine, width), F32),
            pltpu.VMEM((2, own, mine, width), F32),
            pltpu.VMEM((own, mine, width), F32),
            pltpu.VMEM((own, mine, width), F32),
            pltpu.VMEM((per, width, lanes), F32),
            pltpu.VMEM((per, 8, lanes), F32),
            pltpu.VMEM((per, 2, width, tile), BF16),
            pltpu.VMEM((per, 2, 8, tile), F32),
            pltpu.VMEM((per, 2, width, tile), BF16),
            pltpu.VMEM((per, 2, 8, tile), F32),
            pltpu.VMEM((per, width // 2, tile), BF16),
            pltpu.VMEM((per, 8, tile), F32),
            pltpu.VMEM((per, width // 2, tile), BF16),
            pltpu.VMEM((per, 8, tile), F32),
            pltpu.VMEM((2, own, mine, width), F32),
            pltpu.VMEM((own, mine, width), BF16),
            dma((4,)),
            dma((2,)),
            dma((2, per)),
            dma((2, own)),
            dma((2, per)),
            dma((2, per)),
            dma((2, per, 3)),
            dma((2, per, 3)),
            dma((per, 5)),
            dma((per, 5)),
            dma((2, per, 3)),
            dma((2, per, 3)),
            dma((2,)),
            dma((2,)),
            dma,
            dma,
        ],
        compiler_params=pltpu.CompilerParams(
            collective_id=0, has_side_effects=True, vmem_limit_bytes=48 * 1024 * 1024
        ),
        name="cascade",
    )(*(pltpu.with_memory_space_constraint(x, pltpu.HBM) for x in inputs))


def body(
    queries,
    sys_keys,
    sys_values,
    task_keys,
    task_values,
    suffix_keys,
    suffix_values,
    task_ids,
    suffix_len,
):
    n = lax.axis_size("kv")
    rows, heads, width = queries.shape
    kv = sys_keys.shape[0]
    group = heads // kv
    own = suffix_keys.shape[0]
    lanes = n * CAP * group
    half = lanes // 2
    out_shape = jax.ShapeDtypeStruct((own, heads, width), BF16)
    if n == 4 and rows == n * CAP and kv % 2 == 0 and 2 * CAP * group == width:
        args = (
            queries,
            sys_keys,
            sys_values,
            task_keys,
            task_values,
            suffix_keys,
            suffix_values,
            task_ids,
            suffix_len,
        )
        return paired_call(n, args, out_shape)
    vmem = pl.BlockSpec(memory_space=pltpu.VMEM)
    anywhere = pl.BlockSpec(memory_space=pl.ANY)
    dma = pltpu.SemaphoreType.DMA
    return pl.pallas_call(
        functools.partial(kernel, n),
        out_shape=out_shape,
        in_specs=[vmem] * 3 + [anywhere] * 4 + [vmem, pl.BlockSpec(memory_space=pltpu.SMEM)],
        out_specs=vmem,
        scratch_shapes=[
            pltpu.VMEM(task_keys.shape[1:], BF16),
            pltpu.VMEM(task_values.shape[1:], BF16),
            pltpu.VMEM(suffix_keys.shape, BF16),
            pltpu.VMEM(suffix_values.shape, BF16),
            pltpu.VMEM((n, kv, lanes, width), BF16),
            pltpu.VMEM((n, 2, kv, width, half), F32),
            pltpu.VMEM((n, 2, kv, 8, half), F32),
            pltpu.VMEM((n, kv, width, half), F32),
            pltpu.VMEM((n, kv, 8, half), F32),
            pltpu.VMEM((n, kv, width, half), BF16),
            pltpu.VMEM((n, kv, 8, half), F32),
            pltpu.VMEM((2, n, kv, width, half), BF16),
            pltpu.VMEM((2, n, kv, 8, half), F32),
            pltpu.VMEM((2, kv, width, half), F32),
            pltpu.VMEM((2, kv, 8, half), F32),
            pltpu.VMEM((own, heads, width), F32),
            pltpu.VMEM((own, heads, width), F32),
            pltpu.VMEM((own, heads, width), F32),
            dma((2,)),
            dma((2, own)),
            dma((2, kv)),
            dma((n, kv)),
            dma((n, kv)),
            dma((n, kv)),
            dma((n, kv)),
            dma((2, n, kv)),
            dma((2, n, kv)),
            dma((2, n, kv)),
            dma((2, 2, n, kv)),
            dma((2, kv)),
            dma((2, kv)),
        ],
        compiler_params=pltpu.CompilerParams(
            collective_id=0, has_side_effects=True, vmem_limit_bytes=60 * 1024 * 1024
        ),
        name="cascade",
    )(
        queries,
        sys_keys,
        sys_values,
        task_keys,
        task_values,
        suffix_keys,
        suffix_values,
        task_ids.reshape(1, rows),
        suffix_len,
    )


def solution(mesh):
    in_specs = (
        P(("replica", "kv"), "head", None),
        P(("replica", "head"), ("kv", "sub"), None),
        P(("replica", "head"), ("kv", "sub"), None),
        P(("replica", "kv"), "head", "sub", None),
        P(("replica", "kv"), "head", "sub", None),
        P(("replica", "kv", "sub"), "head", None, None),
        P(("replica", "kv", "sub"), "head", None, None),
        P(("replica", "kv")),
        P(("replica", "kv", "sub")),
    )
    out_specs = P(("replica", "kv", "sub"), "head", None)
    return jax.shard_map(body, mesh=mesh, in_specs=in_specs, out_specs=out_specs, check_vma=False)
```

```python
import functools
import math

import jax
import jax.numpy as jnp
from jax import lax
from jax.experimental import pallas as pl
from jax.experimental.pallas import tpu as pltpu
from jax.sharding import PartitionSpec as P

CAP = 8
NEGATIVE = -1e30
MESH = pl.DeviceIdType.MESH
NT = (((1,), (1,)), ((), ()))
TN = (((0,), (0,)), ((), ()))
F32 = jnp.float32
BF16 = jnp.bfloat16


def dot(a, b, dims=(((1,), (0,)), ((), ()))):
    return lax.dot_general(a, b, dims, preferred_element_type=F32)


def merge(first, second):
    top = jnp.maximum(first[1], second[1])
    a = jnp.exp(first[1] - top)
    b = jnp.exp(second[1] - top)
    total = a + b
    inverse = 1.0 / total
    return first[0] * (a * inverse) + second[0] * (b * inverse), top + jnp.log(total)


def iota(shape, dim):
    return lax.broadcasted_iota(jnp.int32, shape, dim)


def selected(value, picks, pieces):
    out = None
    for _ in range(pieces):
        part = value.astype(BF16)
        value = value - part.astype(F32)
        term = dot(part, picks)
        out = term if out is None else out + term
    return out


def kernel(
    n,
    q_ref,
    sk_ref,
    sv_ref,
    tk_hbm,
    tv_hbm,
    uk_hbm,
    uv_hbm,
    ids_ref,
    len_ref,
    out_ref,
    tk,
    tv,
    uk,
    uv,
    qbuf,
    part_o,
    part_e,
    swap_o,
    swap_e,
    send_o,
    send_e,
    chain_o,
    chain_e,
    fin_o,
    fin_e,
    suf_o,
    suf_e,
    out32,
    task_sem,
    suf_sem,
    own_send,
    z_send,
    z_recv,
    d_send,
    d_recv,
    swap_send,
    swap_recv,
    chain_send,
    chain_recv,
    fin_send,
    fin_recv,
):
    rows, heads, width = q_ref.shape
    kv = sk_ref.shape[0]
    group = heads // kv
    own = uk.shape[0]
    lanes = qbuf.shape[2]
    half = lanes // 2
    task_rows = CAP * group
    scale = 1.0 / math.sqrt(width)
    j = lax.axis_index("kv")
    s = lax.axis_index("sub")
    other = 1 - s

    task_copies = []
    for index, (hbm, buf) in enumerate(((tk_hbm, tk), (tv_hbm, tv))):
        copy = pltpu.make_async_copy(hbm.at[0], buf, task_sem.at[index])
        copy.start()
        task_copies.append(copy)

    def suffix_copies(i):
        return (
            pltpu.make_async_copy(uk_hbm.at[i], uk.at[i], suf_sem.at[0, i]),
            pltpu.make_async_copy(uv_hbm.at[i], uv.at[i], suf_sem.at[1, i]),
        )

    @pl.loop(0, own)
    def _(i):
        for copy in suffix_copies(i):
            copy.start()

    barrier = pltpu.get_barrier_semaphore()
    pl.semaphore_signal(barrier, inc=1, device_id={"sub": other}, device_id_type=MESH)

    @pl.when(j > 0)
    def _():
        pl.semaphore_signal(barrier, inc=1, device_id={"kv": j - 1}, device_id_type=MESH)

    @pl.when(j < n - 1)
    def _():
        pl.semaphore_signal(barrier, inc=1, device_id={"kv": j + 1}, device_id_type=MESH)

    ids = ids_ref[...].astype(F32)
    wide = jnp.broadcast_to(ids, (rows, rows))
    down, across = iota((rows, rows), 0), iota((rows, rows), 1)
    ids_column = jnp.sum(jnp.where(down == across, wide, 0.0), axis=1, keepdims=True)
    same = jnp.where((ids_column == wide) & (down < across), 1.0, 0.0)
    places = ids * CAP + jnp.sum(same, axis=0, keepdims=True)
    places8 = jnp.broadcast_to(places, (8, rows)).astype(BF16)

    def spread(count, base):
        shape = (rows, count * group)
        pick = jnp.where(iota(shape, 0) == base + iota(shape, 1) // group, 1.0, 0.0).astype(BF16)
        row = dot(places8, pick)[0:1].astype(jnp.int32)
        shape = (lanes, count * group)
        down, across = iota(shape, 0), iota(shape, 1)
        hit = (down // group == row) & (down % group == across % group)
        return jnp.where(hit, 1.0, 0.0).astype(BF16)

    everyone = spread(rows, 0)
    wide_query = q_ref[...].astype(F32)
    for k in range(kv):
        mine = wide_query[:, k * group : (k + 1) * group, :].reshape(rows * group, width)
        qbuf[j, k] = dot(everyone, mine.astype(BF16)).astype(BF16)

    pl.semaphore_wait(
        barrier, 1 + jnp.where(j > 0, 1, 0) + jnp.where(j < n - 1, 1, 0)
    )

    def query_view(p, k, h):
        return qbuf.at[p, k, pl.ds(pl.multiple_of(h * half, 16), half), :]

    def query_copy(p, k, send_sem, recv_sem, device):
        return pltpu.make_async_remote_copy(
            src_ref=query_view(p, k, s),
            dst_ref=query_view(p, k, s),
            send_sem=send_sem,
            recv_sem=recv_sem,
            device_id=device,
            device_id_type=MESH,
        )

    def own_copy(k, d):
        return query_copy(j, k, own_send.at[d, k], z_recv.at[j, k], {"kv": j + 2 * d - 1})

    def relay_copy(p, k, d):
        return query_copy(p, k, z_send.at[p, k], z_recv.at[p, k], {"kv": j + 1 - 2 * d})

    def side_copy(p, k):
        return query_copy(p, k, d_send.at[p, k], d_recv.at[p, k], {"sub": other})

    def side_arrival(p, k):
        return pltpu.make_async_remote_copy(
            src_ref=query_view(p, k, other),
            dst_ref=query_view(p, k, other),
            send_sem=d_send.at[p, k],
            recv_sem=d_recv.at[p, k],
            device_id={"sub": other},
            device_id_type=MESH,
        )

    @pl.when(j < n - 1)
    def _():
        for k in range(kv):
            own_copy(k, 1).start()

    @pl.when(j > 0)
    def _():
        for k in range(kv):
            own_copy(k, 0).start()

    def swap_copies(p, k):
        return tuple(
            pltpu.make_async_remote_copy(
                src_ref=src.at[p, other, k],
                dst_ref=dst.at[p, k],
                send_sem=swap_send.at[index, p, k],
                recv_sem=swap_recv.at[index, p, k],
                device_id={"sub": other},
                device_id_type=MESH,
            )
            for index, (src, dst) in enumerate(((part_o, swap_o), (part_e, swap_e)))
        )

    def chain_copies(p, k, d, target=None):
        target = {"kv": j + 2 * d - 1} if target is None else target
        return tuple(
            pltpu.make_async_remote_copy(
                src_ref=src.at[p, k],
                dst_ref=dst.at[d, p, k],
                send_sem=chain_send.at[index, p, k],
                recv_sem=chain_recv.at[index, d, p, k],
                device_id=target,
                device_id_type=MESH,
            )
            for index, (src, dst) in enumerate(((send_o, chain_o), (send_e, chain_e)))
        )

    def fin_copies(k):
        return tuple(
            pltpu.make_async_remote_copy(
                src_ref=buf.at[s, k],
                dst_ref=buf.at[s, k],
                send_sem=fin_send.at[index, k],
                recv_sem=fin_recv.at[index, k],
                device_id={"sub": other},
                device_id_type=MESH,
            )
            for index, buf in enumerate((fin_o, fin_e))
        )

    def fin_arrivals(k):
        return tuple(
            pltpu.make_async_remote_copy(
                src_ref=buf.at[other, k],
                dst_ref=buf.at[other, k],
                send_sem=fin_send.at[index, k],
                recv_sem=fin_recv.at[index, k],
                device_id={"sub": other},
                device_id_type=MESH,
            )
            for index, buf in enumerate((fin_o, fin_e))
        )

    def attend(keys, values, query):
        scores = dot(keys, query, NT)
        maxima = jnp.max(scores, axis=0, keepdims=True)
        weights = jnp.exp((scores - maxima) * scale)
        totals = jnp.sum(weights, axis=0, keepdims=True)
        return maxima * scale, totals, dot(values, weights.astype(BF16), TN)

    def block(p, d):
        def arrive(k):
            @pl.when(jnp.logical_not(beyond(d)))
            def _():
                relay_copy(p, k, d).wait_recv()
                side_copy(p, k).start()

        for k in range(kv):
            if d is not None:
                for later in ([0, 1] if k == 0 else [k + 1]):
                    if later < kv:
                        arrive(later)
                side_arrival(p, k).wait_recv()
            top, total, numerator = attend(sk_ref[k], sv_ref[k], qbuf[p, k])
            system = (numerator * (1.0 / total), top + jnp.log(total))
            picked = qbuf[p, k, pl.ds(pl.multiple_of(j * task_rows, 16), task_rows), :]
            doubled = jnp.concatenate([picked, picked], axis=0)
            tokens = tk.shape[1]
            step = min(512, tokens)
            state = None
            for base in range(0, tokens, step):
                part = attend(
                    tk[k, base : base + step, :], tv[k, base : base + step, :], doubled
                )
                if state is None:
                    state = part
                else:
                    top = jnp.maximum(state[0], part[0])
                    a, b = jnp.exp(state[0] - top), jnp.exp(part[0] - top)
                    state = (top, state[1] * a + part[1] * b, state[2] * a + part[2] * b)
            top, total, numerator = state
            repeats = lanes // (2 * task_rows)
            place = iota((1, lanes), 1) // task_rows == j
            task = (
                jnp.concatenate([numerator * (1.0 / total)] * repeats, axis=1),
                jnp.where(
                    place, jnp.concatenate([top + jnp.log(total)] * repeats, axis=1), NEGATIVE
                ),
            )
            result, level = merge(system, task)
            for h in range(2):
                part_o[p, h, k] = result[:, h * half : (h + 1) * half]
                part_e[p, h, k] = jnp.broadcast_to(level[:, h * half : (h + 1) * half], (8, half))
            for copy in swap_copies(p, k):
                copy.start()

    def chip_part(p, k):
        return merge(
            (part_o[p, s, k], part_e[p, s, k][0:1]), (swap_o[p, k], swap_e[p, k][0:1])
        )

    def chain_part(d, p, k):
        return chain_o[d, p, k].astype(F32), chain_e[d, p, k][0:1]

    def finish(p, d, incoming):
        for k in range(kv):
            for copy in swap_copies(p, k):
                copy.wait_recv()
            state = chip_part(p, k)
            if incoming:
                for copy in chain_copies(p, k, d):
                    copy.wait_recv()
                state = merge(state, chain_part(d, p, k))
            send_o[p, k] = state[0].astype(BF16)
            send_e[p, k] = jnp.broadcast_to(state[1], (8, half))
            for copy in chain_copies(p, k, d):
                copy.start()

    def suffix(i):
        for copy in suffix_copies(i):
            copy.wait()
        query = q_ref[s * own + i].astype(F32)
        length = len_ref[i]
        scores = jnp.concatenate(
            [
                dot(query[k * group : (k + 1) * group].astype(BF16), uk[i, k], NT)
                for k in range(kv)
            ],
            axis=0,
        )
        usable = iota(scores.shape, 1) < length
        scores = jnp.where(usable, scores, NEGATIVE)
        maxima = jnp.max(scores, axis=1, keepdims=True)
        weights = jnp.where(usable, jnp.exp((scores - maxima) * scale), 0.0)
        totals = jnp.sum(weights, axis=1, keepdims=True)
        numerator = jnp.concatenate(
            [
                dot(weights[k * group : (k + 1) * group].astype(BF16), uv[i, k])
                for k in range(kv)
            ],
            axis=0,
        )
        suf_o[i] = numerator * (1.0 / totals)
        suf_e[i] = jnp.broadcast_to(maxima * scale + jnp.log(totals), (heads, width))

    def source(t, d):
        return j + (2 * d - 1) * t

    def valid(t, d):
        p = source(t, d)
        return (p >= 0) & (p < n)

    def beyond(d):
        return jnp.where(d == 0, j < n - 1, j > 0)

    early = own // 4
    late, turns = own - early, 2 * n - 2

    @pl.loop(0, early)
    def _(i):
        suffix(i)

    for copy in task_copies:
        copy.wait()

    @pl.loop(1, n)
    def _(t):
        for k in range(kv):
            for d in range(2):

                @pl.when(valid(t, d) & beyond(d))
                def _(d=d, k=k):
                    p = source(t, d)
                    relay_copy(p, k, d).wait_recv()
                    relay_copy(p, k, d).start()
                    side_copy(p, k).start()

        @pl.loop(0, 2)
        def _(d):
            @pl.when(valid(t, d))
            def _():
                block(source(t, d), d)

        for d in range(2):

            @pl.when(valid(t, d) & jnp.logical_not(beyond(d)))
            def _(d=d):
                finish(source(t, d), d, False)

    block(j, None)

    @pl.loop(1, 2 * n - 1)
    def _(turn):
        @pl.loop(early + (turn - 1) * late // turns, early + turn * late // turns)
        def _(i):
            suffix(i)

        low = 2 * (n - 1) - j - turn

        @pl.when((low >= 0) & (low < j) & (j < n - 1))
        def _():
            finish(low, 0, True)

        high = turn - j

        @pl.when((high > j) & (high < n) & (j > 0))
        def _():
            finish(high, 1, True)

    for k in range(kv):
        for copy in swap_copies(j, k):
            copy.wait_recv()
        value, level = chip_part(j, k)
        fin_o[s, k] = value
        fin_e[s, k] = jnp.broadcast_to(level, (8, half))
    chosen = spread(own, s * own)
    for k in range(kv):
        for d in range(2):

            @pl.when(j < n - 1 if d == 0 else j > 0)
            def _(d=d, k=k):
                for copy in chain_copies(j, k, d, {"kv": j + 1 - 2 * d}):
                    copy.wait_recv()
                state = merge((fin_o[s, k], fin_e[s, k][0:1]), chain_part(d, j, k))
                fin_o[s, k] = state[0]
                fin_e[s, k] = jnp.broadcast_to(state[1], (8, half))

        for copy in fin_copies(k):
            copy.start()
    for k in range(kv):
        for copy in fin_arrivals(k):
            copy.wait_recv()
        value = jnp.concatenate([fin_o[0, k], fin_o[1, k]], axis=1)
        level = jnp.concatenate([fin_e[0, k], fin_e[1, k]], axis=1)
        value = selected(value, chosen, 2).T
        level = jnp.broadcast_to(selected(level, chosen, 3)[0:1], (width, own * group)).T
        near = slice(k * group, (k + 1) * group)
        suffix_state = (
            suf_o[:, near, :].reshape(own * group, width),
            suf_e[:, near, :].reshape(own * group, width),
        )
        attended = merge((value, level), suffix_state)[0]
        out32[:, near, :] = attended.reshape(own, group, width)
    out_ref[...] = out32[...].astype(BF16)

    for k in range(kv):

        @pl.when(j < n - 1)
        def _(k=k):
            own_copy(k, 1).wait_send()

        @pl.when(j > 0)
        def _(k=k):
            own_copy(k, 0).wait_send()

        for copy in swap_copies(j, k) + fin_copies(k):
            copy.wait_send()

    @pl.loop(1, n)
    def _(t):
        for d in range(2):

            @pl.when(valid(t, d))
            def _(d=d):
                p = source(t, d)
                for k in range(kv):

                    @pl.when(beyond(d))
                    def _(k=k):
                        relay_copy(p, k, d).wait_send()

                    side_copy(p, k).wait_send()
                    for copy in swap_copies(p, k) + chain_copies(p, k, d):
                        copy.wait_send()


exp2 = jnp.exp2
scope = jax.named_scope


def blend(parts):
    top = parts[0][1]
    for part in parts[1:]:
        top = jnp.maximum(top, part[1])
    factors = [exp2(part[1] - top) for part in parts]
    total = sum(factors[1:], factors[0])
    inverse = 1.0 / total
    value = parts[0][0] * (factors[0] * inverse)
    for part, factor in zip(parts[1:], factors[1:]):
        value = value + part[0] * (factor * inverse)
    return value, top + jnp.log2(total)


def paired(
    n,
    q_hbm,
    sk_hbm,
    sv_hbm,
    tk_hbm,
    tv_hbm,
    uk_hbm,
    uv_hbm,
    ids_hbm,
    len_hbm,
    out_ref,
    qh,
    qo,
    ids_ref,
    len_ref,
    perm,
    qs,
    tq,
    qx,
    sysb,
    taskb,
    uk,
    uv,
    suf_o,
    suf_e,
    sib_o,
    sib_e,
    base_o,
    base_e,
    rs_o,
    rs_e,
    rr_o,
    rr_e,
    ps_o,
    ps_e,
    pr_o,
    pr_e,
    out32,
    outb,
    load_sem,
    sysl_sem,
    task_sem,
    suf_sem,
    tx_send,
    tx_recv,
    sys_send,
    sys_recv,
    q_send,
    q_recv,
    ret_send,
    ret_recv,
    sx_send,
    sx_recv,
    fin_send,
    fin_recv,
):
    rows = qh.shape[0]
    own, heads, width = qo.shape
    mine = qh.shape[1]
    kv = uk.shape[1]
    group = heads // kv
    per = kv // 2
    half_n = n // 2
    cell = CAP * group
    lanes = 2 * half_n * cell
    tile = 2 * cell
    shard = sk_hbm.shape[1]
    stretch = tk_hbm.shape[2]
    scale = math.log2(math.e) / math.sqrt(width)
    j = lax.axis_index("kv")
    s = lax.axis_index("sub")
    other = 1 - s
    side = j // half_n
    e = j % half_n
    mate = j + 1 - 2 * e
    far = (1 - side) * half_n

    barrier = pltpu.get_barrier_semaphore()
    pl.semaphore_signal(barrier, inc=1, device_id={"sub": other}, device_id_type=MESH)
    for d in range(1, n):
        target = lax.rem(j + d, n)
        for z in range(2):
            pl.semaphore_signal(
                barrier, inc=1, device_id={"kv": target, "sub": z}, device_id_type=MESH
            )

    def remote(src, dst, send_sem, recv_sem, device):
        return pltpu.make_async_remote_copy(
            src_ref=src,
            dst_ref=dst,
            send_sem=send_sem,
            recv_sem=recv_sem,
            device_id=device,
            device_id_type=MESH,
        )

    first = pl.multiple_of(s * mine, 16)
    loads = [
        pltpu.make_async_copy(ids_hbm, ids_ref, load_sem.at[0]),
        pltpu.make_async_copy(q_hbm.at[:, pl.ds(first, mine), :], qh, load_sem.at[1]),
        pltpu.make_async_copy(q_hbm.at[pl.ds(s * own, own)], qo, load_sem.at[2]),
        pltpu.make_async_copy(len_hbm, len_ref, load_sem.at[3]),
    ]
    for copy in loads:
        copy.start()

    def spot(chip, core):
        return pl.ds(pl.multiple_of((2 * chip + core) * shard, 128), shard)

    sys_local = [
        pltpu.make_async_copy(
            hbm.at[pl.ds(s * per, per)], sysb.at[kind, :, spot(e, s), :], sysl_sem.at[kind]
        )
        for kind, hbm in enumerate((sk_hbm, sv_hbm))
    ]
    for copy in sys_local:
        copy.start()

    def strip(core):
        return pl.ds(pl.multiple_of(core * stretch, 128), stretch)

    task_local = [
        [
            pltpu.make_async_copy(
                hbm.at[0, s * per + h], taskb.at[kind, h, strip(s), :], task_sem.at[kind, h]
            )
            for kind, hbm in enumerate((tk_hbm, tv_hbm))
        ]
        for h in range(per)
    ]
    def suffix_copies(i):
        return (
            pltpu.make_async_copy(uk_hbm.at[i], uk.at[i], suf_sem.at[0, i]),
            pltpu.make_async_copy(uv_hbm.at[i], uv.at[i], suf_sem.at[1, i]),
        )

    def fetch(low, high):
        @pl.loop(low, high)
        def _(i):
            for copy in suffix_copies(i):
                copy.start()

    fetch(0, own // 4)
    for copies in task_local:
        for copy in copies:
            copy.start()
    fetch(own // 4, own)

    with scope("ids"):
        loads[0].wait()
    ids = ids_ref[...]
    names = ids.astype(F32)
    wide = jnp.broadcast_to(names, (rows, rows))
    down, across = iota((rows, rows), 0), iota((rows, rows), 1)
    column = jnp.sum(jnp.where(down == across, wide, 0.0), axis=1, keepdims=True)
    same = jnp.where((column == wide) & (down < across), 1.0, 0.0)
    seat = ids % half_n
    seat = jnp.where(ids // half_n == side, half_n - 1 - seat, half_n + seat)
    places = seat.astype(F32) * CAP + jnp.sum(same, axis=0, keepdims=True)
    places8 = jnp.broadcast_to(places, (8, rows)).astype(BF16)
    shape = (rows, rows * group)
    pick = jnp.where(iota(shape, 0) == iota(shape, 1) // group, 1.0, 0.0).astype(BF16)
    row = dot(places8, pick)[0:1].astype(jnp.int32)
    shape = (lanes, rows * group)
    down, across = iota(shape, 0), iota(shape, 1)
    hit = (down // group == row) & (down % group == across % group)
    perm[...] = jnp.where(hit, 1.0, 0.0).astype(BF16)
    loads[1].wait()
    wide_query = qh[...].astype(F32)
    for h in range(per):
        flat = wide_query[:, h * group : (h + 1) * group, :].reshape(rows * group, width)
        qs[h] = dot(perm[...], flat.astype(BF16)).astype(BF16)

    def cellat(base):
        return pl.ds(pl.multiple_of(base, 16), cell)

    for h in range(per):
        tq[h, cellat((1 - e) * cell), :] = qs[h, cellat((1 - e) * cell), :]

    def query_copies(h):
        copies = [
            remote(
                qs.at[h, cellat(e * cell), :],
                tq.at[h, cellat(tile + e * cell), :],
                q_send.at[h, 0],
                q_recv.at[h, 0],
                {"kv": mate},
            )
        ]
        for c in range(2):
            copies.append(
                remote(
                    qs.at[h, cellat(tile + c * cell), :],
                    tq.at[h, cellat(e * tile + c * cell), :],
                    q_send.at[h, 1 + c],
                    q_recv.at[h, 1 + e],
                    {"kv": far + c},
                )
            )
            copies.append(
                remote(
                    qs.at[h, cellat((1 - c) * cell), :],
                    qx.at[h, cellat(e * tile + (1 - c) * cell), :],
                    q_send.at[h, 3 + c],
                    q_recv.at[h, 3 + e],
                    {"kv": far + c},
                )
            )
        return copies

    def query_arrivals(h):
        places = [(tq, tile + (1 - e) * cell)]
        places += [(tq, i * tile + e * cell) for i in range(2)]
        places += [(qx, i * tile + (1 - e) * cell) for i in range(2)]
        return [
            remote(
                buf.at[h, cellat(base), :],
                buf.at[h, cellat(base), :],
                q_send.at[h, index],
                q_recv.at[h, index],
                {"kv": mate},
            )
            for index, (buf, base) in enumerate(places)
        ]

    def sys_copies(h):
        copies = []
        for kind, hbm in enumerate((sk_hbm, sv_hbm)):
            dst = sysb.at[kind, h, spot(e, s), :]
            copies.append(
                remote(
                    hbm.at[other * per + h],
                    dst,
                    sys_send.at[kind, h, 0],
                    sys_recv.at[kind, h, 0],
                    {"sub": other},
                )
            )
            for z in range(2):
                copies.append(
                    remote(
                        hbm.at[z * per + h],
                        dst,
                        sys_send.at[kind, h, 1 + z],
                        sys_recv.at[kind, h, 1 + s],
                        {"kv": mate, "sub": z},
                    )
                )
        return copies

    def sys_arrivals(h):
        out = []
        for kind in range(2):
            for index, (chip, core) in enumerate(((e, other), (1 - e, 0), (1 - e, 1))):
                ref = sysb.at[kind, h, spot(chip, core), :]
                out.append(
                    remote(
                        ref,
                        ref,
                        sys_send.at[kind, h, index],
                        sys_recv.at[kind, h, index],
                        {"sub": other},
                    )
                )
        return out

    def task_copies(h):
        return [
            remote(
                hbm.at[0, other * per + h],
                taskb.at[kind, h, strip(s), :],
                tx_send.at[kind, h],
                tx_recv.at[kind, h],
                {"sub": other},
            )
            for kind, hbm in enumerate((tk_hbm, tv_hbm))
        ]

    def task_arrivals(h):
        return [
            remote(
                taskb.at[kind, h, strip(other), :],
                taskb.at[kind, h, strip(other), :],
                tx_send.at[kind, h],
                tx_recv.at[kind, h],
                {"sub": other},
            )
            for kind in range(2)
        ]

    def suffix(base):
        picks = range(4)
        for r in picks:
            for copy in suffix_copies(base + r):
                copy.wait()
        scores = []
        for r in picks:
            query = qo[base + r].astype(F32)
            scores.append(
                jnp.concatenate(
                    [
                        dot(
                            query[k * group : (k + 1) * group].astype(BF16),
                            uk[base + r, k],
                            NT,
                        )
                        for k in range(kv)
                    ],
                    axis=0,
                )
            )
        states = []
        for r in picks:
            usable = iota(scores[r].shape, 1) < len_ref[base + r]
            masked = jnp.where(usable, scores[r], NEGATIVE)
            maxima = jnp.max(masked, axis=1, keepdims=True)
            weights = jnp.where(usable, exp2((masked - maxima) * scale), 0.0)
            states.append((maxima, weights, jnp.sum(weights, axis=1, keepdims=True)))
        for r in picks:
            maxima, weights, totals = states[r]
            numerator = jnp.concatenate(
                [
                    dot(weights[k * group : (k + 1) * group].astype(BF16), uv[base + r, k])
                    for k in range(kv)
                ],
                axis=0,
            )
            value = numerator * (1.0 / totals)
            level = jnp.broadcast_to(maxima * scale + jnp.log2(totals), (heads, width))
            for z in range(2):
                suf_o[z, base + r] = value[z * mine : (z + 1) * mine]
                suf_e[z, base + r] = level[z * mine : (z + 1) * mine]

    def sweep(items):
        states = {}
        ahead = [dot(item[1](), item[3], NT) for item in items[:1]]
        for index, (name, _, values, _) in enumerate(items):
            scores = ahead.pop(0)
            if index + 1 < len(items):
                item = items[index + 1]
                ahead.append(dot(item[1](), item[3], NT))
            top = jnp.max(scores, axis=0, keepdims=True)
            weights = exp2((scores - top) * scale)
            total = jnp.sum(weights, axis=0, keepdims=True)
            part = (top * scale, total, dot(values(), weights.astype(BF16), TN))
            if name in states:
                state = states[name]
                top = jnp.maximum(state[0], part[0])
                a, b = exp2(state[0] - top), exp2(part[0] - top)
                part = (top, state[1] * a + part[1] * b, state[2] * a + part[2] * b)
            states[name] = part
        return {
            name: (numerator * (1.0 / total), top + jnp.log2(total))
            for name, (top, total, numerator) in states.items()
        }

    def pieces(name, buf, h, step, query):
        tokens = buf.shape[2]
        step = min(step, tokens)
        return [
            (
                name,
                lambda base=base: buf[0, h, base : base + step, :],
                lambda base=base: buf[1, h, base : base + step, :],
                query,
            )
            for base in range(0, tokens, step)
        ]

    zone = iota((1, tile), 1) // cell

    slim = (slice(None), pl.ds(0, 1))

    def ret_copies(h, i):
        return [
            remote(
                src.at[h, i, slim[index]],
                dst.at[h, e, slim[index]],
                ret_send.at[index, h, i],
                ret_recv.at[index, h, e],
                {"kv": far + i},
            )
            for index, (src, dst) in enumerate(((rs_o, rr_o), (rs_e, rr_e)))
        ]

    def ret_arrivals(h, i):
        return [
            remote(
                dst.at[h, i, slim[index]],
                dst.at[h, i, slim[index]],
                ret_send.at[index, h, i],
                ret_recv.at[index, h, i],
                {"kv": far + i},
            )
            for index, dst in enumerate((rr_o, rr_e))
        ]

    def mate_copies(h):
        return [
            remote(
                src.at[h, slim[index]],
                dst.at[h, slim[index]],
                ret_send.at[index, h, 2],
                ret_recv.at[index, h, 2],
                {"kv": mate},
            )
            for index, (src, dst) in enumerate(((ps_o, pr_o), (ps_e, pr_e)))
        ]

    def arrive(h):
        with scope("local"):
            for copy in task_local[h]:
                copy.wait()
        with scope("queries"):
            for copy in query_arrivals(h):
                copy.wait_recv()
        with scope("taskwait"):
            for copy in task_arrivals(h):
                copy.wait_recv()

    def system(h):
        with scope("syswait"):
            if h == 0:
                for copy in sys_local:
                    copy.wait()
            for copy in sys_arrivals(h):
                copy.wait_recv()

    def gather(h):
        for i in range(2):
            qx[h, cellat(i * tile + e * cell), :] = tq[h, cellat(i * tile + e * cell), :]

    def task_items(h):
        return pieces("task", taskb, h, 1024, tq[h])

    def cross_items(h):
        return pieces("cross", sysb, h, 1024, qx[h])

    def keep_task(h, found):
        value, level = found
        base_o[h] = value
        base_e[h] = jnp.broadcast_to(level, (8, lanes))
        near = value[:, tile:]
        packed = jnp.where(
            zone == 1 - e,
            near[: width // 2],
            pltpu.roll(near[width // 2 :], cell, 1),
        )
        ps_o[h] = packed.astype(BF16)
        ps_e[h] = jnp.broadcast_to(level[:, tile:], (8, tile))

    def keep_cross(h, found, task):
        value, level = found
        for i in range(2):
            cut = slice(i * tile, (i + 1) * tile)
            task_level = jnp.where(zone == e, task[1][:, cut], NEGATIVE)
            merged = blend([(value[:, cut], level[:, cut]), (task[0][:, cut], task_level)])
            rs_o[h, i] = merged[0].astype(BF16)
            rs_e[h, i] = jnp.broadcast_to(merged[1], (8, tile))

    def home():
        items = []
        for h in range(per):
            items += pieces(h, sysb, h, 1024, qs[h])
        found = sweep(items)
        for h in range(per):
            value, level = found[h]
            task_level = jnp.where(zone == 1 - e, base_e[h, 0:1, :tile], NEGATIVE)
            merged = blend([(value[:, :tile], level[:, :tile]), (base_o[h, :, :tile], task_level)])
            base_o[h] = jnp.concatenate([merged[0], value[:, tile:]], axis=1)
            base_e[h] = jnp.broadcast_to(
                jnp.concatenate([merged[1], level[:, tile:]], axis=1), (8, lanes)
            )

    def exchange():
        return [
            remote(
                src.at[other],
                dst,
                sx_send.at[index],
                sx_recv.at[index],
                {"sub": other},
            )
            for index, (src, dst) in enumerate(((suf_o, sib_o), (suf_e, sib_e)))
        ]

    def span(core):
        return pl.ds(pl.multiple_of(core * own * group, 128), own * group)

    def fold(h):
        value, level = None, None
        for core, o_ref, e_ref in ((s, suf_o.at[s], suf_e.at[s]), (other, sib_o, sib_e)):
            near = slice(h * group, (h + 1) * group)
            rest = o_ref[:, near, :].reshape(own * group, width)
            tall = e_ref[:, near, :].reshape(own * group, width)
            chosen = perm[:, span(core)]
            for _ in range(2):
                piece = rest.astype(BF16)
                rest = rest - piece.astype(F32)
                term = dot(piece, chosen, (((0,), (1,)), ((), ())))
                value = term if value is None else value + term
            tall = tall.T[0:1]
            term = jnp.sum(jnp.where(chosen.astype(F32) > 0.5, tall, 0.0), axis=1, keepdims=True)
            level = term if level is None else level + term
        level = jnp.broadcast_to(level, (lanes, width)).T[0:1]
        merged = blend([(base_o[h], base_e[h][0:1]), (value, level)])
        base_o[h] = merged[0]
        base_e[h] = jnp.broadcast_to(merged[1], (8, lanes))

    def finish(h):
        with scope("retwait"):
            for copy in ret_arrivals(h, 0) + ret_arrivals(h, 1) + mate_copies(h):
                copy.wait_recv()
        low = zone == 0
        far_o = [rr_o[h, c].astype(F32) for c in range(2)]
        far_e = [rr_e[h, c][0:1] for c in range(2)]
        crossed = [
            (jnp.where(low, far_o[1], far_o[0]), jnp.where(low, far_e[1], far_e[0])),
            (jnp.where(low, far_o[0], far_o[1]), jnp.where(low, far_e[0], far_e[1])),
        ]
        packed = pr_o[h].astype(F32)
        near = jnp.concatenate([packed, pltpu.roll(packed, cell, 1)], axis=0)
        near_level = jnp.where(zone == e, pr_e[h][0:1], NEGATIVE)
        results = []
        for i in range(2):
            cut = slice(i * tile, (i + 1) * tile)
            parts = [(base_o[h, :, cut], base_e[h, 0:1, cut]), crossed[i]]
            if i == 0:
                parts.append((near, near_level))
            results.append(blend(parts)[0])
        done = jnp.concatenate(results, axis=1).astype(BF16)
        for index, core in enumerate((other, s)):
            chosen = perm[:, span(core)]
            ordered = dot(chosen, done, (((0,), (1,)), ((), ())))
            out32[index, :, h * group : (h + 1) * group, :] = ordered.reshape(own, group, width)

    for copy in loads[2:]:
        copy.wait()

    def suffixes(low, high):
        with scope("suffix"):

            @pl.loop(low, high)
            def _(i):
                suffix(i * 4)

    with scope("barrier"):
        pl.semaphore_wait(barrier, 2 * n - 1)
    rank = e + side

    @pl.when(rank != 9)
    def _():
        for copy in query_copies(0):
            copy.start()

    @pl.when(rank == 0)
    def _():
        for copy in query_copies(1):
            copy.start()

    for copy in sys_copies(0) + task_copies(0):
        copy.start()

    @pl.when(rank == 9)
    def _():
        for copy in query_copies(0):
            copy.start()

    suffixes(0, 2)
    @pl.when(rank != 0)
    def _():
        for copy in query_copies(1):
            copy.start()

    suffixes(2, 2)
    for copy in sys_copies(1) + task_copies(1):
        copy.start()
    suffixes(2, own // 4 - 1)
    arrive(0)
    system(0)
    with scope("block"):
        gather(0)
        found = sweep(task_items(0) + cross_items(0))
        keep_cross(0, found["cross"], found["task"])
        keep_task(0, found["task"])
        for copy in ret_copies(0, 0) + ret_copies(0, 1) + mate_copies(0):
            copy.start()
    arrive(1)
    with scope("task"):
        gather(1)
        keep_task(1, sweep(task_items(1))["task"])
        for copy in mate_copies(1):
            copy.start()
    system(1)
    with scope("cross"):
        task = (base_o[1], base_e[1, 0:1])
        keep_cross(1, sweep(cross_items(1))["cross"], task)
        for copy in ret_copies(1, 0) + ret_copies(1, 1):
            copy.start()
    suffixes(own // 4 - 1, own // 4)
    for copy in exchange():
        copy.start()
    with scope("home"):
        home()
    with scope("sxwait"):
        for copy in exchange():
            copy.wait_recv()
    with scope("fold"):
        for h in range(per):
            fold(h)
    for h in range(per):
        with scope("finish"):
            finish(h)
    outb[...] = out32[0].astype(BF16)
    give = remote(outb, out_ref.at[:, pl.ds(first, mine), :], fin_send, fin_recv, {"sub": other})
    give.start()
    out_ref[:, pl.ds(first, mine), :] = out32[1].astype(BF16)

    for copy in query_copies(0) + sys_copies(0) + task_copies(0) + query_copies(1) + sys_copies(1) + task_copies(1):
        copy.wait_send()
    for h in range(per):
        for copy in mate_copies(h) + ret_copies(h, 0) + ret_copies(h, 1):
            copy.wait_send()
    for copy in exchange():
        copy.wait_send()
    with scope("tail"):
        give.wait_send()
        theirs = out_ref.at[:, pl.ds(pl.multiple_of(other * mine, 16), mine), :]
        remote(outb, theirs, fin_send, fin_recv, {"sub": other}).wait_recv()


def paired_call(n, args, out_shape):
    queries, sys_keys, _, task_keys, _, suffix_keys, _, task_ids, _ = args
    rows, heads, width = queries.shape
    kv = sys_keys.shape[0]
    group = heads // kv
    own = suffix_keys.shape[0]
    per = kv // 2
    mine = heads // 2
    cell = CAP * group
    tile = 2 * cell
    lanes = n * cell
    dma = pltpu.SemaphoreType.DMA
    inputs = (*args[:7], task_ids.reshape(1, rows), args[8])
    return pl.pallas_call(
        functools.partial(paired, n),
        out_shape=out_shape,
        in_specs=[pl.BlockSpec(memory_space=pl.ANY)] * 9,
        out_specs=pl.BlockSpec(memory_space=pltpu.VMEM),
        scratch_shapes=[
            pltpu.VMEM((rows, mine, width), BF16),
            pltpu.VMEM((own, heads, width), BF16),
            pltpu.VMEM((1, rows), jnp.int32),
            pltpu.SMEM((own,), jnp.int32),
            pltpu.VMEM((lanes, rows * group), BF16),
            pltpu.VMEM((per, lanes, width), BF16),
            pltpu.VMEM((per, lanes, width), BF16),
            pltpu.VMEM((per, lanes, width), BF16),
            pltpu.VMEM((2, per, n * sys_keys.shape[1], width), BF16),
            pltpu.VMEM((2, per, 2 * task_keys.shape[2], width), BF16),
            pltpu.VMEM(suffix_keys.shape, BF16),
            pltpu.VMEM(suffix_keys.shape, BF16),
            pltpu.VMEM((2, own, mine, width), F32),
            pltpu.VMEM((2, own, mine, width), F32),
            pltpu.VMEM((own, mine, width), F32),
            pltpu.VMEM((own, mine, width), F32),
            pltpu.VMEM((per, width, lanes), F32),
            pltpu.VMEM((per, 8, lanes), F32),
            pltpu.VMEM((per, 2, width, tile), BF16),
            pltpu.VMEM((per, 2, 8, tile), F32),
            pltpu.VMEM((per, 2, width, tile), BF16),
            pltpu.VMEM((per, 2, 8, tile), F32),
            pltpu.VMEM((per, width // 2, tile), BF16),
            pltpu.VMEM((per, 8, tile), F32),
            pltpu.VMEM((per, width // 2, tile), BF16),
            pltpu.VMEM((per, 8, tile), F32),
            pltpu.VMEM((2, own, mine, width), F32),
            pltpu.VMEM((own, mine, width), BF16),
            dma((4,)),
            dma((2,)),
            dma((2, per)),
            dma((2, own)),
            dma((2, per)),
            dma((2, per)),
            dma((2, per, 3)),
            dma((2, per, 3)),
            dma((per, 5)),
            dma((per, 5)),
            dma((2, per, 3)),
            dma((2, per, 3)),
            dma((2,)),
            dma((2,)),
            dma,
            dma,
        ],
        compiler_params=pltpu.CompilerParams(
            collective_id=0, has_side_effects=True, vmem_limit_bytes=48 * 1024 * 1024
        ),
        name="cascade",
    )(*(pltpu.with_memory_space_constraint(x, pltpu.HBM) for x in inputs))


def body(
    queries,
    sys_keys,
    sys_values,
    task_keys,
    task_values,
    suffix_keys,
    suffix_values,
    task_ids,
    suffix_len,
):
    n = lax.axis_size("kv")
    rows, heads, width = queries.shape
    kv = sys_keys.shape[0]
    group = heads // kv
    own = suffix_keys.shape[0]
    lanes = n * CAP * group
    half = lanes // 2
    out_shape = jax.ShapeDtypeStruct((own, heads, width), BF16)
    if n == 4 and rows == n * CAP and kv % 2 == 0 and 2 * CAP * group == width:
        args = (
            queries,
            sys_keys,
            sys_values,
            task_keys,
            task_values,
            suffix_keys,
            suffix_values,
            task_ids,
            suffix_len,
        )
        return paired_call(n, args, out_shape)
    vmem = pl.BlockSpec(memory_space=pltpu.VMEM)
    anywhere = pl.BlockSpec(memory_space=pl.ANY)
    dma = pltpu.SemaphoreType.DMA
    return pl.pallas_call(
        functools.partial(kernel, n),
        out_shape=out_shape,
        in_specs=[vmem] * 3 + [anywhere] * 4 + [vmem, pl.BlockSpec(memory_space=pltpu.SMEM)],
        out_specs=vmem,
        scratch_shapes=[
            pltpu.VMEM(task_keys.shape[1:], BF16),
            pltpu.VMEM(task_values.shape[1:], BF16),
            pltpu.VMEM(suffix_keys.shape, BF16),
            pltpu.VMEM(suffix_values.shape, BF16),
            pltpu.VMEM((n, kv, lanes, width), BF16),
            pltpu.VMEM((n, 2, kv, width, half), F32),
            pltpu.VMEM((n, 2, kv, 8, half), F32),
            pltpu.VMEM((n, kv, width, half), F32),
            pltpu.VMEM((n, kv, 8, half), F32),
            pltpu.VMEM((n, kv, width, half), BF16),
            pltpu.VMEM((n, kv, 8, half), F32),
            pltpu.VMEM((2, n, kv, width, half), BF16),
            pltpu.VMEM((2, n, kv, 8, half), F32),
            pltpu.VMEM((2, kv, width, half), F32),
            pltpu.VMEM((2, kv, 8, half), F32),
            pltpu.VMEM((own, heads, width), F32),
            pltpu.VMEM((own, heads, width), F32),
            pltpu.VMEM((own, heads, width), F32),
            dma((2,)),
            dma((2, own)),
            dma((2, kv)),
            dma((n, kv)),
            dma((n, kv)),
            dma((n, kv)),
            dma((n, kv)),
            dma((2, n, kv)),
            dma((2, n, kv)),
            dma((2, n, kv)),
            dma((2, 2, n, kv)),
            dma((2, kv)),
            dma((2, kv)),
        ],
        compiler_params=pltpu.CompilerParams(
            collective_id=0, has_side_effects=True, vmem_limit_bytes=60 * 1024 * 1024
        ),
        name="cascade",
    )(
        queries,
        sys_keys,
        sys_values,
        task_keys,
        task_values,
        suffix_keys,
        suffix_values,
        task_ids.reshape(1, rows),
        suffix_len,
    )


def solution(mesh):
    in_specs = (
        P(("replica", "kv"), "head", None),
        P(("replica", "head"), ("kv", "sub"), None),
        P(("replica", "head"), ("kv", "sub"), None),
        P(("replica", "kv"), "head", "sub", None),
        P(("replica", "kv"), "head", "sub", None),
        P(("replica", "kv", "sub"), "head", None, None),
        P(("replica", "kv", "sub"), "head", None, None),
        P(("replica", "kv")),
        P(("replica", "kv", "sub")),
    )
    out_specs = P(("replica", "kv", "sub"), "head", None)
    return jax.shard_map(body, mesh=mesh, in_specs=in_specs, out_specs=out_specs, check_vma=False)
```
